32 devices in a mesh: ang: 4 (over y, x), gy: 2 (over core), gx: 4 (over z).
Axes of the slice: x: 2, y: 2, z: 4, core: 2. Of those that a mesh axis runs over, the one named last changes fastest.
Arguments:
- spectrum_data: bfloat16 [2, 16, 16, 2048], P(None, None, 'gy', 'ang'), may hold values from -6 to 6
- offsets: int32 [2048], P('ang'), may hold values from 0 to 1020
- view_index: int32 [2048], P('ang'), may hold values from 0 to 1499
- kernel: float32 [4, 2048], P(None, 'ang'), may hold values from 0.25 to 1
- view_weight: float32 [1500], replicated, may hold values from 0.5 to 2
- volume: float32 [16, 16, 4096], P('ang', 'gy', 'gx'), may hold values from -6 to 6
- multiplier: float32 [16, 16, 4096], P('ang', 'gy', 'gx'), may hold values from -4 to 4
Outputs:
- denoised: float32 [16, 16, 4096], P('ang', 'gy', 'gx')
The draws below stay inside these ranges and needn't reach their ends.
Inputs may be any that keep to these rules, and one draw needn't show every extreme that they name: `offsets`: each offset is a cell of its sample's block of 1024 frequencies with the three cells after it in the block too.
All inputs are finite; a program needn't handle non-finite values.
Results may differ from the reference program's by a relative error of at most 0.0032.
Values sent between devices are 32-bit elements; how exact they have to be, the bound alone decides.
No kernel may reach another device: no remote copies, remote signals or barrier semaphores. Data moves between devices by JAX's collectives and lax.ppermute only.
A program may use at most 64 MiB of HBM per device.

```python
import math
import jax
import jax.numpy as jnp
from jax import lax

NX = 4096
VIEWS = 1500
TAPS = 4
PLANES = 16
TV_STEPS = 4
SAMP_DEV = 512
NY = 16
KB = 1024
SAMPLES = 2048
N_ANG = 4


def with_ends(values, stream_key, smallest, high):
    dims = values.shape
    index_at = [jax.random.randint(jax.random.fold_in(stream_key, axis), (), 0, dims[axis]) for axis in range(len(dims))]
    values = values.at[tuple(index_at)].set(smallest)
    longest = dims.index(max(dims))
    index_at[longest] = (index_at[longest] + 1) % dims[longest]
    return values.at[tuple(index_at)].set(high)


def levels(key, shape, shards, least, largest):
    loudness, own = 1.0, jax.random.fold_in(key, 6)
    for position, parts in shards:
        steps = jnp.exp(jax.random.uniform(jax.random.fold_in(own, position), (parts,), jnp.float32, least / len(shards), largest / len(shards)))
        loudness = loudness * jnp.repeat(steps, shape[position] // parts).reshape([-1 if axis == position else 1 for axis in range(len(shape))])
    return loudness


def bell_draw(own_key, extent, scale, reach, cuts=(), kind=jnp.bfloat16):
    values = jax.random.normal(own_key, extent, jnp.float32) * scale
    if len(cuts) > 0:
        values = levels(own_key, extent, cuts, -0.22, 0.18) * values
    return jnp.clip(values, min=-reach, max=reach).astype(kind)


def setup_inputs(seed: int = 0) -> dict:
    seeds = jax.random.split(jax.random.key(seed), 8)
    spectrum_data = bell_draw(seeds[0], (2, PLANES, NY, SAMPLES), 1.0, 6.0, ((2, 2), (3, 4)))
    offsets = with_ends(jax.random.randint(seeds[1], (SAMPLES,), 0, KB - 3), jax.random.fold_in(seeds[1], 1), 0, (KB - 3) - 1).astype(jnp.int32)
    view_index = with_ends(jax.random.randint(seeds[2], (SAMPLES,), 0, VIEWS), jax.random.fold_in(seeds[2], 1), 0, VIEWS - 1).astype(jnp.int32)
    kernel = jnp.clip(0.25 + 0.75 * jax.random.uniform(seeds[3], (TAPS, SAMPLES), jnp.float32) ** levels(seeds[3], (TAPS, SAMPLES), ((1, 4),), -0.2, 0.2), 0.25, 1.0)
    view_weight = jnp.clip(jnp.exp(jax.random.uniform(seeds[4], (VIEWS,), jnp.float32, math.log(0.5), math.log(2.0))), 0.5, 2.0)
    volume = bell_draw(seeds[5], (PLANES, NY, NX), 1.0, 6.0, ((0, 4), (1, 2), (2, 4)), jnp.float32)
    multiplier = bell_draw(seeds[6], (PLANES, NY, NX), 0.5, 4.0, ((0, 4), (1, 2), (2, 4)), jnp.float32)
    return {"spectrum_data": spectrum_data, "offsets": offsets, "view_index": view_index, "kernel": kernel, "view_weight": view_weight, "volume": volume, "multiplier": multiplier}


smooth_weight = 0.5
dual_step = 1.0 / 12.0

def wave_table(freq_first, freq_count, cell_first, cell_count):
    freq_ids = freq_first + jnp.arange(freq_count, dtype=jnp.int32)
    cell_ids = cell_first + jnp.arange(cell_count, dtype=jnp.int32)
    phase_cells = freq_ids[:, None] * cell_ids[None, :] % NX
    phase_angle = phase_cells.astype(jnp.float32) * (2.0 * math.pi / NX)
    return jnp.concatenate([jnp.cos(phase_angle), -jnp.sin(phase_angle)], axis=0).astype(jnp.bfloat16)

def spread_blocks(offsets, view_index, kernel, view_weight):
    block_size = NX // N_ANG
    cell_ids = jnp.arange(block_size, dtype=jnp.int32)
    local_first = offsets.reshape(N_ANG, SAMP_DEV).astype(jnp.int32)
    kernel_rows = kernel.reshape(kernel.shape[0], N_ANG, SAMP_DEV)
    spread_sum = jnp.zeros((N_ANG, SAMP_DEV, block_size), jnp.float32)
    for tap_index in range(kernel.shape[0]):
        spread_sum = spread_sum + jnp.where(cell_ids[None, None, :] == (local_first + tap_index)[:, :, None], kernel_rows[tap_index][:, :, None], jnp.float32(0.0))
    weights = view_weight[view_index].reshape(N_ANG, SAMP_DEV)
    return (weights[:, :, None] * spread_sum).astype(jnp.bfloat16)

def divergence(flow_field):
    plane_part = flow_field[0] - jnp.pad(flow_field[0], ((1, 0), (0, 0), (0, 0)))[:-1]
    row_part = flow_field[1] - jnp.pad(flow_field[1], ((0, 0), (1, 0), (0, 0)))[:, :-1]
    cell_part = flow_field[2] - jnp.pad(flow_field[2], ((0, 0), (0, 0), (1, 0)))[:, :, :-1]
    return plane_part + row_part + cell_part

def slopes(values):
    slope_plane = jnp.pad(values[1:] - values[:-1], ((0, 1), (0, 0), (0, 0)))
    slope_row = jnp.pad(values[:, 1:] - values[:, :-1], ((0, 0), (0, 1), (0, 0)))
    slope_cell = jnp.pad(values[:, :, 1:] - values[:, :, :-1], ((0, 0), (0, 0), (0, 1)))
    return (slope_plane, slope_row, slope_cell)

def reference(spectrum_data, offsets, view_index, kernel, view_weight, volume, multiplier):
    spread = spread_blocks(offsets, view_index, kernel, view_weight).astype(jnp.float32)
    wave_rows = wave_table(0, NX, 0, NX).astype(jnp.float32)
    line_count = spectrum_data.shape[2]

    def one_plane(plane_data):
        grouped = plane_data.astype(jnp.float32).reshape(2 * line_count, N_ANG, SAMP_DEV)
        gridded = jnp.einsum('rbs,bsk->rbk', grouped, spread, precision=lax.Precision.HIGHEST)
        gridded = gridded.astype(jnp.bfloat16).reshape(2 * line_count, NX)
        joined = jnp.concatenate([gridded[:line_count], gridded[line_count:]], axis=1).astype(jnp.float32)
        return jnp.dot(joined, wave_rows, precision=lax.Precision.HIGHEST)
    back = lax.map(one_plane, jnp.moveaxis(spectrum_data, 1, 0)) * NX ** (-0.5)
    source = volume - back + multiplier
    scaled = source / smooth_weight
    flow_field = jnp.zeros((3,) + source.shape, jnp.float32)
    for repeat in range(TV_STEPS):
        slope_plane, slope_row, slope_cell = slopes(divergence(flow_field) - scaled)
        slope_norm = jnp.sqrt(slope_plane * slope_plane + slope_row * slope_row + slope_cell * slope_cell)
        flow_field = (flow_field + dual_step * jnp.stack([slope_plane, slope_row, slope_cell])) / (1.0 + dual_step * slope_norm)
    return source - smooth_weight * divergence(flow_field)
```

```python
import functools
import math

import jax
import jax.numpy as jnp
from jax import lax
from jax.experimental import pallas as pl
from jax.experimental.pallas import tpu as pltpu
from jax.sharding import PartitionSpec as P

NX = 4096
TV_STEPS = 4
HALO = TV_STEPS
CHUNK = 128

smooth_weight = 0.5
dual_step = 1.0 / 12.0

NT = (((1,), (1,)), ((), ()))


def unit_circle(phase):
    phase = phase & (NX - 1)
    quarter = (phase + NX // 8) // (NX // 4)
    angle = (phase - quarter * (NX // 4)).astype(jnp.float32) * (2.0 * math.pi / NX)
    square = angle * angle
    sine = angle * (1.0 + square * (-1.0 / 6 + square * (1.0 / 120 + square * (-1.0 / 5040 + square * (1.0 / 362880)))))
    cosine = 1.0 + square * (-0.5 + square * (1.0 / 24 + square * (-1.0 / 720 + square * (1.0 / 40320))))
    odd = (quarter & 1) == 1
    first = jnp.where(odd, -sine, cosine)
    second = jnp.where(odd, cosine, sine)
    flip = (quarter & 2) == 2
    return jnp.where(flip, -first, first), jnp.where(flip, -second, second)


def project_kernel(
    place_ref, data_ref, offsets_ref, view_ref, taps_ref, weight_ref, volume_ref, multiplier_ref, edge_ref,
    out_ref,
    spread_ref, grid_ref, cos_ref, sin_ref, step_cos_ref, step_sin_ref, part_cos_ref, part_sin_ref, lines_ref, halo_ref, vm_ref,
):
    ang, gx = place_ref[0], place_ref[1]
    samples = data_ref.shape[1]
    lines = data_ref.shape[0] // 2
    block_size = spread_ref.shape[0]
    columns = volume_ref.shape[1]
    local_lines = volume_ref.shape[0]
    dests, window, _ = out_ref.shape
    block = window - 2 * HALO

    pieces = []
    for piece in range(samples // 128):
        view = view_ref[pl.ds(piece, 1), :]
        found = jnp.zeros((1, 128), jnp.float32)
        lane = jnp.broadcast_to(view & 127, (8, 128))
        for row in range(weight_ref.shape[0]):
            table = jnp.broadcast_to(weight_ref[pl.ds(row, 1), :], (8, 128))
            picked = jnp.take_along_axis(table, lane, axis=1)[:1]
            found = jnp.where(view // 128 == row, picked, found)
        pieces.append(found)
    weight = jnp.concatenate(pieces, axis=1)
    values = [weight * taps_ref[pl.ds(tap, 1), :] for tap in range(taps_ref.shape[0])]
    offsets = jnp.concatenate([offsets_ref[pl.ds(piece, 1), :] for piece in range(samples // 128)], axis=1)

    rows = 16
    cell = lax.broadcasted_iota(jnp.int32, (rows, samples), 0)
    start = jnp.broadcast_to(offsets, (rows, samples))
    values = [jnp.broadcast_to(value, (rows, samples)) for value in values]
    for first in range(0, block_size, rows):
        tap = cell - (start - first)
        spread = jnp.zeros((rows, samples), jnp.float32)
        for index, value in enumerate(values):
            spread = jnp.where(tap == index, value, spread)
        spread_ref[pl.ds(first, rows), :] = spread.astype(jnp.bfloat16)

    grid_ref[...] = lax.dot_general(
        data_ref[...], spread_ref[...], NT, preferred_element_type=jnp.float32
    ).astype(jnp.bfloat16)

    lines_ref[...] = jnp.zeros_like(lines_ref)
    lines_ref[pl.ds(pl.multiple_of(ang * local_lines, 8), local_lines), :] = volume_ref[...] + multiplier_ref[...]
    halo_ref[...] = jnp.zeros_like(halo_ref)
    halo_ref[pl.ds(pl.multiple_of(ang * local_lines, 8), local_lines), :] = edge_ref[...]
    edges = halo_ref[...].T
    vm_ref[pl.ds(0, HALO), :] = edges[:HALO]
    vm_ref[pl.ds(HALO + columns, HALO), :] = edges[HALO : 2 * HALO]
    for first in range(0, columns, 128):
        vm_ref[pl.ds(HALO + first, 128), :] = lines_ref[:, pl.ds(first, 128)].T

    freq = ang * block_size + lax.broadcasted_iota(jnp.int32, (8, block_size), 1)
    row = lax.broadcasted_iota(jnp.int32, (8, block_size), 0)
    base_cos, base_sin = unit_circle(freq * (gx * columns - HALO + row))
    for first in range(0, CHUNK // 8, 8):
        step_cos_ref[pl.ds(first, 8), :], step_sin_ref[pl.ds(first, 8), :] = unit_circle(freq * (8 * (row + first)))
    for first in range(0, part_cos_ref.shape[0], 8):
        part_cos_ref[pl.ds(first, 8), :], part_sin_ref[pl.ds(first, 8), :] = unit_circle(
            freq * (CHUNK * (row + first))
        )

    total = columns + 2 * HALO
    for part in range(pl.cdiv(total, CHUNK)):
        first = part * CHUNK
        count = min(CHUNK, total - first)
        slot = part % 2
        part_cos, part_sin = part_cos_ref[pl.ds(part, 1), :], part_sin_ref[pl.ds(part, 1), :]
        here_cos = base_cos * part_cos - base_sin * part_sin
        here_sin = base_sin * part_cos + base_cos * part_sin
        for step in range(0, pl.cdiv(count, 8), 2):
            pair_cos, pair_sin = [], []
            for one in (step, step + 1):
                step_cos, step_sin = step_cos_ref[pl.ds(one, 1), :], step_sin_ref[pl.ds(one, 1), :]
                pair_cos.append(here_cos * step_cos - here_sin * step_sin)
                pair_sin.append(-(here_sin * step_cos + here_cos * step_sin))
            cos_ref[slot, pl.ds(8 * step, 16), :] = jnp.concatenate(pair_cos, axis=0).astype(jnp.bfloat16)
            sin_ref[slot, pl.ds(8 * step, 16), :] = jnp.concatenate(pair_sin, axis=0).astype(jnp.bfloat16)
        made = max(16, count)
        total_part = lax.dot_general(
            cos_ref[slot, pl.ds(0, made), :], grid_ref[pl.ds(0, lines), :], NT, preferred_element_type=jnp.float32
        ) + lax.dot_general(
            sin_ref[slot, pl.ds(0, made), :], grid_ref[pl.ds(lines, lines), :], NT, preferred_element_type=jnp.float32
        )
        sent = vm_ref[pl.ds(first, count), :] - total_part[:count] * NX ** (-0.5)
        for dest in range(dests):
            low, high = max(first, dest * block), min(first + count, dest * block + window)
            if low < high:
                out_ref[dest, pl.ds(low - dest * block, high - low), :] = sent[low - first : high - first]


def project(place, data, offsets, view_index, taps, view_weight, volume, multiplier, edge, dests):
    lines = data.shape[0] // 2
    samples = data.shape[1]
    columns = volume.shape[1]
    block_size = NX // lax.axis_size("ang")
    window = columns // dests + 2 * HALO
    parts = pl.cdiv(columns + 2 * HALO, CHUNK)
    vmem = pl.BlockSpec(memory_space=pltpu.VMEM)
    return pl.pallas_call(
        project_kernel,
        out_shape=jax.ShapeDtypeStruct((dests, window, lines), jnp.float32),
        in_specs=[pl.BlockSpec(memory_space=pltpu.SMEM)] + [vmem] * 8,
        out_specs=vmem,
        scratch_shapes=[
            pltpu.VMEM((block_size, samples), jnp.bfloat16),
            pltpu.VMEM((2 * lines, block_size), jnp.bfloat16),
            pltpu.VMEM((2, CHUNK, block_size), jnp.bfloat16),
            pltpu.VMEM((2, CHUNK, block_size), jnp.bfloat16),
            pltpu.VMEM((CHUNK // 8, block_size), jnp.float32),
            pltpu.VMEM((CHUNK // 8, block_size), jnp.float32),
            pltpu.VMEM((8 * pl.cdiv(parts, 8), block_size), jnp.float32),
            pltpu.VMEM((8 * pl.cdiv(parts, 8), block_size), jnp.float32),
            pltpu.VMEM((lines, columns), jnp.float32),
            pltpu.VMEM((lines, 128), jnp.float32),
            pltpu.VMEM((columns + 2 * HALO, lines), jnp.float32),
        ],
        name="project",
    )(place, data, offsets, view_index, taps, view_weight, volume, multiplier, edge)


def smooth_kernel(planes, place_ref, parts_ref, out_ref):
    dests, local_lines, block = out_ref.shape
    sources, window, lines = parts_ref.shape
    groups = dests * local_lines // lines
    angs = sources // groups
    rows = lines // planes
    lane = lax.broadcasted_iota(jnp.int32, (window, lines), 1)
    lane_row = lane % rows
    column = place_ref[2] + lax.broadcasted_iota(jnp.int32, (window, lines), 0)
    plane_open = lane // rows < planes - 1
    row_first = lane_row == 0
    row_last = lane_row == rows - 1
    cell_open = (column >= 0) & (column < NX - 1)
    zero = jnp.float32(0.0)

    source = []
    for group in range(groups):
        total = parts_ref[group]
        for ang in range(1, angs):
            total = total + parts_ref[ang * groups + group]
        source.append(total)
    scaled = [value / smooth_weight for value in source]

    def down(values):
        lower = []
        for group in range(groups):
            previous = values[group - 1]
            lower.append(
                jnp.where(
                    row_first, pltpu.roll(previous, lines - (rows - 1), 1), pltpu.roll(values[group], 1, 1)
                )
            )
        return lower

    flow = None
    for repeat in range(TV_STEPS + 1):
        if flow is None:
            target = [-value for value in scaled]
        else:
            lower_row = down([f[1] for f in flow])
            local_div = []
            for group in range(groups):
                f0, f1, f2 = flow[group]
                plane_part = f0 - pltpu.roll(f0, rows, 1)
                row_part = f1 - lower_row[group]
                cell_part = f2 - pltpu.roll(f2, 1, 0)
                local_div.append(plane_part + row_part + cell_part)
            if repeat == TV_STEPS:
                for group in range(groups):
                    done = source[group] - smooth_weight * local_div[group]
                    turned = done[HALO : HALO + block].T
                    for ang in range(angs):
                        out_ref[ang * groups + group] = turned[ang * local_lines : (ang + 1) * local_lines]
                return
            target = [local_div[group] - scaled[group] for group in range(groups)]
        updated = []
        for group in range(groups):
            here = target[group]
            slope_plane = jnp.where(plane_open, pltpu.roll(here, lines - rows, 1) - here, zero)
            if group + 1 < groups:
                upper = jnp.where(
                    row_last, pltpu.roll(target[group + 1], rows - 1, 1), pltpu.roll(here, lines - 1, 1)
                )
                slope_row = upper - here
            else:
                slope_row = jnp.where(row_last, zero, pltpu.roll(here, lines - 1, 1) - here)
            slope_cell = jnp.where(cell_open, pltpu.roll(here, window - 1, 0) - here, zero)
            slope_norm = jnp.sqrt(slope_plane * slope_plane + slope_row * slope_row + slope_cell * slope_cell)
            scale = 1.0 / (1.0 + dual_step * slope_norm)
            moved = [dual_step * slope_plane, dual_step * slope_row, dual_step * slope_cell]
            if flow is not None:
                moved = [f + m for f, m in zip(flow[group], moved)]
            updated.append([m * scale for m in moved])
        flow = updated


def smooth(place, parts, planes, local_lines):
    sources, window, lines = parts.shape
    vmem = pl.BlockSpec(memory_space=pltpu.VMEM)
    return pl.pallas_call(
        functools.partial(smooth_kernel, planes),
        out_shape=jax.ShapeDtypeStruct((sources, local_lines, window - 2 * HALO), jnp.float32),
        in_specs=[pl.BlockSpec(memory_space=pltpu.SMEM), vmem],
        out_specs=vmem,
        name="smooth",
    )(place, parts)


def passed_along(block, axis, distance):
    devices = range(lax.axis_size(axis))
    route = [(i - distance, i) for i in devices if i - distance in devices]
    return lax.ppermute(block, axis, route)


def per_device(spectrum_data, offsets, view_index, kernel, view_weight, volume, multiplier):
    local_planes, rows, columns = volume.shape
    planes = spectrum_data.shape[1]
    samples = spectrum_data.shape[3]
    dests = lax.axis_size("ang") * lax.axis_size("gy")
    block = columns // dests
    local_lines = local_planes * rows
    lines = planes * rows
    ang, gy, gx = lax.axis_index("ang"), lax.axis_index("gy"), lax.axis_index("gx")
    first_column = gx * columns + (ang * lax.axis_size("gy") + gy) * block - HALO
    place = jnp.stack([ang, gx, first_column]).astype(jnp.int32)

    volume = volume.reshape(local_lines, columns)
    multiplier = multiplier.reshape(local_lines, columns)
    left = passed_along(volume[:, -HALO:] + multiplier[:, -HALO:], "gx", 1)
    right = passed_along(volume[:, :HALO] + multiplier[:, :HALO], "gx", -1)
    edge = jnp.pad(jnp.concatenate([left, right], axis=1), ((0, 0), (0, 128 - 2 * HALO)))
    views = view_weight.shape[0]
    weight_rows = -(-views // 128)
    table = jnp.pad(view_weight, (0, weight_rows * 128 - views)).reshape(weight_rows, 128)
    parts = project(
        place,
        spectrum_data.reshape(2 * lines, samples),
        offsets.reshape(samples // 128, 128),
        view_index.reshape(samples // 128, 128),
        kernel,
        table,
        volume,
        multiplier,
        edge,
        dests,
    )
    parts = lax.all_to_all(parts, ("ang", "gy"), split_axis=0, concat_axis=0)
    done = smooth(place, parts, planes, local_lines)
    done = lax.all_to_all(done, ("ang", "gy"), split_axis=0, concat_axis=0)
    return jnp.transpose(done, (1, 0, 2)).reshape(local_planes, rows, columns)


def solution(mesh):
    placed = (
        P(None, None, "gy", "ang"),
        P("ang"),
        P("ang"),
        P(None, "ang"),
        P(),
        P("ang", "gy", "gx"),
        P("ang", "gy", "gx"),
    )
    return jax.shard_map(
        per_device, mesh=mesh, in_specs=placed, out_specs=P("ang", "gy", "gx"), check_vma=False
    )
```

```python
import functools
import math

import jax
import jax.numpy as jnp
from jax import lax
from jax.experimental import pallas as pl
from jax.experimental.pallas import tpu as pltpu
from jax.sharding import PartitionSpec as P

NX = 4096
TV_STEPS = 4
HALO = TV_STEPS
CHUNK = 128

smooth_weight = 0.5
dual_step = 1.0 / 12.0

NT = (((1,), (1,)), ((), ()))


def unit_circle(phase):
    phase = phase & (NX - 1)
    quarter = (phase + NX // 8) // (NX // 4)
    angle = (phase - quarter * (NX // 4)).astype(jnp.float32) * (2.0 * math.pi / NX)
    square = angle * angle
    sine = angle * (1.0 + square * (-1.0 / 6 + square * (1.0 / 120 + square * (-1.0 / 5040 + square * (1.0 / 362880)))))
    cosine = 1.0 + square * (-0.5 + square * (1.0 / 24 + square * (-1.0 / 720 + square * (1.0 / 40320))))
    odd = (quarter & 1) == 1
    first = jnp.where(odd, -sine, cosine)
    second = jnp.where(odd, cosine, sine)
    flip = (quarter & 2) == 2
    return jnp.where(flip, -first, first), jnp.where(flip, -second, second)


def project_kernel(
    data_ref, offsets_ref, view_ref, taps_ref, weight_ref, volume_ref, multiplier_ref,
    out_ref,
    spread_ref, grid_ref, cos_ref, sin_ref, step_cos_ref, step_sin_ref, part_cos_ref, part_sin_ref, lines_ref, vm_ref,
):
    ang, gx = lax.axis_index("ang"), lax.axis_index("gx")
    samples = data_ref.shape[1]
    lines = data_ref.shape[0] // 2
    block_size = spread_ref.shape[0]
    columns = volume_ref.shape[1]
    local_lines = volume_ref.shape[0]
    dests, window, _ = out_ref.shape
    block = window - 2 * HALO

    views = weight_ref.shape[0]
    pieces = []
    for piece in range(samples // 128):
        view = view_ref[pl.ds(piece, 1), :]
        found = jnp.zeros((1, 128), jnp.float32)
        lane = jnp.broadcast_to(view & 127, (8, 128))
        for first in range(0, views, 128):
            table = weight_ref[pl.ds(first, min(128, views - first))].reshape(1, -1)
            if views - first < 128:
                table = jnp.concatenate([table, jnp.zeros((1, 128 - (views - first)), jnp.float32)], axis=1)
            picked = jnp.take_along_axis(jnp.broadcast_to(table, (8, 128)), lane, axis=1)[:1]
            found = jnp.where(view // 128 == first // 128, picked, found)
        pieces.append(found)
    weight = jnp.concatenate(pieces, axis=1)
    values = [weight * taps_ref[pl.ds(tap, 1), :] for tap in range(taps_ref.shape[0])]
    offsets = jnp.concatenate([offsets_ref[pl.ds(piece, 1), :] for piece in range(samples // 128)], axis=1)

    rows = 16
    cell = lax.broadcasted_iota(jnp.int32, (rows, samples), 0)
    start = jnp.broadcast_to(offsets, (rows, samples))
    values = [jnp.broadcast_to(value, (rows, samples)) for value in values]
    for first in range(0, block_size, rows):
        tap = cell - (start - first)
        spread = jnp.zeros((rows, samples), jnp.float32)
        for index, value in enumerate(values):
            spread = jnp.where(tap == index, value, spread)
        spread_ref[pl.ds(first, rows), :] = spread.astype(jnp.bfloat16)

    grid_ref[...] = lax.dot_general(
        data_ref[...], spread_ref[...], NT, preferred_element_type=jnp.float32
    ).astype(jnp.bfloat16)

    lines_ref[...] = jnp.zeros_like(lines_ref)
    lines_ref[pl.ds(pl.multiple_of(ang * local_lines, 8), local_lines), :] = volume_ref[...] + multiplier_ref[...]
    vm_ref[pl.ds(0, HALO), :] = jnp.zeros((HALO, lines), jnp.float32)
    vm_ref[pl.ds(HALO + columns, HALO), :] = jnp.zeros((HALO, lines), jnp.float32)
    for first in range(0, columns, 128):
        vm_ref[pl.ds(HALO + first, 128), :] = lines_ref[:, pl.ds(first, 128)].T

    freq = ang * block_size + lax.broadcasted_iota(jnp.int32, (8, block_size), 1)
    row = lax.broadcasted_iota(jnp.int32, (8, block_size), 0)
    base_cos, base_sin = unit_circle(freq * (gx * columns - HALO + row))
    for first in range(0, CHUNK // 8, 8):
        step_cos_ref[pl.ds(first, 8), :], step_sin_ref[pl.ds(first, 8), :] = unit_circle(freq * (8 * (row + first)))
    for first in range(0, part_cos_ref.shape[0], 8):
        part_cos_ref[pl.ds(first, 8), :], part_sin_ref[pl.ds(first, 8), :] = unit_circle(
            freq * (CHUNK * (row + first))
        )

    total = columns + 2 * HALO
    for part in range(pl.cdiv(total, CHUNK)):
        first = part * CHUNK
        count = min(CHUNK, total - first)
        slot = part % 2
        part_cos, part_sin = part_cos_ref[pl.ds(part, 1), :], part_sin_ref[pl.ds(part, 1), :]
        here_cos = base_cos * part_cos - base_sin * part_sin
        here_sin = base_sin * part_cos + base_cos * part_sin
        for step in range(0, pl.cdiv(count, 8), 2):
            pair_cos, pair_sin = [], []
            for one in (step, step + 1):
                step_cos, step_sin = step_cos_ref[pl.ds(one, 1), :], step_sin_ref[pl.ds(one, 1), :]
                pair_cos.append(here_cos * step_cos - here_sin * step_sin)
                pair_sin.append(-(here_sin * step_cos + here_cos * step_sin))
            cos_ref[slot, pl.ds(8 * step, 16), :] = jnp.concatenate(pair_cos, axis=0).astype(jnp.bfloat16)
            sin_ref[slot, pl.ds(8 * step, 16), :] = jnp.concatenate(pair_sin, axis=0).astype(jnp.bfloat16)
        made = max(16, count)
        total_part = lax.dot_general(
            cos_ref[slot, pl.ds(0, made), :], grid_ref[pl.ds(0, lines), :], NT, preferred_element_type=jnp.float32
        ) + lax.dot_general(
            sin_ref[slot, pl.ds(0, made), :], grid_ref[pl.ds(lines, lines), :], NT, preferred_element_type=jnp.float32
        )
        sent = vm_ref[pl.ds(first, count), :] - total_part[:count] * NX ** (-0.5)
        for dest in range(dests):
            low, high = max(first, dest * block), min(first + count, dest * block + window)
            if low < high:
                out_ref[dest, pl.ds(low - dest * block, high - low), :] = sent[low - first : high - first]


def project(data, offsets, view_index, taps, view_weight, volume, multiplier, dests):
    lines = data.shape[0] // 2
    samples = data.shape[1]
    columns = volume.shape[1]
    block_size = NX // lax.axis_size("ang")
    window = columns // dests + 2 * HALO
    parts = pl.cdiv(columns + 2 * HALO, CHUNK)
    vmem = pl.BlockSpec(memory_space=pltpu.VMEM)
    return pl.pallas_call(
        project_kernel,
        out_shape=pltpu.VMEM((dests, window, lines), jnp.float32),
        in_specs=[vmem] * 7,
        out_specs=vmem,
        scratch_shapes=[
            pltpu.VMEM((block_size, samples), jnp.bfloat16),
            pltpu.VMEM((2 * lines, block_size), jnp.bfloat16),
            pltpu.VMEM((2, CHUNK, block_size), jnp.bfloat16),
            pltpu.VMEM((2, CHUNK, block_size), jnp.bfloat16),
            pltpu.VMEM((CHUNK // 8, block_size), jnp.float32),
            pltpu.VMEM((CHUNK // 8, block_size), jnp.float32),
            pltpu.VMEM((8 * pl.cdiv(parts, 8), block_size), jnp.float32),
            pltpu.VMEM((8 * pl.cdiv(parts, 8), block_size), jnp.float32),
            pltpu.VMEM((lines, columns), jnp.float32),
            pltpu.VMEM((columns + 2 * HALO, lines), jnp.float32),
        ],
        cost_estimate=pl.CostEstimate(flops=4 * 10**9, transcendentals=0, bytes_accessed=10**6),
        name="project",
    )(data, offsets, view_index, taps, view_weight, volume, multiplier)


def close_kernel(parts_ref, left_ref, right_ref, out_ref, halo_ref):
    ang = lax.axis_index("ang")
    dests, window, lines = parts_ref.shape
    local_lines = left_ref.shape[0]
    halo_ref[...] = jnp.zeros_like(halo_ref)
    own = pl.ds(pl.multiple_of(ang * local_lines, 8), local_lines)
    halo_ref[own, pl.ds(0, HALO)] = left_ref[...]
    halo_ref[own, pl.ds(HALO, HALO)] = right_ref[...]
    edges = halo_ref[...].T
    out_ref[0, pl.ds(0, HALO), :] = parts_ref[0, pl.ds(0, HALO), :] + edges[:HALO]
    last = pl.ds(window - HALO, HALO)
    out_ref[dests - 1, last, :] = parts_ref[dests - 1, last, :] + edges[HALO : 2 * HALO]


def close(parts, left, right):
    vmem = pl.BlockSpec(memory_space=pltpu.VMEM)
    return pl.pallas_call(
        close_kernel,
        out_shape=pltpu.VMEM(parts.shape, parts.dtype),
        in_specs=[vmem] * 3,
        out_specs=vmem,
        scratch_shapes=[pltpu.VMEM((parts.shape[2], 128), jnp.float32)],
        input_output_aliases={0: 0},
        name="close",
    )(parts, left, right)


def smooth_kernel(planes, columns, parts_ref, out_ref):
    dests, local_lines, block = out_ref.shape
    sources, window, lines = parts_ref.shape
    groups = dests * local_lines // lines
    angs = sources // groups
    rows = lines // planes
    lane = lax.broadcasted_iota(jnp.int32, (window, lines), 1)
    lane_row = lane % rows
    place = lax.axis_index("ang") * groups + lax.axis_index("gy")
    column = lax.axis_index("gx") * columns + place * block - HALO + lax.broadcasted_iota(jnp.int32, (window, lines), 0)
    plane_open = lane // rows < planes - 1
    row_first = lane_row == 0
    row_last = lane_row == rows - 1
    cell_open = (column >= 0) & (column < NX - 1)
    zero = jnp.float32(0.0)

    source = []
    for group in range(groups):
        total = parts_ref[group]
        for ang in range(1, angs):
            total = total + parts_ref[ang * groups + group]
        source.append(total)
    scaled = [value / smooth_weight for value in source]

    def down(values):
        lower = []
        for group in range(groups):
            previous = values[group - 1]
            lower.append(
                jnp.where(
                    row_first, pltpu.roll(previous, lines - (rows - 1), 1), pltpu.roll(values[group], 1, 1)
                )
            )
        return lower

    flow = None
    for repeat in range(TV_STEPS + 1):
        if flow is None:
            target = [-value for value in scaled]
        else:
            lower_row = down([f[1] for f in flow])
            local_div = []
            for group in range(groups):
                f0, f1, f2 = flow[group]
                plane_part = f0 - pltpu.roll(f0, rows, 1)
                row_part = f1 - lower_row[group]
                cell_part = f2 - pltpu.roll(f2, 1, 0)
                local_div.append(plane_part + row_part + cell_part)
            if repeat == TV_STEPS:
                for group in range(groups):
                    done = source[group] - smooth_weight * local_div[group]
                    turned = done[HALO : HALO + block].T
                    for ang in range(angs):
                        out_ref[ang * groups + group] = turned[ang * local_lines : (ang + 1) * local_lines]
                return
            target = [local_div[group] - scaled[group] for group in range(groups)]
        updated = []
        for group in range(groups):
            here = target[group]
            slope_plane = jnp.where(plane_open, pltpu.roll(here, lines - rows, 1) - here, zero)
            if group + 1 < groups:
                upper = jnp.where(
                    row_last, pltpu.roll(target[group + 1], rows - 1, 1), pltpu.roll(here, lines - 1, 1)
                )
                slope_row = upper - here
            else:
                slope_row = jnp.where(row_last, zero, pltpu.roll(here, lines - 1, 1) - here)
            slope_cell = jnp.where(cell_open, pltpu.roll(here, window - 1, 0) - here, zero)
            slope_norm = jnp.sqrt(slope_plane * slope_plane + slope_row * slope_row + slope_cell * slope_cell)
            scale = 1.0 / (1.0 + dual_step * slope_norm)
            moved = [dual_step * slope_plane, dual_step * slope_row, dual_step * slope_cell]
            if flow is not None:
                moved = [f + m for f, m in zip(flow[group], moved)]
            updated.append([m * scale for m in moved])
        flow = updated


def smooth(parts, planes, local_lines, columns):
    sources, window, lines = parts.shape
    vmem = pl.BlockSpec(memory_space=pltpu.VMEM)
    return pl.pallas_call(
        functools.partial(smooth_kernel, planes, columns),
        out_shape=pltpu.VMEM((sources, local_lines, window - 2 * HALO), jnp.float32),
        in_specs=[vmem],
        out_specs=vmem,
        name="smooth",
    )(parts)


def passed_along(block, axis, distance):
    devices = range(lax.axis_size(axis))
    route = [(i - distance, i) for i in devices if i - distance in devices]
    return lax.ppermute(block, axis, route)


def per_device(spectrum_data, offsets, view_index, kernel, view_weight, volume, multiplier):
    local_planes, rows, columns = volume.shape
    planes = spectrum_data.shape[1]
    samples = spectrum_data.shape[3]
    dests = lax.axis_size("ang") * lax.axis_size("gy")
    local_lines = local_planes * rows
    lines = planes * rows

    volume = volume.reshape(local_lines, columns)
    multiplier = multiplier.reshape(local_lines, columns)
    left = passed_along(volume[:, -HALO:] + multiplier[:, -HALO:], "gx", 1)
    right = passed_along(volume[:, :HALO] + multiplier[:, :HALO], "gx", -1)
    parts = project(
        spectrum_data.reshape(2 * lines, samples),
        offsets.reshape(samples // 128, 128),
        view_index.reshape(samples // 128, 128),
        kernel,
        view_weight,
        volume,
        multiplier,
        dests,
    )
    left = pltpu.with_memory_space_constraint(left, pltpu.VMEM)
    right = pltpu.with_memory_space_constraint(right, pltpu.VMEM)
    parts = close(parts, left, right)
    parts = lax.all_to_all(parts, ("ang", "gy"), split_axis=0, concat_axis=0)
    parts = pltpu.with_memory_space_constraint(parts, pltpu.VMEM)
    done = smooth(parts, planes, local_lines, columns)
    done = lax.all_to_all(done, ("ang", "gy"), split_axis=0, concat_axis=0)
    return jnp.transpose(done, (1, 0, 2)).reshape(local_planes, rows, columns)


def solution(mesh):
    placed = (
        P(None, None, "gy", "ang"),
        P("ang"),
        P("ang"),
        P(None, "ang"),
        P(),
        P("ang", "gy", "gx"),
        P("ang", "gy", "gx"),
    )
    return jax.shard_map(
        per_device, mesh=mesh, in_specs=placed, out_specs=P("ang", "gy", "gx"), check_vma=False
    )
```

```python
import functools
import math

import jax
import jax.numpy as jnp
from jax import lax
from jax.experimental import pallas as pl
from jax.experimental.pallas import tpu as pltpu
from jax.sharding import PartitionSpec as P

NX = 4096
TV_STEPS = 4
HALO = TV_STEPS
CHUNK = 128

smooth_weight = 0.5
dual_step = 1.0 / 12.0

NT = (((1,), (1,)), ((), ()))


def unit_circle(phase):
    phase = phase & (NX - 1)
    quarter = (phase + NX // 8) // (NX // 4)
    angle = (phase - quarter * (NX // 4)).astype(jnp.float32) * (2.0 * math.pi / NX)
    square = angle * angle
    sine = angle * (1.0 + square * (-1.0 / 6 + square * (1.0 / 120 + square * (-1.0 / 5040 + square * (1.0 / 362880)))))
    cosine = 1.0 + square * (-0.5 + square * (1.0 / 24 + square * (-1.0 / 720 + square * (1.0 / 40320))))
    odd = (quarter & 1) == 1
    first = jnp.where(odd, -sine, cosine)
    second = jnp.where(odd, cosine, sine)
    flip = (quarter & 2) == 2
    return jnp.where(flip, -first, first), jnp.where(flip, -second, second)


def project_kernel(
    data_ref, offsets_ref, view_ref, taps_ref, weight_ref, volume_ref, multiplier_ref,
    out_ref,
    spread_ref, grid_ref, cos_ref, sin_ref, step_cos_ref, step_sin_ref, part_cos_ref, part_sin_ref, lines_ref, vm_ref,
):
    ang, gx = lax.axis_index("ang"), lax.axis_index("gx")
    samples = data_ref.shape[1]
    lines = data_ref.shape[0] // 2
    block_size = spread_ref.shape[0]
    columns = volume_ref.shape[1]
    local_lines = volume_ref.shape[0]
    dests, window, _ = out_ref.shape
    block = window - 2 * HALO

    views = weight_ref.shape[0]
    pieces = []
    for piece in range(samples // 128):
        view = view_ref[pl.ds(piece, 1), :]
        found = jnp.zeros((1, 128), jnp.float32)
        lane = jnp.broadcast_to(view & 127, (8, 128))
        for first in range(0, views, 128):
            table = weight_ref[pl.ds(first, min(128, views - first))].reshape(1, -1)
            if views - first < 128:
                table = jnp.concatenate([table, jnp.zeros((1, 128 - (views - first)), jnp.float32)], axis=1)
            picked = jnp.take_along_axis(jnp.broadcast_to(table, (8, 128)), lane, axis=1)[:1]
            found = jnp.where(view // 128 == first // 128, picked, found)
        pieces.append(found)
    weight = jnp.concatenate(pieces, axis=1)
    values = [weight * taps_ref[pl.ds(tap, 1), :] for tap in range(taps_ref.shape[0])]
    offsets = jnp.concatenate([offsets_ref[pl.ds(piece, 1), :] for piece in range(samples // 128)], axis=1)

    rows = 16
    cell = lax.broadcasted_iota(jnp.int32, (rows, samples), 0)
    start = jnp.broadcast_to(offsets, (rows, samples))
    values = [jnp.broadcast_to(value, (rows, samples)) for value in values]
    for first in range(0, block_size, rows):
        tap = cell - (start - first)
        spread = jnp.zeros((rows, samples), jnp.float32)
        for index, value in enumerate(values):
            spread = jnp.where(tap == index, value, spread)
        spread_ref[pl.ds(first, rows), :] = spread.astype(jnp.bfloat16)

    grid_ref[...] = lax.dot_general(
        data_ref[...], spread_ref[...], NT, preferred_element_type=jnp.float32
    ).astype(jnp.bfloat16)

    lines_ref[...] = jnp.zeros_like(lines_ref)
    lines_ref[pl.ds(pl.multiple_of(ang * local_lines, 8), local_lines), :] = volume_ref[...] + multiplier_ref[...]
    vm_ref[pl.ds(0, HALO), :] = jnp.zeros((HALO, lines), jnp.float32)
    vm_ref[pl.ds(HALO + columns, HALO), :] = jnp.zeros((HALO, lines), jnp.float32)
    for first in range(0, columns, 128):
        vm_ref[pl.ds(HALO + first, 128), :] = lines_ref[:, pl.ds(first, 128)].T

    freq = ang * block_size + lax.broadcasted_iota(jnp.int32, (8, block_size), 1)
    row = lax.broadcasted_iota(jnp.int32, (8, block_size), 0)
    base_cos, base_sin = unit_circle(freq * (gx * columns - HALO + row))
    for first in range(0, CHUNK // 8, 8):
        step_cos_ref[pl.ds(first, 8), :], step_sin_ref[pl.ds(first, 8), :] = unit_circle(freq * (8 * (row + first)))
    for first in range(0, part_cos_ref.shape[0], 8):
        part_cos_ref[pl.ds(first, 8), :], part_sin_ref[pl.ds(first, 8), :] = unit_circle(
            freq * (CHUNK * (row + first))
        )

    total = columns + 2 * HALO
    for part in range(pl.cdiv(total, CHUNK)):
        first = part * CHUNK
        count = min(CHUNK, total - first)
        slot = part % 2
        part_cos, part_sin = part_cos_ref[pl.ds(part, 1), :], part_sin_ref[pl.ds(part, 1), :]
        here_cos = base_cos * part_cos - base_sin * part_sin
        here_sin = base_sin * part_cos + base_cos * part_sin
        for step in range(0, pl.cdiv(count, 8), 2):
            pair_cos, pair_sin = [], []
            for one in (step, step + 1):
                step_cos, step_sin = step_cos_ref[pl.ds(one, 1), :], step_sin_ref[pl.ds(one, 1), :]
                pair_cos.append(here_cos * step_cos - here_sin * step_sin)
                pair_sin.append(-(here_sin * step_cos + here_cos * step_sin))
            cos_ref[slot, pl.ds(8 * step, 16), :] = jnp.concatenate(pair_cos, axis=0).astype(jnp.bfloat16)
            sin_ref[slot, pl.ds(8 * step, 16), :] = jnp.concatenate(pair_sin, axis=0).astype(jnp.bfloat16)
        made = max(16, count)
        total_part = lax.dot_general(
            cos_ref[slot, pl.ds(0, made), :], grid_ref[pl.ds(0, lines), :], NT, preferred_element_type=jnp.float32
        ) + lax.dot_general(
            sin_ref[slot, pl.ds(0, made), :], grid_ref[pl.ds(lines, lines), :], NT, preferred_element_type=jnp.float32
        )
        sent = vm_ref[pl.ds(first, count), :] - total_part[:count] * NX ** (-0.5)
        for dest in range(dests):
            low, high = max(first, dest * block), min(first + count, dest * block + window)
            if low < high:
                out_ref[dest, pl.ds(low - dest * block, high - low), :] = sent[low - first : high - first]


def project(data, offsets, view_index, taps, view_weight, volume, multiplier, dests):
    lines = data.shape[0] // 2
    samples = data.shape[1]
    columns = volume.shape[1]
    block_size = NX // lax.axis_size("ang")
    window = columns // dests + 2 * HALO
    parts = pl.cdiv(columns + 2 * HALO, CHUNK)
    vmem = pl.BlockSpec(memory_space=pltpu.VMEM)
    return pl.pallas_call(
        project_kernel,
        out_shape=pltpu.VMEM((dests, window, lines), jnp.float32),
        in_specs=[vmem] * 7,
        out_specs=vmem,
        scratch_shapes=[
            pltpu.VMEM((block_size, samples), jnp.bfloat16),
            pltpu.VMEM((2 * lines, block_size), jnp.bfloat16),
            pltpu.VMEM((2, CHUNK, block_size), jnp.bfloat16),
            pltpu.VMEM((2, CHUNK, block_size), jnp.bfloat16),
            pltpu.VMEM((CHUNK // 8, block_size), jnp.float32),
            pltpu.VMEM((CHUNK // 8, block_size), jnp.float32),
            pltpu.VMEM((8 * pl.cdiv(parts, 8), block_size), jnp.float32),
            pltpu.VMEM((8 * pl.cdiv(parts, 8), block_size), jnp.float32),
            pltpu.VMEM((lines, columns), jnp.float32),
            pltpu.VMEM((columns + 2 * HALO, lines), jnp.float32),
        ],
        cost_estimate=pl.CostEstimate(flops=4 * 10**9, transcendentals=0, bytes_accessed=10**6),
        name="project",
    )(data, offsets, view_index, taps, view_weight, volume, multiplier)


def close_kernel(parts_ref, inner_ref, outer_ref, out_ref, halo_ref):
    ang = lax.axis_index("ang")
    even = lax.axis_index("gx") % 2 == 0
    dests, window, lines = parts_ref.shape
    local_lines = inner_ref.shape[0]
    halo_ref[...] = jnp.zeros_like(halo_ref)
    own = pl.ds(pl.multiple_of(ang * local_lines, 8), local_lines)
    inner, outer = inner_ref[...], outer_ref[...]
    halo_ref[own, pl.ds(0, HALO)] = jnp.where(even, outer, inner)
    halo_ref[own, pl.ds(HALO, HALO)] = jnp.where(even, inner, outer)
    edges = halo_ref[...].T
    out_ref[0, pl.ds(0, HALO), :] = parts_ref[0, pl.ds(0, HALO), :] + edges[:HALO]
    last = pl.ds(window - HALO, HALO)
    out_ref[dests - 1, last, :] = parts_ref[dests - 1, last, :] + edges[HALO : 2 * HALO]


def close(parts, inner, outer):
    vmem = pl.BlockSpec(memory_space=pltpu.VMEM)
    return pl.pallas_call(
        close_kernel,
        out_shape=pltpu.VMEM(parts.shape, parts.dtype),
        in_specs=[vmem] * 3,
        out_specs=vmem,
        scratch_shapes=[pltpu.VMEM((parts.shape[2], 128), jnp.float32)],
        input_output_aliases={0: 0},
        name="close",
    )(parts, inner, outer)


def smooth_kernel(planes, columns, parts_ref, out_ref):
    dests, local_lines, block = out_ref.shape
    sources, window, lines = parts_ref.shape
    groups = dests * local_lines // lines
    angs = sources // groups
    rows = lines // planes
    lane = lax.broadcasted_iota(jnp.int32, (window, lines), 1)
    lane_row = lane % rows
    place = lax.axis_index("ang") * groups + lax.axis_index("gy")
    column = lax.axis_index("gx") * columns + place * block - HALO + lax.broadcasted_iota(jnp.int32, (window, lines), 0)
    plane_open = lane // rows < planes - 1
    row_first = lane_row == 0
    row_last = lane_row == rows - 1
    cell_open = (column >= 0) & (column < NX - 1)
    zero = jnp.float32(0.0)

    source = []
    for group in range(groups):
        total = parts_ref[group]
        for ang in range(1, angs):
            total = total + parts_ref[ang * groups + group]
        source.append(total)
    scaled = [value / smooth_weight for value in source]

    def down(values):
        lower = []
        for group in range(groups):
            previous = values[group - 1]
            lower.append(
                jnp.where(
                    row_first, pltpu.roll(previous, lines - (rows - 1), 1), pltpu.roll(values[group], 1, 1)
                )
            )
        return lower

    flow = None
    for repeat in range(TV_STEPS + 1):
        if flow is None:
            target = [-value for value in scaled]
        else:
            lower_row = down([f[1] for f in flow])
            local_div = []
            for group in range(groups):
                f0, f1, f2 = flow[group]
                plane_part = f0 - pltpu.roll(f0, rows, 1)
                row_part = f1 - lower_row[group]
                cell_part = f2 - pltpu.roll(f2, 1, 0)
                local_div.append(plane_part + row_part + cell_part)
            if repeat == TV_STEPS:
                for group in range(groups):
                    done = source[group] - smooth_weight * local_div[group]
                    turned = done[HALO : HALO + block].T
                    for ang in range(angs):
                        out_ref[ang * groups + group] = turned[ang * local_lines : (ang + 1) * local_lines]
                return
            target = [local_div[group] - scaled[group] for group in range(groups)]
        updated = []
        for group in range(groups):
            here = target[group]
            slope_plane = jnp.where(plane_open, pltpu.roll(here, lines - rows, 1) - here, zero)
            if group + 1 < groups:
                upper = jnp.where(
                    row_last, pltpu.roll(target[group + 1], rows - 1, 1), pltpu.roll(here, lines - 1, 1)
                )
                slope_row = upper - here
            else:
                slope_row = jnp.where(row_last, zero, pltpu.roll(here, lines - 1, 1) - here)
            slope_cell = jnp.where(cell_open, pltpu.roll(here, window - 1, 0) - here, zero)
            slope_norm = jnp.sqrt(slope_plane * slope_plane + slope_row * slope_row + slope_cell * slope_cell)
            scale = 1.0 / (1.0 + dual_step * slope_norm)
            moved = [dual_step * slope_plane, dual_step * slope_row, dual_step * slope_cell]
            if flow is not None:
                moved = [f + m for f, m in zip(flow[group], moved)]
            updated.append([m * scale for m in moved])
        flow = updated


def smooth(parts, planes, local_lines, columns):
    sources, window, lines = parts.shape
    vmem = pl.BlockSpec(memory_space=pltpu.VMEM)
    return pl.pallas_call(
        functools.partial(smooth_kernel, planes, columns),
        out_shape=pltpu.VMEM((sources, local_lines, window - 2 * HALO), jnp.float32),
        in_specs=[vmem],
        out_specs=vmem,
        name="smooth",
    )(parts)


def exchanged(block, axis, shift):
    count = lax.axis_size(axis)
    route = []
    for low in range(shift, count + shift - 1, 2):
        pair = (low % count, (low + 1) % count)
        route += [pair, pair[::-1]]
    return lax.ppermute(block, axis, route)


def per_device(spectrum_data, offsets, view_index, kernel, view_weight, volume, multiplier):
    local_planes, rows, columns = volume.shape
    planes = spectrum_data.shape[1]
    samples = spectrum_data.shape[3]
    dests = lax.axis_size("ang") * lax.axis_size("gy")
    local_lines = local_planes * rows
    lines = planes * rows

    volume = volume.reshape(local_lines, columns)
    multiplier = multiplier.reshape(local_lines, columns)
    first_edge = volume[:, :HALO] + multiplier[:, :HALO]
    last_edge = volume[:, -HALO:] + multiplier[:, -HALO:]
    even = lax.axis_index("gx") % 2 == 0
    inner = exchanged(jnp.where(even, last_edge, first_edge), "gx", 0)
    outer = exchanged(jnp.where(even, first_edge, last_edge), "gx", 1)
    parts = project(
        spectrum_data.reshape(2 * lines, samples),
        offsets.reshape(samples // 128, 128),
        view_index.reshape(samples // 128, 128),
        kernel,
        view_weight,
        volume,
        multiplier,
        dests,
    )
    inner = pltpu.with_memory_space_constraint(inner, pltpu.VMEM)
    outer = pltpu.with_memory_space_constraint(outer, pltpu.VMEM)
    parts = close(parts, inner, outer)
    parts = lax.all_to_all(parts, ("ang", "gy"), split_axis=0, concat_axis=0)
    parts = pltpu.with_memory_space_constraint(parts, pltpu.VMEM)
    done = smooth(parts, planes, local_lines, columns)
    done = lax.all_to_all(done, ("ang", "gy"), split_axis=0, concat_axis=0)
    return jnp.transpose(done, (1, 0, 2)).reshape(local_planes, rows, columns)


def solution(mesh):
    placed = (
        P(None, None, "gy", "ang"),
        P("ang"),
        P("ang"),
        P(None, "ang"),
        P(),
        P("ang", "gy", "gx"),
        P("ang", "gy", "gx"),
    )
    return jax.shard_map(
        per_device, mesh=mesh, in_specs=placed, out_specs=P("ang", "gy", "gx"), check_vma=False
    )
```

```python
import functools
import math

import jax
import jax.numpy as jnp
from jax import lax
from jax.experimental import pallas as pl
from jax.experimental.pallas import tpu as pltpu
from jax.sharding import PartitionSpec as P

NX = 4096
TV_STEPS = 4
HALO = TV_STEPS
CHUNK = 128
VMEM_LIMIT = 24 * 2**20

smooth_weight = 0.5
dual_step = 1.0 / 12.0

NT = (((1,), (1,)), ((), ()))


def unit_circle(phase):
    phase = phase & (NX - 1)
    quarter = (phase + NX // 8) // (NX // 4)
    angle = (phase - quarter * (NX // 4)).astype(jnp.float32) * (2.0 * math.pi / NX)
    square = angle * angle
    sine = angle * (1.0 + square * (-1.0 / 6 + square * (1.0 / 120 + square * (-1.0 / 5040 + square * (1.0 / 362880)))))
    cosine = 1.0 + square * (-0.5 + square * (1.0 / 24 + square * (-1.0 / 720 + square * (1.0 / 40320))))
    odd = (quarter & 1) == 1
    first = jnp.where(odd, -sine, cosine)
    second = jnp.where(odd, cosine, sine)
    flip = (quarter & 2) == 2
    return jnp.where(flip, -first, first), jnp.where(flip, -second, second)


def make_spread(offsets_ref, view_ref, taps_ref, weight_ref, spread_ref):
    block_size, samples = spread_ref.shape
    views = weight_ref.shape[0]
    pieces = []
    for piece in range(samples // 128):
        view = view_ref[pl.ds(piece, 1), :]
        found = jnp.zeros((1, 128), jnp.float32)
        lane = jnp.broadcast_to(view & 127, (8, 128))
        for first in range(0, views, 128):
            table = weight_ref[pl.ds(first, min(128, views - first))].reshape(1, -1)
            if views - first < 128:
                table = jnp.concatenate([table, jnp.zeros((1, 128 - (views - first)), jnp.float32)], axis=1)
            picked = jnp.take_along_axis(jnp.broadcast_to(table, (8, 128)), lane, axis=1)[:1]
            found = jnp.where(view // 128 == first // 128, picked, found)
        pieces.append(found)
    weight = jnp.concatenate(pieces, axis=1)
    values = [weight * taps_ref[pl.ds(tap, 1), :] for tap in range(taps_ref.shape[0])]
    offsets = jnp.concatenate([offsets_ref[pl.ds(piece, 1), :] for piece in range(samples // 128)], axis=1)

    rows = 16
    cell = lax.broadcasted_iota(jnp.int32, (rows, samples), 0)
    start = jnp.broadcast_to(offsets, (rows, samples))
    values = [jnp.broadcast_to(value, (rows, samples)) for value in values]
    for first in range(0, block_size, rows):
        tap = cell - (start - first)
        spread = jnp.zeros((rows, samples), jnp.float32)
        for index, value in enumerate(values):
            spread = jnp.where(tap == index, value, spread)
        spread_ref[pl.ds(first, rows), :] = spread.astype(jnp.bfloat16)


def make_angles(first_column, step_cos_ref, step_sin_ref, part_cos_ref, part_sin_ref):
    block_size = step_cos_ref.shape[1]
    freq = lax.axis_index("ang") * block_size + lax.broadcasted_iota(jnp.int32, (8, block_size), 1)
    row = lax.broadcasted_iota(jnp.int32, (8, block_size), 0)
    for first in range(0, CHUNK // 8, 8):
        step_cos_ref[pl.ds(first, 8), :], step_sin_ref[pl.ds(first, 8), :] = unit_circle(freq * (8 * (row + first)))
    for first in range(0, part_cos_ref.shape[0], 8):
        part_cos_ref[pl.ds(first, 8), :], part_sin_ref[pl.ds(first, 8), :] = unit_circle(
            freq * (CHUNK * (row + first))
        )
    return unit_circle(freq * (first_column + row))


def make_waves(base, part, count, step_cos_ref, step_sin_ref, part_cos_ref, part_sin_ref, put):
    base_cos, base_sin = base
    part_cos, part_sin = part_cos_ref[pl.ds(part, 1), :], part_sin_ref[pl.ds(part, 1), :]
    here_cos = base_cos * part_cos - base_sin * part_sin
    here_sin = base_sin * part_cos + base_cos * part_sin
    for step in range(0, pl.cdiv(count, 8), 2):
        pair_cos, pair_sin = [], []
        for one in (step, step + 1):
            step_cos, step_sin = step_cos_ref[pl.ds(one, 1), :], step_sin_ref[pl.ds(one, 1), :]
            pair_cos.append(here_cos * step_cos - here_sin * step_sin)
            pair_sin.append(-(here_sin * step_cos + here_cos * step_sin))
        put(
            8 * step,
            jnp.concatenate(pair_cos, axis=0).astype(jnp.bfloat16),
            jnp.concatenate(pair_sin, axis=0).astype(jnp.bfloat16),
        )


def chunks(total):
    return [(part, part * CHUNK, min(CHUNK, total - part * CHUNK)) for part in range(pl.cdiv(total, CHUNK))]


def put_windows(out_ref, first, count, sent):
    dests, window, _ = out_ref.shape
    block = window - 2 * HALO
    for dest in range(dests):
        low, high = max(first, dest * block), min(first + count, dest * block + window)
        if low < high:
            out_ref[dest, pl.ds(low - dest * block, high - low), :] = sent[low - first : high - first]


def project_kernel(
    data_ref, offsets_ref, view_ref, taps_ref, weight_ref, volume_ref, multiplier_ref,
    out_ref,
    spread_ref, grid_ref, cos_ref, sin_ref, step_cos_ref, step_sin_ref, part_cos_ref, part_sin_ref, lines_ref, vm_ref,
):
    ang, gx = lax.axis_index("ang"), lax.axis_index("gx")
    lines = data_ref.shape[0] // 2
    local_lines, columns = volume_ref.shape

    make_spread(offsets_ref, view_ref, taps_ref, weight_ref, spread_ref)
    grid_ref[...] = lax.dot_general(
        data_ref[...], spread_ref[...], NT, preferred_element_type=jnp.float32
    ).astype(jnp.bfloat16)

    lines_ref[...] = jnp.zeros_like(lines_ref)
    lines_ref[pl.ds(pl.multiple_of(ang * local_lines, 8), local_lines), :] = volume_ref[...] + multiplier_ref[...]
    vm_ref[pl.ds(0, HALO), :] = jnp.zeros((HALO, lines), jnp.float32)
    vm_ref[pl.ds(HALO + columns, HALO), :] = jnp.zeros((HALO, lines), jnp.float32)
    for first in range(0, columns, 128):
        vm_ref[pl.ds(HALO + first, 128), :] = lines_ref[:, pl.ds(first, 128)].T

    angles = (step_cos_ref, step_sin_ref, part_cos_ref, part_sin_ref)
    base = make_angles(gx * columns - HALO, *angles)
    for part, first, count in chunks(columns + 2 * HALO):
        slot = part % 2

        def put(at, cosines, sines):
            cos_ref[slot, pl.ds(at, 16), :] = cosines
            sin_ref[slot, pl.ds(at, 16), :] = sines

        make_waves(base, part, count, *angles, put)
        made = max(16, count)
        total_part = lax.dot_general(
            cos_ref[slot, pl.ds(0, made), :], grid_ref[pl.ds(0, lines), :], NT, preferred_element_type=jnp.float32
        ) + lax.dot_general(
            sin_ref[slot, pl.ds(0, made), :], grid_ref[pl.ds(lines, lines), :], NT, preferred_element_type=jnp.float32
        )
        put_windows(out_ref, first, count, vm_ref[pl.ds(first, count), :] - total_part[:count] * NX ** (-0.5))


def project(data, offsets, view_index, taps, view_weight, volume, multiplier, dests):
    lines = data.shape[0] // 2
    samples = data.shape[1]
    columns = volume.shape[1]
    block_size = NX // lax.axis_size("ang")
    window = columns // dests + 2 * HALO
    parts = pl.cdiv(columns + 2 * HALO, CHUNK)
    vmem = pl.BlockSpec(memory_space=pltpu.VMEM)
    return pl.pallas_call(
        project_kernel,
        out_shape=pltpu.VMEM((dests, window, lines), jnp.float32),
        in_specs=[vmem] * 7,
        out_specs=vmem,
        scratch_shapes=[
            pltpu.VMEM((block_size, samples), jnp.bfloat16),
            pltpu.VMEM((2 * lines, block_size), jnp.bfloat16),
            pltpu.VMEM((2, CHUNK, block_size), jnp.bfloat16),
            pltpu.VMEM((2, CHUNK, block_size), jnp.bfloat16),
            pltpu.VMEM((CHUNK // 8, block_size), jnp.float32),
            pltpu.VMEM((CHUNK // 8, block_size), jnp.float32),
            pltpu.VMEM((8 * pl.cdiv(parts, 8), block_size), jnp.float32),
            pltpu.VMEM((8 * pl.cdiv(parts, 8), block_size), jnp.float32),
            pltpu.VMEM((lines, columns), jnp.float32),
            pltpu.VMEM((columns + 2 * HALO, lines), jnp.float32),
        ],
        cost_estimate=pl.CostEstimate(flops=4 * 10**9, transcendentals=0, bytes_accessed=10**6),
        compiler_params=pltpu.CompilerParams(vmem_limit_bytes=VMEM_LIMIT),
        name="project",
    )(data, offsets, view_index, taps, view_weight, volume, multiplier)


def close_kernel(parts_ref, inner_ref, outer_ref, out_ref, halo_ref):
    ang = lax.axis_index("ang")
    even = lax.axis_index("gx") % 2 == 0
    dests, window, lines = parts_ref.shape
    local_lines = inner_ref.shape[0]
    halo_ref[...] = jnp.zeros_like(halo_ref)
    own = pl.ds(pl.multiple_of(ang * local_lines, 8), local_lines)
    inner, outer = inner_ref[...], outer_ref[...]
    halo_ref[own, pl.ds(0, HALO)] = jnp.where(even, outer, inner)
    halo_ref[own, pl.ds(HALO, HALO)] = jnp.where(even, inner, outer)
    edges = halo_ref[...].T
    out_ref[0, pl.ds(0, HALO), :] = parts_ref[0, pl.ds(0, HALO), :] + edges[:HALO]
    last = pl.ds(window - HALO, HALO)
    out_ref[dests - 1, last, :] = parts_ref[dests - 1, last, :] + edges[HALO : 2 * HALO]


def close(parts, inner, outer):
    vmem = pl.BlockSpec(memory_space=pltpu.VMEM)
    return pl.pallas_call(
        close_kernel,
        out_shape=pltpu.VMEM(parts.shape, parts.dtype),
        in_specs=[vmem] * 3,
        out_specs=vmem,
        scratch_shapes=[pltpu.VMEM((parts.shape[2], 128), jnp.float32)],
        input_output_aliases={0: 0},
        compiler_params=pltpu.CompilerParams(vmem_limit_bytes=VMEM_LIMIT),
        name="close",
    )(parts, inner, outer)


def smooth_kernel(planes, columns, parts_ref, out_ref):
    dests, local_lines, block = out_ref.shape
    window = parts_ref.shape[1]
    angs, groups = lax.axis_size("ang"), lax.axis_size("gy")
    lines = angs * local_lines
    rows = lines // planes
    joined = parts_ref.shape[0] == angs
    lane = lax.broadcasted_iota(jnp.int32, (window, lines), 1)
    lane_row = lane % rows
    place = lax.axis_index("gy") * angs + lax.axis_index("ang")
    column = lax.axis_index("gx") * columns + place * block - HALO + lax.broadcasted_iota(jnp.int32, (window, lines), 0)
    plane_open = lane // rows < planes - 1
    row_first = lane_row == 0
    row_last = lane_row == rows - 1
    cell_open = (column >= 0) & (column < NX - 1)
    zero = jnp.float32(0.0)

    source = []
    for group in range(groups):
        total = None
        for ang in range(angs):
            if joined:
                part = parts_ref[ang, :, pl.ds(group * lines, lines)]
            else:
                part = parts_ref[group * angs + ang]
            total = part if total is None else total + part
        source.append(total)
    scaled = [value / smooth_weight for value in source]

    def down(values):
        lower = []
        for group in range(groups):
            previous = values[group - 1]
            lower.append(
                jnp.where(
                    row_first, pltpu.roll(previous, lines - (rows - 1), 1), pltpu.roll(values[group], 1, 1)
                )
            )
        return lower

    flow = None
    for repeat in range(TV_STEPS + 1):
        if flow is None:
            target = [-value for value in scaled]
        else:
            lower_row = down([f[1] for f in flow])
            local_div = []
            for group in range(groups):
                f0, f1, f2 = flow[group]
                plane_part = f0 - pltpu.roll(f0, rows, 1)
                row_part = f1 - lower_row[group]
                cell_part = f2 - pltpu.roll(f2, 1, 0)
                local_div.append(plane_part + row_part + cell_part)
            if repeat == TV_STEPS:
                for group in range(groups):
                    done = source[group] - smooth_weight * local_div[group]
                    turned = done[HALO : HALO + block].T
                    for ang in range(angs):
                        out_ref[group * angs + ang] = turned[ang * local_lines : (ang + 1) * local_lines]
                return
            target = [local_div[group] - scaled[group] for group in range(groups)]
        updated = []
        for group in range(groups):
            here = target[group]
            slope_plane = jnp.where(plane_open, pltpu.roll(here, lines - rows, 1) - here, zero)
            if group + 1 < groups:
                upper = jnp.where(
                    row_last, pltpu.roll(target[group + 1], rows - 1, 1), pltpu.roll(here, lines - 1, 1)
                )
                slope_row = upper - here
            else:
                slope_row = jnp.where(row_last, zero, pltpu.roll(here, lines - 1, 1) - here)
            slope_cell = jnp.where(cell_open, pltpu.roll(here, window - 1, 0) - here, zero)
            slope_norm = jnp.sqrt(slope_plane * slope_plane + slope_row * slope_row + slope_cell * slope_cell)
            scale = 1.0 / (1.0 + dual_step * slope_norm)
            moved = [dual_step * slope_plane, dual_step * slope_row, dual_step * slope_cell]
            if flow is not None:
                moved = [f + m for f, m in zip(flow[group], moved)]
            updated.append([m * scale for m in moved])
        flow = updated


def smooth(parts, planes, local_lines, columns):
    window = parts.shape[1]
    dests = lax.axis_size("ang") * lax.axis_size("gy")
    vmem = pl.BlockSpec(memory_space=pltpu.VMEM)
    return pl.pallas_call(
        functools.partial(smooth_kernel, planes, columns),
        out_shape=pltpu.VMEM((dests, local_lines, window - 2 * HALO), jnp.float32),
        in_specs=[vmem],
        out_specs=vmem,
        compiler_params=pltpu.CompilerParams(vmem_limit_bytes=VMEM_LIMIT),
        name="smooth",
    )(parts)


def exchanged(block, axis, shift):
    count = lax.axis_size(axis)
    route = []
    for low in range(shift, count + shift - 1, 2):
        pair = (low % count, (low + 1) % count)
        route += [pair, pair[::-1]]
    return lax.ppermute(block, axis, route)


def pack_kernel(
    data_ref, offsets_ref, view_ref, taps_ref, weight_ref, volume_ref, multiplier_ref,
    sent_ref, data_out, offsets_out, view_out, taps_out, weight_out, own_ref,
    volume_here, multiplier_here, sems,
):
    rows = data_ref.shape[0]
    half = volume_ref.shape[1] // 2
    first = lax.axis_index("gy") == 0
    pairs = (
        (data_ref, data_out),
        (volume_ref, volume_here),
        (multiplier_ref, multiplier_here),
        (offsets_ref, offsets_out),
        (view_ref, view_out),
        (taps_ref, taps_out),
        (weight_ref, weight_out),
    )
    copies = [pltpu.make_async_copy(source, target, sems.at[at]) for at, (source, target) in enumerate(pairs)]
    for copy in copies:
        copy.start()
    copies[0].wait()
    sent_ref[pl.ds(0, rows), :] = data_out[...].astype(jnp.float32)
    copies[1].wait()
    copies[2].wait()
    low = volume_here[:, pl.ds(0, half)] + multiplier_here[:, pl.ds(0, half)]
    high = volume_here[:, pl.ds(half, half)] + multiplier_here[:, pl.ds(half, half)]
    below, above = low[:, half - HALO :], high[:, :HALO]
    local_lines = low.shape[0]
    own_ref[:, pl.ds(0, half)] = jnp.where(first, low, high)
    own_ref[:, pl.ds(half, HALO)] = jnp.where(first, above, below)
    sent_ref[pl.ds(rows, local_lines), :] = jnp.where(first, high, low)
    sent_ref[pl.ds(rows + local_lines, local_lines), pl.ds(0, HALO)] = jnp.where(first, below, above)
    for copy in copies[3:]:
        copy.wait()


def pack(data, offsets, view_index, taps, view_weight, volume, multiplier):
    rows, samples = data.shape
    local_lines, columns = volume.shape
    vmem = pl.BlockSpec(memory_space=pltpu.VMEM)
    return pl.pallas_call(
        pack_kernel,
        out_shape=[
            pltpu.VMEM((rows + 2 * local_lines, samples), jnp.float32),
            pltpu.VMEM(data.shape, data.dtype),
            pltpu.VMEM(offsets.shape, offsets.dtype),
            pltpu.VMEM(view_index.shape, view_index.dtype),
            pltpu.VMEM(taps.shape, taps.dtype),
            pltpu.VMEM(view_weight.shape, view_weight.dtype),
            pltpu.VMEM((local_lines, columns // 2 + 128), jnp.float32),
        ],
        in_specs=[pl.BlockSpec(memory_space=pltpu.HBM)] * 7,
        out_specs=[vmem] * 7,
        scratch_shapes=[
            pltpu.VMEM(volume.shape, volume.dtype),
            pltpu.VMEM(multiplier.shape, multiplier.dtype),
            pltpu.SemaphoreType.DMA((7,)),
        ],
        compiler_params=pltpu.CompilerParams(vmem_limit_bytes=VMEM_LIMIT),
        name="pack",
    )(
        *(
            pltpu.with_memory_space_constraint(array, pltpu.HBM)
            for array in (data, offsets, view_index, taps, view_weight, volume, multiplier)
        )
    )


def tables_kernel(
    columns, offsets_ref, view_ref, taps_ref, weight_ref,
    spread_ref, cos_ref, sin_ref,
    step_cos_ref, step_sin_ref, part_cos_ref, part_sin_ref,
):
    make_spread(offsets_ref, view_ref, taps_ref, weight_ref, spread_ref)
    angles = (step_cos_ref, step_sin_ref, part_cos_ref, part_sin_ref)
    base = make_angles(lax.axis_index("gx") * 2 * columns + lax.axis_index("gy") * columns - HALO, *angles)
    for part, first, count in chunks(columns + 2 * HALO):

        def put(at, cosines, sines):
            cos_ref[pl.ds(first + at, 16), :] = cosines
            sin_ref[pl.ds(first + at, 16), :] = sines

        make_waves(base, part, count, *angles, put)


def tables(offsets, view_index, taps, view_weight, columns):
    samples = taps.shape[1]
    block_size = NX // lax.axis_size("ang")
    made = 16 * pl.cdiv(columns + 2 * HALO, 16)
    parts = 8 * pl.cdiv(pl.cdiv(columns + 2 * HALO, CHUNK), 8)
    vmem = pl.BlockSpec(memory_space=pltpu.VMEM)
    return pl.pallas_call(
        functools.partial(tables_kernel, columns),
        out_shape=[
            pltpu.VMEM((block_size, samples), jnp.bfloat16),
            pltpu.VMEM((made, block_size), jnp.bfloat16),
            pltpu.VMEM((made, block_size), jnp.bfloat16),
        ],
        in_specs=[vmem] * 4,
        out_specs=[vmem] * 3,
        scratch_shapes=[
            pltpu.VMEM((CHUNK // 8, block_size), jnp.float32),
            pltpu.VMEM((CHUNK // 8, block_size), jnp.float32),
            pltpu.VMEM((parts, block_size), jnp.float32),
            pltpu.VMEM((parts, block_size), jnp.float32),
        ],
        cost_estimate=pl.CostEstimate(flops=2 * 10**9, transcendentals=0, bytes_accessed=10**6),
        compiler_params=pltpu.CompilerParams(vmem_limit_bytes=VMEM_LIMIT),
        name="tables",
    )(offsets, view_index, taps, view_weight)


def line_places(lines, local_lines):
    gy, inner = lax.axis_index("gy"), lax.axis_index("ang") * local_lines
    return [
        pl.ds(pl.multiple_of(group * lines + inner, 8), local_lines) for group in (gy, 1 - gy)
    ]


def edge_kernel(lines, own_ref, got_ref, out_ref, lines_ref):
    local_lines, half = own_ref.shape[0], own_ref.shape[1] - 128
    rows = got_ref.shape[0] - 2 * local_lines
    first = lax.axis_index("gy") == 0
    lines_ref[...] = jnp.zeros_like(lines_ref)
    own_place, other_place = line_places(lines, local_lines)
    other = pl.ds(rows, local_lines)
    for place, ref, at in ((own_place, own_ref, pl.ds(0, local_lines)), (other_place, got_ref, other)):
        lines_ref[place, pl.ds(0, HALO)] = jnp.where(
            first, ref[at, pl.ds(0, HALO)], ref[at, pl.ds(half - HALO, HALO)]
        )
    for group in range(2):
        out_ref[:, pl.ds(group * lines, lines)] = lines_ref[pl.ds(group * lines, lines), :].T[:8]


def edge(own, got, lines):
    vmem = pl.BlockSpec(memory_space=pltpu.VMEM)
    return pl.pallas_call(
        functools.partial(edge_kernel, lines),
        out_shape=pltpu.VMEM((8, 2 * lines), jnp.float32),
        in_specs=[vmem] * 2,
        out_specs=vmem,
        scratch_shapes=[pltpu.VMEM((2 * lines, 128), jnp.float32)],
        compiler_params=pltpu.CompilerParams(vmem_limit_bytes=VMEM_LIMIT),
        name="edge",
    )(own, got)


def combine_kernel(
    data_ref, own_ref, got_ref, spread_ref, cos_ref, sin_ref,
    out_ref,
    grid_ref, lines_ref, vm_ref,
):
    rows = data_ref.shape[0]
    lines = rows // 2
    local_lines, columns = own_ref.shape[0], own_ref.shape[1] - 128
    gy = lax.axis_index("gy")
    for group, data in ((gy, data_ref[...]), (1 - gy, got_ref[pl.ds(0, rows), :].astype(jnp.bfloat16))):
        made = lax.dot_general(data, spread_ref[...], NT, preferred_element_type=jnp.float32).astype(jnp.bfloat16)
        for component in range(2):
            place = pl.multiple_of((2 * component + group) * lines, 16)
            grid_ref[pl.ds(place, lines), :] = made[component * lines : (component + 1) * lines]

    lines_ref[...] = jnp.zeros_like(lines_ref)
    own_place, other_place = line_places(lines, local_lines)
    side = pl.ds(columns, HALO)
    lines_ref[own_place, pl.ds(0, columns)] = own_ref[:, pl.ds(0, columns)]
    lines_ref[own_place, side] = own_ref[:, side]
    lines_ref[other_place, pl.ds(0, columns)] = got_ref[pl.ds(rows, local_lines), :]
    lines_ref[other_place, side] = got_ref[pl.ds(rows + local_lines, local_lines), pl.ds(0, HALO)]
    for group in range(2):
        group_lines = pl.ds(group * lines, lines)
        inner = lines_ref[group_lines, pl.ds(columns, 128)].T[:HALO]
        vm_ref[pl.ds(0, HALO), group_lines] = jnp.where(gy == 0, 0.0, inner)
        vm_ref[pl.ds(HALO + columns, HALO), group_lines] = jnp.where(gy == 0, inner, 0.0)
    for first in range(0, columns, 128):
        for group in range(2):
            vm_ref[pl.ds(HALO + first, 128), pl.ds(group * lines, lines)] = lines_ref[
                pl.ds(group * lines, lines), pl.ds(first, 128)
            ].T

    for part, first, count in chunks(columns + 2 * HALO):
        made = pl.ds(first, max(16, count))
        total = lax.dot_general(
            cos_ref[made, :], grid_ref[pl.ds(0, 2 * lines), :], NT, preferred_element_type=jnp.float32
        ) + lax.dot_general(
            sin_ref[made, :], grid_ref[pl.ds(2 * lines, 2 * lines), :], NT, preferred_element_type=jnp.float32
        )
        put_windows(out_ref, first, count, vm_ref[pl.ds(first, count), :] - total[:count] * NX ** (-0.5))


def combine(data, own, got, spread, cosines, sines):
    lines = data.shape[0] // 2
    columns = own.shape[1] - 128
    dests = lax.axis_size("ang")
    vmem = pl.BlockSpec(memory_space=pltpu.VMEM)
    return pl.pallas_call(
        combine_kernel,
        out_shape=pltpu.VMEM((dests, columns // dests + 2 * HALO, 2 * lines), jnp.float32),
        in_specs=[vmem] * 6,
        out_specs=vmem,
        scratch_shapes=[
            pltpu.VMEM((4 * lines, spread.shape[0]), jnp.bfloat16),
            pltpu.VMEM((2 * lines, columns + 128), jnp.float32),
            pltpu.VMEM((columns + 2 * HALO, 2 * lines), jnp.float32),
        ],
        cost_estimate=pl.CostEstimate(flops=2 * 10**9, transcendentals=0, bytes_accessed=10**6),
        compiler_params=pltpu.CompilerParams(vmem_limit_bytes=VMEM_LIMIT),
        name="combine",
    )(data, own, got, spread, cosines, sines)


def join_kernel(parts_ref, edge_ref, out_ref):
    dests, window, _ = parts_ref.shape
    first = lax.axis_index("gy") == 0
    edge = edge_ref[...][:HALO]
    out_ref[0, pl.ds(0, HALO), :] = parts_ref[0, pl.ds(0, HALO), :] + jnp.where(first, edge, 0.0)
    last = pl.ds(window - HALO, HALO)
    out_ref[dests - 1, last, :] = parts_ref[dests - 1, last, :] + jnp.where(first, 0.0, edge)


def join(parts, got_edge):
    vmem = pl.BlockSpec(memory_space=pltpu.VMEM)
    return pl.pallas_call(
        join_kernel,
        out_shape=pltpu.VMEM(parts.shape, parts.dtype),
        in_specs=[vmem] * 2,
        out_specs=vmem,
        input_output_aliases={0: 0},
        compiler_params=pltpu.CompilerParams(vmem_limit_bytes=VMEM_LIMIT),
        name="join",
    )(parts, got_edge)


def on_chip(*arrays):
    return [pltpu.with_memory_space_constraint(array, pltpu.VMEM) for array in arrays]


def project_paired(data, offsets, view_index, taps, view_weight, volume, multiplier):
    lines = data.shape[0] // 2
    columns = volume.shape[1] // 2
    sent, data, offsets, view_index, taps, view_weight, own = pack(
        data, offsets, view_index, taps, view_weight, volume, multiplier
    )
    got = lax.ppermute(sent, "gy", [(0, 1), (1, 0)])
    spread, cosines, sines = tables(*on_chip(offsets, view_index, taps, view_weight), columns)
    own, got = on_chip(own, got)
    count = lax.axis_size("gx")
    route = []
    for low in range(count):
        pair = (count + low, (low + 1) % count)
        route += [pair, pair[::-1]]
    got_edge = lax.ppermute(edge(own, got, lines), ("gy", "gx"), route)
    data, spread, cosines, sines = on_chip(data, spread, cosines, sines)
    parts = combine(data, own, got, spread, cosines, sines)
    parts = join(*on_chip(parts, got_edge))
    return lax.all_to_all(parts, "ang", split_axis=0, concat_axis=0)


def per_device(spectrum_data, offsets, view_index, kernel, view_weight, volume, multiplier):
    local_planes, rows, columns = volume.shape
    planes = spectrum_data.shape[1]
    samples = spectrum_data.shape[3]
    dests = lax.axis_size("ang") * lax.axis_size("gy")
    local_lines = local_planes * rows
    lines = planes * rows

    volume = volume.reshape(local_lines, columns)
    multiplier = multiplier.reshape(local_lines, columns)
    arrays = (
        spectrum_data.reshape(2 * lines, samples),
        offsets.reshape(samples // 128, 128),
        view_index.reshape(samples // 128, 128),
        kernel,
        view_weight,
        volume,
        multiplier,
    )
    if lax.axis_size("gy") == 2 and columns // 2 == samples:
        parts = project_paired(*arrays)
    else:
        first_edge = volume[:, :HALO] + multiplier[:, :HALO]
        last_edge = volume[:, -HALO:] + multiplier[:, -HALO:]
        even = lax.axis_index("gx") % 2 == 0
        inner = exchanged(jnp.where(even, last_edge, first_edge), "gx", 0)
        outer = exchanged(jnp.where(even, first_edge, last_edge), "gx", 1)
        parts = close(project(*arrays, dests), *on_chip(inner, outer))
        parts = lax.all_to_all(parts, ("gy", "ang"), split_axis=0, concat_axis=0)
    done = smooth(*on_chip(parts), planes, local_lines, columns)
    done = lax.all_to_all(done, ("gy", "ang"), split_axis=0, concat_axis=0)
    return jnp.transpose(done, (1, 0, 2)).reshape(local_planes, rows, columns)


def solution(mesh):
    placed = (
        P(None, None, "gy", "ang"),
        P("ang"),
        P("ang"),
        P(None, "ang"),
        P(),
        P("ang", "gy", "gx"),
        P("ang", "gy", "gx"),
    )
    return jax.shard_map(
        per_device, mesh=mesh, in_specs=placed, out_specs=P("ang", "gy", "gx"), check_vma=False
    )
```

```python
import functools
import math

import jax
import jax.numpy as jnp
from jax import lax
from jax.experimental import pallas as pl
from jax.experimental.pallas import tpu as pltpu
from jax.sharding import PartitionSpec as P

NX = 4096
TV_STEPS = 4
HALO = TV_STEPS
CHUNK = 128
VMEM_LIMIT = 24 * 2**20

smooth_weight = 0.5
dual_step = 1.0 / 12.0

NT = (((1,), (1,)), ((), ()))


def unit_circle(phase):
    phase = phase & (NX - 1)
    quarter = (phase + NX // 8) // (NX // 4)
    angle = (phase - quarter * (NX // 4)).astype(jnp.float32) * (2.0 * math.pi / NX)
    square = angle * angle
    sine = angle * (1.0 + square * (-1.0 / 6 + square * (1.0 / 120 + square * (-1.0 / 5040 + square * (1.0 / 362880)))))
    cosine = 1.0 + square * (-0.5 + square * (1.0 / 24 + square * (-1.0 / 720 + square * (1.0 / 40320))))
    odd = (quarter & 1) == 1
    first = jnp.where(odd, -sine, cosine)
    second = jnp.where(odd, cosine, sine)
    flip = (quarter & 2) == 2
    return jnp.where(flip, -first, first), jnp.where(flip, -second, second)


def make_spread(offsets_ref, view_ref, taps_ref, weight_ref, spread_ref):
    block_size, samples = spread_ref.shape
    views = weight_ref.shape[0]
    pieces = []
    for piece in range(samples // 128):
        view = view_ref[pl.ds(piece, 1), :]
        found = jnp.zeros((1, 128), jnp.float32)
        lane = jnp.broadcast_to(view & 127, (8, 128))
        for first in range(0, views, 128):
            table = weight_ref[pl.ds(first, min(128, views - first))].reshape(1, -1)
            if views - first < 128:
                table = jnp.concatenate([table, jnp.zeros((1, 128 - (views - first)), jnp.float32)], axis=1)
            picked = jnp.take_along_axis(jnp.broadcast_to(table, (8, 128)), lane, axis=1)[:1]
            found = jnp.where(view // 128 == first // 128, picked, found)
        pieces.append(found)
    weight = jnp.concatenate(pieces, axis=1)
    values = [weight * taps_ref[pl.ds(tap, 1), :] for tap in range(taps_ref.shape[0])]
    offsets = jnp.concatenate([offsets_ref[pl.ds(piece, 1), :] for piece in range(samples // 128)], axis=1)

    rows = 16
    cell = lax.broadcasted_iota(jnp.int32, (rows, samples), 0)
    start = jnp.broadcast_to(offsets, (rows, samples))
    values = [jnp.broadcast_to(value, (rows, samples)) for value in values]
    for first in range(0, block_size, rows):
        tap = cell - (start - first)
        spread = jnp.zeros((rows, samples), jnp.float32)
        for index, value in enumerate(values):
            spread = jnp.where(tap == index, value, spread)
        spread_ref[pl.ds(first, rows), :] = spread.astype(jnp.bfloat16)


def make_angles(first_column, step_cos_ref, step_sin_ref, part_cos_ref, part_sin_ref):
    block_size = step_cos_ref.shape[1]
    freq = lax.axis_index("ang") * block_size + lax.broadcasted_iota(jnp.int32, (8, block_size), 1)
    row = lax.broadcasted_iota(jnp.int32, (8, block_size), 0)
    for first in range(0, CHUNK // 8, 8):
        step_cos_ref[pl.ds(first, 8), :], step_sin_ref[pl.ds(first, 8), :] = unit_circle(freq * (8 * (row + first)))
    for first in range(0, part_cos_ref.shape[0], 8):
        part_cos_ref[pl.ds(first, 8), :], part_sin_ref[pl.ds(first, 8), :] = unit_circle(
            freq * (CHUNK * (row + first))
        )
    return unit_circle(freq * (first_column + row))


def make_waves(base, part, count, step_cos_ref, step_sin_ref, part_cos_ref, part_sin_ref, put):
    base_cos, base_sin = base
    part_cos, part_sin = part_cos_ref[pl.ds(part, 1), :], part_sin_ref[pl.ds(part, 1), :]
    here_cos = base_cos * part_cos - base_sin * part_sin
    here_sin = base_sin * part_cos + base_cos * part_sin
    for step in range(0, pl.cdiv(count, 8), 2):
        pair_cos, pair_sin = [], []
        for one in (step, step + 1):
            step_cos, step_sin = step_cos_ref[pl.ds(one, 1), :], step_sin_ref[pl.ds(one, 1), :]
            pair_cos.append(here_cos * step_cos - here_sin * step_sin)
            pair_sin.append(-(here_sin * step_cos + here_cos * step_sin))
        put(
            8 * step,
            jnp.concatenate(pair_cos, axis=0).astype(jnp.bfloat16),
            jnp.concatenate(pair_sin, axis=0).astype(jnp.bfloat16),
        )


def chunks(total):
    return [(part, part * CHUNK, min(CHUNK, total - part * CHUNK)) for part in range(pl.cdiv(total, CHUNK))]


def put_windows(out_ref, first, count, sent):
    dests, window, _ = out_ref.shape
    block = window - 2 * HALO
    for dest in range(dests):
        low, high = max(first, dest * block), min(first + count, dest * block + window)
        if low < high:
            out_ref[dest, pl.ds(low - dest * block, high - low), :] = sent[low - first : high - first]


def project_kernel(
    data_ref, offsets_ref, view_ref, taps_ref, weight_ref, volume_ref, multiplier_ref,
    out_ref,
    spread_ref, grid_ref, cos_ref, sin_ref, step_cos_ref, step_sin_ref, part_cos_ref, part_sin_ref, lines_ref, vm_ref,
):
    ang, gx = lax.axis_index("ang"), lax.axis_index("gx")
    lines = data_ref.shape[0] // 2
    local_lines, columns = volume_ref.shape

    make_spread(offsets_ref, view_ref, taps_ref, weight_ref, spread_ref)
    grid_ref[...] = lax.dot_general(
        data_ref[...], spread_ref[...], NT, preferred_element_type=jnp.float32
    ).astype(jnp.bfloat16)

    lines_ref[...] = jnp.zeros_like(lines_ref)
    lines_ref[pl.ds(pl.multiple_of(ang * local_lines, 8), local_lines), :] = volume_ref[...] + multiplier_ref[...]
    vm_ref[pl.ds(0, HALO), :] = jnp.zeros((HALO, lines), jnp.float32)
    vm_ref[pl.ds(HALO + columns, HALO), :] = jnp.zeros((HALO, lines), jnp.float32)
    for first in range(0, columns, 128):
        vm_ref[pl.ds(HALO + first, 128), :] = lines_ref[:, pl.ds(first, 128)].T

    angles = (step_cos_ref, step_sin_ref, part_cos_ref, part_sin_ref)
    base = make_angles(gx * columns - HALO, *angles)
    for part, first, count in chunks(columns + 2 * HALO):
        slot = part % 2

        def put(at, cosines, sines):
            cos_ref[slot, pl.ds(at, 16), :] = cosines
            sin_ref[slot, pl.ds(at, 16), :] = sines

        make_waves(base, part, count, *angles, put)
        made = max(16, count)
        total_part = lax.dot_general(
            cos_ref[slot, pl.ds(0, made), :], grid_ref[pl.ds(0, lines), :], NT, preferred_element_type=jnp.float32
        ) + lax.dot_general(
            sin_ref[slot, pl.ds(0, made), :], grid_ref[pl.ds(lines, lines), :], NT, preferred_element_type=jnp.float32
        )
        put_windows(out_ref, first, count, vm_ref[pl.ds(first, count), :] - total_part[:count] * NX ** (-0.5))


def project(data, offsets, view_index, taps, view_weight, volume, multiplier, dests):
    lines = data.shape[0] // 2
    samples = data.shape[1]
    columns = volume.shape[1]
    block_size = NX // lax.axis_size("ang")
    window = columns // dests + 2 * HALO
    parts = pl.cdiv(columns + 2 * HALO, CHUNK)
    vmem = pl.BlockSpec(memory_space=pltpu.VMEM)
    return pl.pallas_call(
        project_kernel,
        out_shape=pltpu.VMEM((dests, window, lines), jnp.float32),
        in_specs=[vmem] * 7,
        out_specs=vmem,
        scratch_shapes=[
            pltpu.VMEM((block_size, samples), jnp.bfloat16),
            pltpu.VMEM((2 * lines, block_size), jnp.bfloat16),
            pltpu.VMEM((2, CHUNK, block_size), jnp.bfloat16),
            pltpu.VMEM((2, CHUNK, block_size), jnp.bfloat16),
            pltpu.VMEM((CHUNK // 8, block_size), jnp.float32),
            pltpu.VMEM((CHUNK // 8, block_size), jnp.float32),
            pltpu.VMEM((8 * pl.cdiv(parts, 8), block_size), jnp.float32),
            pltpu.VMEM((8 * pl.cdiv(parts, 8), block_size), jnp.float32),
            pltpu.VMEM((lines, columns), jnp.float32),
            pltpu.VMEM((columns + 2 * HALO, lines), jnp.float32),
        ],
        cost_estimate=pl.CostEstimate(flops=4 * 10**9, transcendentals=0, bytes_accessed=10**6),
        compiler_params=pltpu.CompilerParams(vmem_limit_bytes=VMEM_LIMIT),
        name="project",
    )(data, offsets, view_index, taps, view_weight, volume, multiplier)


def close_kernel(parts_ref, inner_ref, outer_ref, out_ref, halo_ref):
    ang = lax.axis_index("ang")
    even = lax.axis_index("gx") % 2 == 0
    dests, window, lines = parts_ref.shape
    local_lines = inner_ref.shape[0]
    halo_ref[...] = jnp.zeros_like(halo_ref)
    own = pl.ds(pl.multiple_of(ang * local_lines, 8), local_lines)
    inner, outer = inner_ref[...], outer_ref[...]
    halo_ref[own, pl.ds(0, HALO)] = jnp.where(even, outer, inner)
    halo_ref[own, pl.ds(HALO, HALO)] = jnp.where(even, inner, outer)
    edges = halo_ref[...].T
    out_ref[0, pl.ds(0, HALO), :] = parts_ref[0, pl.ds(0, HALO), :] + edges[:HALO]
    last = pl.ds(window - HALO, HALO)
    out_ref[dests - 1, last, :] = parts_ref[dests - 1, last, :] + edges[HALO : 2 * HALO]


def close(parts, inner, outer):
    vmem = pl.BlockSpec(memory_space=pltpu.VMEM)
    return pl.pallas_call(
        close_kernel,
        out_shape=pltpu.VMEM(parts.shape, parts.dtype),
        in_specs=[vmem] * 3,
        out_specs=vmem,
        scratch_shapes=[pltpu.VMEM((parts.shape[2], 128), jnp.float32)],
        input_output_aliases={0: 0},
        compiler_params=pltpu.CompilerParams(vmem_limit_bytes=VMEM_LIMIT),
        name="close",
    )(parts, inner, outer)


def smooth_kernel(planes, columns, *refs):
    *parts_refs, out_ref = refs
    dests, local_lines, block = out_ref.shape
    window = parts_refs[0].shape[-2]
    angs, groups = lax.axis_size("ang"), lax.axis_size("gy")
    lines = angs * local_lines
    rows = lines // planes
    lane = lax.broadcasted_iota(jnp.int32, (window, lines), 1)
    lane_row = lane % rows
    place = lax.axis_index("gy") * angs + lax.axis_index("ang")
    column = lax.axis_index("gx") * columns + place * block - HALO + lax.broadcasted_iota(jnp.int32, (window, lines), 0)
    plane_open = lane // rows < planes - 1
    row_first = lane_row == 0
    row_last = lane_row == rows - 1
    cell_open = (column >= 0) & (column < NX - 1)
    zero = jnp.float32(0.0)

    source = []
    for group in range(groups):
        total = None
        for ang in range(angs):
            if len(parts_refs) > 1:
                part = parts_refs[ang][:, pl.ds(group * lines, lines)]
            else:
                part = parts_refs[0][group * angs + ang]
            total = part if total is None else total + part
        source.append(total)
    scaled = [value / smooth_weight for value in source]

    def down(values):
        lower = []
        for group in range(groups):
            previous = values[group - 1]
            lower.append(
                jnp.where(
                    row_first, pltpu.roll(previous, lines - (rows - 1), 1), pltpu.roll(values[group], 1, 1)
                )
            )
        return lower

    flow = None
    for repeat in range(TV_STEPS + 1):
        if flow is None:
            target = [-value for value in scaled]
        else:
            lower_row = down([f[1] for f in flow])
            local_div = []
            for group in range(groups):
                f0, f1, f2 = flow[group]
                plane_part = f0 - pltpu.roll(f0, rows, 1)
                row_part = f1 - lower_row[group]
                cell_part = f2 - pltpu.roll(f2, 1, 0)
                local_div.append(plane_part + row_part + cell_part)
            if repeat == TV_STEPS:
                for group in range(groups):
                    done = source[group] - smooth_weight * local_div[group]
                    turned = done[HALO : HALO + block].T
                    for ang in range(angs):
                        out_ref[group * angs + ang] = turned[ang * local_lines : (ang + 1) * local_lines]
                return
            target = [local_div[group] - scaled[group] for group in range(groups)]
        updated = []
        for group in range(groups):
            here = target[group]
            slope_plane = jnp.where(plane_open, pltpu.roll(here, lines - rows, 1) - here, zero)
            if group + 1 < groups:
                upper = jnp.where(
                    row_last, pltpu.roll(target[group + 1], rows - 1, 1), pltpu.roll(here, lines - 1, 1)
                )
                slope_row = upper - here
            else:
                slope_row = jnp.where(row_last, zero, pltpu.roll(here, lines - 1, 1) - here)
            slope_cell = jnp.where(cell_open, pltpu.roll(here, window - 1, 0) - here, zero)
            slope_norm = jnp.sqrt(slope_plane * slope_plane + slope_row * slope_row + slope_cell * slope_cell)
            scale = 1.0 / (1.0 + dual_step * slope_norm)
            moved = [dual_step * slope_plane, dual_step * slope_row, dual_step * slope_cell]
            if flow is not None:
                moved = [f + m for f, m in zip(flow[group], moved)]
            updated.append([m * scale for m in moved])
        flow = updated


def smooth(parts, planes, local_lines, columns):
    window = parts[0].shape[-2]
    dests = lax.axis_size("ang") * lax.axis_size("gy")
    vmem = pl.BlockSpec(memory_space=pltpu.VMEM)
    return pl.pallas_call(
        functools.partial(smooth_kernel, planes, columns),
        out_shape=pltpu.VMEM((dests, local_lines, window - 2 * HALO), jnp.float32),
        in_specs=[vmem] * len(parts),
        out_specs=vmem,
        compiler_params=pltpu.CompilerParams(vmem_limit_bytes=VMEM_LIMIT),
        name="smooth",
    )(*parts)


def exchanged(block, axis, shift):
    count = lax.axis_size(axis)
    route = []
    for low in range(shift, count + shift - 1, 2):
        pair = (low % count, (low + 1) % count)
        route += [pair, pair[::-1]]
    return lax.ppermute(block, axis, route)


def pack_kernel(
    data_ref, offsets_ref, view_ref, taps_ref, weight_ref, volume_ref, multiplier_ref,
    sent_ref, data_out, offsets_out, view_out, taps_out, weight_out, own_ref,
    volume_here, multiplier_here, sems,
):
    rows = data_ref.shape[0]
    half = volume_ref.shape[1] // 2
    first = lax.axis_index("gy") == 0
    pairs = (
        (data_ref, data_out),
        (volume_ref, volume_here),
        (multiplier_ref, multiplier_here),
        (offsets_ref, offsets_out),
        (view_ref, view_out),
        (taps_ref, taps_out),
        (weight_ref, weight_out),
    )
    copies = [pltpu.make_async_copy(source, target, sems.at[at]) for at, (source, target) in enumerate(pairs)]
    for copy in copies:
        copy.start()
    copies[0].wait()
    sent_ref[pl.ds(0, rows), :] = data_out[...].astype(jnp.float32)
    copies[1].wait()
    copies[2].wait()
    low = volume_here[:, pl.ds(0, half)] + multiplier_here[:, pl.ds(0, half)]
    high = volume_here[:, pl.ds(half, half)] + multiplier_here[:, pl.ds(half, half)]
    below, above = low[:, half - HALO :], high[:, :HALO]
    local_lines = low.shape[0]
    own_ref[:, pl.ds(0, half)] = jnp.where(first, low, high)
    own_ref[:, pl.ds(half, HALO)] = jnp.where(first, above, below)
    sent_ref[pl.ds(rows, local_lines), :] = jnp.where(first, high, low)
    sent_ref[pl.ds(rows + local_lines, local_lines), pl.ds(0, HALO)] = jnp.where(first, below, above)
    for copy in copies[3:]:
        copy.wait()


def pack(data, offsets, view_index, taps, view_weight, volume, multiplier):
    rows, samples = data.shape
    local_lines, columns = volume.shape
    vmem = pl.BlockSpec(memory_space=pltpu.VMEM)
    return pl.pallas_call(
        pack_kernel,
        out_shape=[
            pltpu.VMEM((rows + 2 * local_lines, samples), jnp.float32),
            pltpu.VMEM(data.shape, data.dtype),
            pltpu.VMEM(offsets.shape, offsets.dtype),
            pltpu.VMEM(view_index.shape, view_index.dtype),
            pltpu.VMEM(taps.shape, taps.dtype),
            pltpu.VMEM(view_weight.shape, view_weight.dtype),
            pltpu.VMEM((local_lines, columns // 2 + 128), jnp.float32),
        ],
        in_specs=[pl.BlockSpec(memory_space=pltpu.HBM)] * 7,
        out_specs=[vmem] * 7,
        scratch_shapes=[
            pltpu.VMEM(volume.shape, volume.dtype),
            pltpu.VMEM(multiplier.shape, multiplier.dtype),
            pltpu.SemaphoreType.DMA((7,)),
        ],
        compiler_params=pltpu.CompilerParams(vmem_limit_bytes=VMEM_LIMIT),
        name="pack",
    )(
        *(
            pltpu.with_memory_space_constraint(array, pltpu.HBM)
            for array in (data, offsets, view_index, taps, view_weight, volume, multiplier)
        )
    )


def tables_kernel(
    columns, offsets_ref, view_ref, taps_ref, weight_ref,
    spread_ref, wave_ref,
    step_cos_ref, step_sin_ref, part_cos_ref, part_sin_ref,
):
    block_size = spread_ref.shape[0]
    make_spread(offsets_ref, view_ref, taps_ref, weight_ref, spread_ref)
    angles = (step_cos_ref, step_sin_ref, part_cos_ref, part_sin_ref)
    base = make_angles(lax.axis_index("gx") * 2 * columns + lax.axis_index("gy") * columns - HALO, *angles)
    for part, first, count in chunks(columns + 2 * HALO):

        def put(at, cosines, sines):
            wave_ref[pl.ds(first + at, 16), pl.ds(0, block_size)] = cosines
            wave_ref[pl.ds(first + at, 16), pl.ds(block_size, block_size)] = sines

        make_waves(base, part, count, *angles, put)


def tables(offsets, view_index, taps, view_weight, columns):
    samples = taps.shape[1]
    block_size = NX // lax.axis_size("ang")
    made = 16 * pl.cdiv(columns + 2 * HALO, 16)
    parts = 8 * pl.cdiv(pl.cdiv(columns + 2 * HALO, CHUNK), 8)
    vmem = pl.BlockSpec(memory_space=pltpu.VMEM)
    return pl.pallas_call(
        functools.partial(tables_kernel, columns),
        out_shape=[
            pltpu.VMEM((block_size, samples), jnp.bfloat16),
            pltpu.VMEM((made, 2 * block_size), jnp.bfloat16),
        ],
        in_specs=[vmem] * 4,
        out_specs=[vmem] * 2,
        scratch_shapes=[
            pltpu.VMEM((CHUNK // 8, block_size), jnp.float32),
            pltpu.VMEM((CHUNK // 8, block_size), jnp.float32),
            pltpu.VMEM((parts, block_size), jnp.float32),
            pltpu.VMEM((parts, block_size), jnp.float32),
        ],
        cost_estimate=pl.CostEstimate(flops=2 * 10**9, transcendentals=0, bytes_accessed=10**6),
        compiler_params=pltpu.CompilerParams(vmem_limit_bytes=VMEM_LIMIT),
        name="tables",
    )(offsets, view_index, taps, view_weight)


def line_places(lines, local_lines):
    gy, inner = lax.axis_index("gy"), lax.axis_index("ang") * local_lines
    return [
        pl.ds(pl.multiple_of(group * lines + inner, 8), local_lines) for group in (gy, 1 - gy)
    ]


def edge_kernel(lines, own_ref, got_ref, out_ref, lines_ref):
    local_lines, half = own_ref.shape[0], own_ref.shape[1] - 128
    rows = got_ref.shape[0] - 2 * local_lines
    first = lax.axis_index("gy") == 0
    lines_ref[...] = jnp.zeros_like(lines_ref)
    own_place, other_place = line_places(lines, local_lines)
    other = pl.ds(rows, local_lines)
    for place, ref, at in ((own_place, own_ref, pl.ds(0, local_lines)), (other_place, got_ref, other)):
        lines_ref[place, pl.ds(0, HALO)] = jnp.where(
            first, ref[at, pl.ds(0, HALO)], ref[at, pl.ds(half - HALO, HALO)]
        )
    for group in range(2):
        out_ref[:, pl.ds(group * lines, lines)] = lines_ref[pl.ds(group * lines, lines), :].T[:8]


def edge(own, got, lines):
    vmem = pl.BlockSpec(memory_space=pltpu.VMEM)
    return pl.pallas_call(
        functools.partial(edge_kernel, lines),
        out_shape=pltpu.VMEM((8, 2 * lines), jnp.float32),
        in_specs=[vmem] * 2,
        out_specs=vmem,
        scratch_shapes=[pltpu.VMEM((2 * lines, 128), jnp.float32)],
        compiler_params=pltpu.CompilerParams(vmem_limit_bytes=VMEM_LIMIT),
        name="edge",
    )(own, got)


def grid_kernel(data_ref, own_ref, got_ref, spread_ref, grid_ref, vm_ref, both_ref, lines_ref):
    rows = data_ref.shape[0]
    lines = rows // 2
    block_size = spread_ref.shape[0]
    local_lines, columns = own_ref.shape[0], own_ref.shape[1] - 128
    gy = lax.axis_index("gy")
    for component in range(2):
        for group, ref in ((gy, data_ref), (1 - gy, got_ref)):
            place = pl.multiple_of((2 * component + group) * lines, 16)
            both_ref[pl.ds(place, lines), :] = ref[pl.ds(component * lines, lines), :].astype(jnp.bfloat16)
    for component in range(2):
        grid_ref[pl.ds(component * block_size, block_size), :] = lax.dot_general(
            spread_ref[...],
            both_ref[pl.ds(2 * component * lines, 2 * lines), :],
            NT,
            preferred_element_type=jnp.float32,
        ).astype(jnp.bfloat16)

    lines_ref[...] = jnp.zeros_like(lines_ref)
    own_place, other_place = line_places(lines, local_lines)
    side = pl.ds(columns, HALO)
    lines_ref[own_place, pl.ds(0, columns)] = own_ref[:, pl.ds(0, columns)]
    lines_ref[own_place, side] = own_ref[:, side]
    lines_ref[other_place, pl.ds(0, columns)] = got_ref[pl.ds(rows, local_lines), :]
    lines_ref[other_place, side] = got_ref[pl.ds(rows + local_lines, local_lines), pl.ds(0, HALO)]
    for group in range(2):
        group_lines = pl.ds(group * lines, lines)
        inner = lines_ref[group_lines, pl.ds(columns, 128)].T[:HALO]
        vm_ref[pl.ds(0, HALO), group_lines] = jnp.where(gy == 0, 0.0, inner)
        vm_ref[pl.ds(HALO + columns, HALO), group_lines] = jnp.where(gy == 0, inner, 0.0)
        for first in range(0, columns, 128):
            vm_ref[pl.ds(HALO + first, 128), group_lines] = lines_ref[group_lines, pl.ds(first, 128)].T


def grid(data, own, got, spread):
    lines = data.shape[0] // 2
    columns = own.shape[1] - 128
    vmem = pl.BlockSpec(memory_space=pltpu.VMEM)
    return pl.pallas_call(
        grid_kernel,
        out_shape=[
            pltpu.VMEM((2 * spread.shape[0], 2 * lines), jnp.bfloat16),
            pltpu.VMEM((columns + 2 * HALO, 2 * lines), jnp.float32),
        ],
        in_specs=[vmem] * 4,
        out_specs=[vmem] * 2,
        scratch_shapes=[
            pltpu.VMEM((4 * lines, data.shape[1]), jnp.bfloat16),
            pltpu.VMEM((2 * lines, columns + 128), jnp.float32),
        ],
        cost_estimate=pl.CostEstimate(flops=10**9, transcendentals=0, bytes_accessed=10**6),
        compiler_params=pltpu.CompilerParams(vmem_limit_bytes=VMEM_LIMIT),
        name="grid",
    )(data, own, got, spread)


def block_kernel(apart, wave_ref, grid_ref, vm_ref, edge_ref, out_ref):
    window = out_ref.shape[0]
    block = window - 2 * HALO
    angs = lax.axis_size("ang")
    dest = lax.axis_index("ang") ^ apart
    gy = lax.axis_index("gy")
    first = pl.multiple_of(dest * block, 16)
    made = 16 * pl.cdiv(window, 16)
    total = jnp.dot(wave_ref[pl.ds(first, made), :], grid_ref[...], preferred_element_type=jnp.float32)
    out_ref[...] = vm_ref[pl.ds(first, window), :] - total[:window] * NX ** (-0.5)
    edge = edge_ref[...][:HALO]
    opens = jnp.logical_and(dest == 0, gy == 0)
    out_ref[pl.ds(0, HALO), :] += jnp.where(opens, edge, 0.0)
    closes = jnp.logical_and(dest == angs - 1, gy == 1)
    out_ref[pl.ds(window - HALO, HALO), :] += jnp.where(closes, edge, 0.0)


def block_of(apart, wave, grid, vm, got_edge):
    window = (vm.shape[0] - 2 * HALO) // lax.axis_size("ang") + 2 * HALO
    vmem = pl.BlockSpec(memory_space=pltpu.VMEM)
    return pl.pallas_call(
        functools.partial(block_kernel, apart),
        out_shape=pltpu.VMEM((window, vm.shape[1]), jnp.float32),
        in_specs=[vmem] * 4,
        out_specs=vmem,
        cost_estimate=pl.CostEstimate(flops=10**9, transcendentals=0, bytes_accessed=10**6),
        compiler_params=pltpu.CompilerParams(vmem_limit_bytes=VMEM_LIMIT),
        name=f"block{apart}",
    )(wave, grid, vm, got_edge)


def on_chip(*arrays):
    return [pltpu.with_memory_space_constraint(array, pltpu.VMEM) for array in arrays]


def project_paired(data, offsets, view_index, taps, view_weight, volume, multiplier):
    lines = data.shape[0] // 2
    columns = volume.shape[1] // 2
    sent, data, offsets, view_index, taps, view_weight, own = pack(
        data, offsets, view_index, taps, view_weight, volume, multiplier
    )
    got = lax.ppermute(sent, "gy", [(0, 1), (1, 0)])
    spread, wave = tables(*on_chip(offsets, view_index, taps, view_weight), columns)
    own, got = on_chip(own, got)
    count = lax.axis_size("gx")
    route = []
    for low in range(count):
        pair = (count + low, (low + 1) % count)
        route += [pair, pair[::-1]]
    got_edge = lax.ppermute(edge(own, got, lines), ("gy", "gx"), route)
    gridded, vm = grid(*on_chip(data, own, got, spread))
    wave, gridded, vm, got_edge = on_chip(wave, gridded, vm, got_edge)
    angs = lax.axis_size("ang")
    parts = []
    for apart in range(angs - 1, 0, -1):
        part = block_of(apart, wave, gridded, vm, got_edge)
        parts.append(lax.ppermute(part, "ang", [(ang, ang ^ apart) for ang in range(angs)]))
    return [block_of(0, wave, gridded, vm, got_edge)] + parts


def per_device(spectrum_data, offsets, view_index, kernel, view_weight, volume, multiplier):
    local_planes, rows, columns = volume.shape
    planes = spectrum_data.shape[1]
    samples = spectrum_data.shape[3]
    dests = lax.axis_size("ang") * lax.axis_size("gy")
    local_lines = local_planes * rows
    lines = planes * rows

    volume = volume.reshape(local_lines, columns)
    multiplier = multiplier.reshape(local_lines, columns)
    arrays = (
        spectrum_data.reshape(2 * lines, samples),
        offsets.reshape(samples // 128, 128),
        view_index.reshape(samples // 128, 128),
        kernel,
        view_weight,
        volume,
        multiplier,
    )
    angs = lax.axis_size("ang")
    if lax.axis_size("gy") == 2 and columns // 2 == samples and angs & (angs - 1) == 0:
        parts = project_paired(*arrays)
    else:
        first_edge = volume[:, :HALO] + multiplier[:, :HALO]
        last_edge = volume[:, -HALO:] + multiplier[:, -HALO:]
        even = lax.axis_index("gx") % 2 == 0
        inner = exchanged(jnp.where(even, last_edge, first_edge), "gx", 0)
        outer = exchanged(jnp.where(even, first_edge, last_edge), "gx", 1)
        parts = close(project(*arrays, dests), *on_chip(inner, outer))
        parts = [lax.all_to_all(parts, ("gy", "ang"), split_axis=0, concat_axis=0)]
    done = smooth(on_chip(*parts), planes, local_lines, columns)
    done = lax.all_to_all(done, ("gy", "ang"), split_axis=0, concat_axis=0)
    return jnp.transpose(done, (1, 0, 2)).reshape(local_planes, rows, columns)


def solution(mesh):
    placed = (
        P(None, None, "gy", "ang"),
        P("ang"),
        P("ang"),
        P(None, "ang"),
        P(),
        P("ang", "gy", "gx"),
        P("ang", "gy", "gx"),
    )
    return jax.shard_map(
        per_device, mesh=mesh, in_specs=placed, out_specs=P("ang", "gy", "gx"), check_vma=False
    )
```

```python
import functools
import math

import jax
import jax.numpy as jnp
from jax import lax
from jax.experimental import pallas as pl
from jax.experimental.pallas import tpu as pltpu
from jax.sharding import PartitionSpec as P


NX = 4096
TV_STEPS = 4
HALO = TV_STEPS
CHUNK = 128
VMEM_LIMIT = 24 * 2**20

smooth_weight = 0.5
dual_step = 1.0 / 12.0

NT = (((1,), (1,)), ((), ()))


def unit_circle(phase):
    phase = phase & (NX - 1)
    quarter = (phase + NX // 8) // (NX // 4)
    angle = (phase - quarter * (NX // 4)).astype(jnp.float32) * (2.0 * math.pi / NX)
    square = angle * angle
    sine = angle * (1.0 + square * (-1.0 / 6 + square * (1.0 / 120 + square * (-1.0 / 5040 + square * (1.0 / 362880)))))
    cosine = 1.0 + square * (-0.5 + square * (1.0 / 24 + square * (-1.0 / 720 + square * (1.0 / 40320))))
    odd = (quarter & 1) == 1
    first = jnp.where(odd, -sine, cosine)
    second = jnp.where(odd, cosine, sine)
    flip = (quarter & 2) == 2
    return jnp.where(flip, -first, first), jnp.where(flip, -second, second)


def make_spread(offsets_ref, view_ref, taps_ref, weight_ref, spread_ref):
    block_size, samples = spread_ref.shape
    views = weight_ref.shape[0]
    pieces = []
    for piece in range(samples // 128):
        view = view_ref[pl.ds(piece, 1), :]
        found = jnp.zeros((1, 128), jnp.float32)
        lane = jnp.broadcast_to(view & 127, (8, 128))
        for first in range(0, views, 128):
            table = weight_ref[pl.ds(first, min(128, views - first))].reshape(1, -1)
            if views - first < 128:
                table = jnp.concatenate([table, jnp.zeros((1, 128 - (views - first)), jnp.float32)], axis=1)
            picked = jnp.take_along_axis(jnp.broadcast_to(table, (8, 128)), lane, axis=1)[:1]
            found = jnp.where(view // 128 == first // 128, picked, found)
        pieces.append(found)
    weight = jnp.concatenate(pieces, axis=1)
    values = [weight * taps_ref[pl.ds(tap, 1), :] for tap in range(taps_ref.shape[0])]
    offsets = jnp.concatenate([offsets_ref[pl.ds(piece, 1), :] for piece in range(samples // 128)], axis=1)

    rows = 16
    cell = lax.broadcasted_iota(jnp.int32, (rows, samples), 0)
    starts = [jnp.broadcast_to(offsets + index, (rows, samples)) for index in range(len(values))]
    values = [jnp.broadcast_to(value, (rows, samples)) for value in values]
    for first in range(0, block_size, rows):
        here = cell + first
        spread = jnp.zeros((rows, samples), jnp.float32)
        for start, value in zip(starts, values):
            spread = jnp.where(here == start, value, spread)
        spread_ref[pl.ds(first, rows), :] = spread.astype(jnp.bfloat16)


def make_angles(first_column, step_cos_ref, step_sin_ref, part_cos_ref, part_sin_ref):
    block_size = step_cos_ref.shape[1]
    freq = lax.axis_index("ang") * block_size + lax.broadcasted_iota(jnp.int32, (8, block_size), 1)
    row = lax.broadcasted_iota(jnp.int32, (8, block_size), 0)
    for first in range(0, CHUNK // 8, 8):
        step_cos_ref[pl.ds(first, 8), :], step_sin_ref[pl.ds(first, 8), :] = unit_circle(-freq * (8 * (row + first)))
    for first in range(0, part_cos_ref.shape[0], 8):
        part_cos_ref[pl.ds(first, 8), :], part_sin_ref[pl.ds(first, 8), :] = unit_circle(
            -freq * (CHUNK * (row + first))
        )
    return unit_circle(-freq * (first_column + row))


def make_waves(base, part, count, step_cos_ref, step_sin_ref, part_cos_ref, part_sin_ref, put):
    base_cos, base_sin = base
    part_cos, part_sin = part_cos_ref[pl.ds(part, 1), :], part_sin_ref[pl.ds(part, 1), :]
    here_cos = base_cos * part_cos - base_sin * part_sin
    here_sin = base_sin * part_cos + base_cos * part_sin
    for step in range(0, pl.cdiv(count, 8), 2):
        pair_cos, pair_sin = [], []
        for one in (step, step + 1):
            step_cos, step_sin = step_cos_ref[pl.ds(one, 1), :], step_sin_ref[pl.ds(one, 1), :]
            pair_cos.append(here_cos * step_cos - here_sin * step_sin)
            pair_sin.append(here_sin * step_cos + here_cos * step_sin)
        put(
            8 * step,
            jnp.concatenate(pair_cos, axis=0).astype(jnp.bfloat16),
            jnp.concatenate(pair_sin, axis=0).astype(jnp.bfloat16),
        )


def chunks(total):
    return [(part, part * CHUNK, min(CHUNK, total - part * CHUNK)) for part in range(pl.cdiv(total, CHUNK))]


def put_windows(out_ref, first, count, sent):
    dests, window, _ = out_ref.shape
    block = window - 2 * HALO
    for dest in range(dests):
        low, high = max(first, dest * block), min(first + count, dest * block + window)
        if low < high:
            out_ref[dest, pl.ds(low - dest * block, high - low), :] = sent[low - first : high - first]


def project_kernel(
    data_ref, offsets_ref, view_ref, taps_ref, weight_ref, volume_ref, multiplier_ref,
    out_ref,
    spread_ref, grid_ref, cos_ref, sin_ref, step_cos_ref, step_sin_ref, part_cos_ref, part_sin_ref, lines_ref, vm_ref,
):
    ang, gx = lax.axis_index("ang"), lax.axis_index("gx")
    lines = data_ref.shape[0] // 2
    local_lines, columns = volume_ref.shape

    make_spread(offsets_ref, view_ref, taps_ref, weight_ref, spread_ref)
    grid_ref[...] = lax.dot_general(
        data_ref[...], spread_ref[...], NT, preferred_element_type=jnp.float32
    ).astype(jnp.bfloat16)

    lines_ref[...] = jnp.zeros_like(lines_ref)
    lines_ref[pl.ds(pl.multiple_of(ang * local_lines, 8), local_lines), :] = volume_ref[...] + multiplier_ref[...]
    vm_ref[pl.ds(0, HALO), :] = jnp.zeros((HALO, lines), jnp.float32)
    vm_ref[pl.ds(HALO + columns, HALO), :] = jnp.zeros((HALO, lines), jnp.float32)
    for first in range(0, columns, 128):
        vm_ref[pl.ds(HALO + first, 128), :] = lines_ref[:, pl.ds(first, 128)].T

    angles = (step_cos_ref, step_sin_ref, part_cos_ref, part_sin_ref)
    base = make_angles(gx * columns - HALO, *angles)
    for part, first, count in chunks(columns + 2 * HALO):
        slot = part % 2

        def put(at, cosines, sines):
            cos_ref[slot, pl.ds(at, 16), :] = cosines
            sin_ref[slot, pl.ds(at, 16), :] = sines

        make_waves(base, part, count, *angles, put)
        made = max(16, count)
        total_part = lax.dot_general(
            cos_ref[slot, pl.ds(0, made), :], grid_ref[pl.ds(0, lines), :], NT, preferred_element_type=jnp.float32
        ) + lax.dot_general(
            sin_ref[slot, pl.ds(0, made), :], grid_ref[pl.ds(lines, lines), :], NT, preferred_element_type=jnp.float32
        )
        put_windows(out_ref, first, count, vm_ref[pl.ds(first, count), :] - total_part[:count] * NX ** (-0.5))


def project(data, offsets, view_index, taps, view_weight, volume, multiplier, dests):
    lines = data.shape[0] // 2
    samples = data.shape[1]
    columns = volume.shape[1]
    block_size = NX // lax.axis_size("ang")
    window = columns // dests + 2 * HALO
    parts = pl.cdiv(columns + 2 * HALO, CHUNK)
    vmem = pl.BlockSpec(memory_space=pltpu.VMEM)
    return pl.pallas_call(
        project_kernel,
        out_shape=pltpu.VMEM((dests, window, lines), jnp.float32),
        in_specs=[vmem] * 7,
        out_specs=vmem,
        scratch_shapes=[
            pltpu.VMEM((block_size, samples), jnp.bfloat16),
            pltpu.VMEM((2 * lines, block_size), jnp.bfloat16),
            pltpu.VMEM((2, CHUNK, block_size), jnp.bfloat16),
            pltpu.VMEM((2, CHUNK, block_size), jnp.bfloat16),
            pltpu.VMEM((CHUNK // 8, block_size), jnp.float32),
            pltpu.VMEM((CHUNK // 8, block_size), jnp.float32),
            pltpu.VMEM((8 * pl.cdiv(parts, 8), block_size), jnp.float32),
            pltpu.VMEM((8 * pl.cdiv(parts, 8), block_size), jnp.float32),
            pltpu.VMEM((lines, columns), jnp.float32),
            pltpu.VMEM((columns + 2 * HALO, lines), jnp.float32),
        ],
        cost_estimate=pl.CostEstimate(flops=4 * 10**9, transcendentals=0, bytes_accessed=10**6),
        compiler_params=pltpu.CompilerParams(vmem_limit_bytes=VMEM_LIMIT),
        name="project",
    )(data, offsets, view_index, taps, view_weight, volume, multiplier)


def close_kernel(parts_ref, inner_ref, outer_ref, out_ref, halo_ref):
    ang = lax.axis_index("ang")
    even = lax.axis_index("gx") % 2 == 0
    dests, window, _ = parts_ref.shape
    local_lines = inner_ref.shape[0]
    halo_ref[...] = jnp.zeros_like(halo_ref)
    own = pl.ds(pl.multiple_of(ang * local_lines, 8), local_lines)
    inner, outer = inner_ref[...], outer_ref[...]
    halo_ref[own, pl.ds(0, HALO)] = jnp.where(even, outer, inner)
    halo_ref[own, pl.ds(HALO, HALO)] = jnp.where(even, inner, outer)
    edges = halo_ref[...].T
    out_ref[0, pl.ds(0, HALO), :] = parts_ref[0, pl.ds(0, HALO), :] + edges[:HALO]
    last = pl.ds(window - HALO, HALO)
    out_ref[dests - 1, last, :] = parts_ref[dests - 1, last, :] + edges[HALO : 2 * HALO]


def close(parts, inner, outer):
    vmem = pl.BlockSpec(memory_space=pltpu.VMEM)
    return pl.pallas_call(
        close_kernel,
        out_shape=pltpu.VMEM(parts.shape, parts.dtype),
        in_specs=[vmem] * 3,
        out_specs=vmem,
        scratch_shapes=[pltpu.VMEM((parts.shape[2], 128), jnp.float32)],
        input_output_aliases={0: 0},
        compiler_params=pltpu.CompilerParams(vmem_limit_bytes=VMEM_LIMIT),
        name="close",
    )(parts, inner, outer)


def smooth_kernel(planes, columns, *refs):
    *parts_refs, out_ref = refs
    _, local_lines, block = out_ref.shape
    window = parts_refs[0].shape[-2]
    angs, groups = lax.axis_size("ang"), lax.axis_size("gy")
    lines = angs * local_lines
    rows = lines // planes
    lane = lax.broadcasted_iota(jnp.int32, (window, lines), 1)
    lane_row = lane % rows
    place = lax.axis_index("gy") * angs + lax.axis_index("ang")
    column = lax.axis_index("gx") * columns + place * block - HALO + lax.broadcasted_iota(jnp.int32, (window, lines), 0)
    plane_open = lane // rows < planes - 1
    row_first = lane_row == 0
    row_last = lane_row == rows - 1
    cell_open = (column >= 0) & (column < NX - 1)
    zero = jnp.float32(0.0)

    source = []
    for group in range(groups):
        total = None
        for ang in range(angs):
            if len(parts_refs) > 1:
                part = parts_refs[ang][:, pl.ds(group * lines, lines)]
            else:
                part = parts_refs[0][group * angs + ang]
            total = part if total is None else total + part
        source.append(total)
    scaled = [value * (dual_step / smooth_weight) for value in source]

    def down(values):
        lower = []
        for group in range(groups):
            previous = values[group - 1]
            lower.append(
                jnp.where(
                    row_first, pltpu.roll(previous, lines - (rows - 1), 1), pltpu.roll(values[group], 1, 1)
                )
            )
        return lower

    flow = None
    for repeat in range(TV_STEPS + 1):
        if flow is None:
            target = [-value for value in scaled]
        else:
            lower_row = down([f[1] for f in flow])
            local_div = []
            for group in range(groups):
                f0, f1, f2 = flow[group]
                plane_part = f0 - pltpu.roll(f0, rows, 1)
                row_part = f1 - lower_row[group]
                cell_part = f2 - pltpu.roll(f2, 1, 0)
                local_div.append(plane_part + row_part + cell_part)
            if repeat == TV_STEPS:
                for group in range(groups):
                    done = source[group] - smooth_weight * local_div[group]
                    turned = done[HALO : HALO + block].T
                    for ang in range(angs):
                        out_ref[group * angs + ang] = turned[ang * local_lines : (ang + 1) * local_lines]
                return
            target = [dual_step * local_div[group] - scaled[group] for group in range(groups)]
        updated = []
        for group in range(groups):
            here = target[group]
            slope_plane = jnp.where(plane_open, pltpu.roll(here, lines - rows, 1) - here, zero)
            if group + 1 < groups:
                upper = jnp.where(
                    row_last, pltpu.roll(target[group + 1], rows - 1, 1), pltpu.roll(here, lines - 1, 1)
                )
                slope_row = upper - here
            else:
                slope_row = jnp.where(row_last, zero, pltpu.roll(here, lines - 1, 1) - here)
            slope_cell = jnp.where(cell_open, pltpu.roll(here, window - 1, 0) - here, zero)
            square = slope_plane * slope_plane + slope_row * slope_row + slope_cell * slope_cell
            scale = 1.0 / (1.0 + square * lax.rsqrt(jnp.maximum(square, 1e-30)))
            moved = [slope_plane, slope_row, slope_cell]
            if flow is not None:
                moved = [f + m for f, m in zip(flow[group], moved)]
            updated.append([m * scale for m in moved])
        flow = updated


def smooth(parts, planes, local_lines, columns):
    window = parts[0].shape[-2]
    dests = lax.axis_size("ang") * lax.axis_size("gy")
    vmem = pl.BlockSpec(memory_space=pltpu.VMEM)
    return pl.pallas_call(
        functools.partial(smooth_kernel, planes, columns),
        out_shape=pltpu.VMEM((dests, local_lines, window - 2 * HALO), jnp.float32),
        in_specs=[vmem] * len(parts),
        out_specs=vmem,
        compiler_params=pltpu.CompilerParams(vmem_limit_bytes=VMEM_LIMIT),
        name="smooth",
    )(*parts)


def exchanged(block, axis, shift):
    count = lax.axis_size(axis)
    route = []
    for low in range(shift, count + shift - 1, 2):
        pair = (low % count, (low + 1) % count)
        route += [pair, pair[::-1]]
    return lax.ppermute(block, axis, route)


def line_places(lines, local_lines):
    gy, inner = lax.axis_index("gy"), lax.axis_index("ang") * local_lines
    return [
        pl.ds(pl.multiple_of(group * lines + inner, 8), local_lines) for group in (gy, 1 - gy)
    ]


def pack_kernel(
    data_ref, offsets_ref, view_ref, taps_ref, weight_ref, volume_ref, multiplier_ref,
    sent_ref, data_out, offsets_out, view_out, taps_out, weight_out, own_ref, wave_ref, edge_ref, edge_sent_ref,
    volume_here, multiplier_here, step_cos_ref, step_sin_ref, part_cos_ref, part_sin_ref, lines_ref, sems,
):
    rows = data_ref.shape[0]
    lines = rows // 2
    local_lines, columns = volume_ref.shape
    half = columns // 2
    block_size = wave_ref.shape[1] // 2
    gx, gy = lax.axis_index("gx"), lax.axis_index("gy")
    first_core = gy == 0
    pairs = (
        (volume_ref, volume_here),
        (multiplier_ref, multiplier_here),
        (data_ref, data_out),
        (offsets_ref, offsets_out),
        (view_ref, view_out),
        (taps_ref, taps_out),
        (weight_ref, weight_out),
    )
    copies = [pltpu.make_async_copy(source, target, sems.at[at]) for at, (source, target) in enumerate(pairs)]
    for copy in copies:
        copy.start()

    lines_ref[...] = jnp.zeros_like(lines_ref)
    angles = (step_cos_ref, step_sin_ref, part_cos_ref, part_sin_ref)
    base = make_angles(gx * columns + gy * half - HALO, *angles)
    for part, first, count in chunks(half + 2 * HALO):

        def put(at, cosines, sines):
            wave_ref[pl.ds(first + at, 16), pl.ds(0, block_size)] = cosines
            wave_ref[pl.ds(first + at, 16), pl.ds(block_size, block_size)] = sines

        make_waves(base, part, count, *angles, put)

    copies[0].wait()
    copies[1].wait()
    low = volume_here[:, pl.ds(0, half)] + multiplier_here[:, pl.ds(0, half)]
    high = volume_here[:, pl.ds(half, half)] + multiplier_here[:, pl.ds(half, half)]
    outer = (low[:, :HALO], high[:, half - HALO :])
    place = line_places(lines, local_lines)[0]
    lines_ref[place, pl.ds(0, HALO)] = jnp.where(first_core, outer[0], outer[1])
    lines_ref[place, pl.ds(8, HALO)] = jnp.where(first_core, outer[1], outer[0])
    for group in range(2):
        group_lines = pl.ds(group * lines, lines)
        turned = lines_ref[group_lines, :].T
        edge_ref[:, group_lines] = turned[:8]
        edge_sent_ref[:, group_lines] = turned[8:16]

    below, above = low[:, half - HALO :], high[:, :HALO]
    own_ref[:, pl.ds(0, half)] = jnp.where(first_core, low, high)
    own_ref[:, pl.ds(half, HALO)] = jnp.where(first_core, above, below)
    sent_ref[pl.ds(rows, local_lines), :] = jnp.where(first_core, high, low)
    sent_ref[pl.ds(rows + local_lines, local_lines), pl.ds(0, HALO)] = jnp.where(first_core, below, above)
    copies[2].wait()
    sent_ref[pl.ds(0, rows), :] = data_out[...].astype(jnp.float32)
    for copy in copies[3:]:
        copy.wait()


def pack(data, offsets, view_index, taps, view_weight, volume, multiplier):
    rows, samples = data.shape
    local_lines, columns = volume.shape
    block_size = NX // lax.axis_size("ang")
    made = 16 * pl.cdiv(columns // 2 + 2 * HALO, 16)
    parts = 8 * pl.cdiv(pl.cdiv(columns // 2 + 2 * HALO, CHUNK), 8)
    vmem = pl.BlockSpec(memory_space=pltpu.VMEM)
    return pl.pallas_call(
        pack_kernel,
        out_shape=[
            pltpu.VMEM((rows + 2 * local_lines, samples), jnp.float32),
            pltpu.VMEM(data.shape, data.dtype),
            pltpu.VMEM(offsets.shape, offsets.dtype),
            pltpu.VMEM(view_index.shape, view_index.dtype),
            pltpu.VMEM(taps.shape, taps.dtype),
            pltpu.VMEM(view_weight.shape, view_weight.dtype),
            pltpu.VMEM((local_lines, columns // 2 + 128), jnp.float32),
            pltpu.VMEM((made, 2 * block_size), jnp.bfloat16),
            pltpu.VMEM((8, rows), jnp.float32),
            pltpu.VMEM((8, rows), jnp.float32),
        ],
        in_specs=[pl.BlockSpec(memory_space=pltpu.HBM)] * 7,
        out_specs=[vmem] * 10,
        scratch_shapes=[
            pltpu.VMEM(volume.shape, volume.dtype),
            pltpu.VMEM(multiplier.shape, multiplier.dtype),
            pltpu.VMEM((CHUNK // 8, block_size), jnp.float32),
            pltpu.VMEM((CHUNK // 8, block_size), jnp.float32),
            pltpu.VMEM((parts, block_size), jnp.float32),
            pltpu.VMEM((parts, block_size), jnp.float32),
            pltpu.VMEM((rows, 128), jnp.float32),
            pltpu.SemaphoreType.DMA((7,)),
        ],
        compiler_params=pltpu.CompilerParams(vmem_limit_bytes=VMEM_LIMIT),
        name="pack",
    )(
        *(
            pltpu.with_memory_space_constraint(array, pltpu.HBM)
            for array in (data, offsets, view_index, taps, view_weight, volume, multiplier)
        )
    )


def spread_of(offsets, view_index, taps, view_weight):
    block_size = NX // lax.axis_size("ang")
    vmem = pl.BlockSpec(memory_space=pltpu.VMEM)
    return pl.pallas_call(
        make_spread,
        out_shape=pltpu.VMEM((block_size, taps.shape[1]), jnp.bfloat16),
        in_specs=[vmem] * 4,
        out_specs=vmem,
        cost_estimate=pl.CostEstimate(flops=2 * 10**9, transcendentals=0, bytes_accessed=10**6),
        compiler_params=pltpu.CompilerParams(vmem_limit_bytes=VMEM_LIMIT),
        name="spread",
    )(offsets, view_index, taps, view_weight)


def grid_kernel(data_ref, own_ref, got_ref, spread_ref, grid_ref, vm_ref, both_ref, lines_ref):
    rows = data_ref.shape[0]
    lines = rows // 2
    block_size = spread_ref.shape[0]
    local_lines, columns = own_ref.shape[0], own_ref.shape[1] - 128
    gy = lax.axis_index("gy")
    for component in range(2):
        for group, ref in ((gy, data_ref), (1 - gy, got_ref)):
            place = pl.multiple_of((2 * component + group) * lines, 16)
            both_ref[pl.ds(place, lines), :] = ref[pl.ds(component * lines, lines), :].astype(jnp.bfloat16)
    for component in range(2):
        grid_ref[pl.ds(component * block_size, block_size), :] = lax.dot_general(
            spread_ref[...],
            both_ref[pl.ds(2 * component * lines, 2 * lines), :],
            NT,
            preferred_element_type=jnp.float32,
        ).astype(jnp.bfloat16)

    lines_ref[...] = jnp.zeros_like(lines_ref)
    own_place, other_place = line_places(lines, local_lines)
    side = pl.ds(columns, HALO)
    lines_ref[own_place, pl.ds(0, columns)] = own_ref[:, pl.ds(0, columns)]
    lines_ref[own_place, side] = own_ref[:, side]
    lines_ref[other_place, pl.ds(0, columns)] = got_ref[pl.ds(rows, local_lines), :]
    lines_ref[other_place, side] = got_ref[pl.ds(rows + local_lines, local_lines), pl.ds(0, HALO)]
    for group in range(2):
        group_lines = pl.ds(group * lines, lines)
        inner = lines_ref[group_lines, pl.ds(columns, 128)].T[:HALO]
        vm_ref[pl.ds(0, HALO), group_lines] = jnp.where(gy == 0, 0.0, inner)
        vm_ref[pl.ds(HALO + columns, HALO), group_lines] = jnp.where(gy == 0, inner, 0.0)
        for first in range(0, columns, 128):
            vm_ref[pl.ds(HALO + first, 128), group_lines] = lines_ref[group_lines, pl.ds(first, 128)].T


def grid(data, own, got, spread):
    lines = data.shape[0] // 2
    columns = own.shape[1] - 128
    vmem = pl.BlockSpec(memory_space=pltpu.VMEM)
    return pl.pallas_call(
        grid_kernel,
        out_shape=[
            pltpu.VMEM((2 * spread.shape[0], 2 * lines), jnp.bfloat16),
            pltpu.VMEM((columns + 2 * HALO, 2 * lines), jnp.float32),
        ],
        in_specs=[vmem] * 4,
        out_specs=[vmem] * 2,
        scratch_shapes=[
            pltpu.VMEM((4 * lines, data.shape[1]), jnp.bfloat16),
            pltpu.VMEM((2 * lines, columns + 128), jnp.float32),
        ],
        cost_estimate=pl.CostEstimate(flops=10**9, transcendentals=0, bytes_accessed=10**6),
        compiler_params=pltpu.CompilerParams(vmem_limit_bytes=VMEM_LIMIT),
        name="grid",
    )(data, own, got, spread)


def block_kernel(apart, wave_ref, grid_ref, vm_ref, edge_ref, out_ref):
    window = out_ref.shape[0]
    block = window - 2 * HALO
    angs = lax.axis_size("ang")
    dest = lax.axis_index("ang") ^ apart
    gy = lax.axis_index("gy")
    first = pl.multiple_of(dest * block, 16)
    made = 16 * pl.cdiv(window, 16)
    total = jnp.dot(wave_ref[pl.ds(first, made), :], grid_ref[...], preferred_element_type=jnp.float32)
    out_ref[...] = vm_ref[pl.ds(first, window), :] - total[:window] * NX ** (-0.5)
    edge = edge_ref[...][:HALO]
    opens = jnp.logical_and(dest == 0, gy == 0)
    out_ref[pl.ds(0, HALO), :] += jnp.where(opens, edge, 0.0)
    closes = jnp.logical_and(dest == angs - 1, gy == 1)
    out_ref[pl.ds(window - HALO, HALO), :] += jnp.where(closes, edge, 0.0)


def block_of(apart, wave, grid, vm, got_edge):
    window = (vm.shape[0] - 2 * HALO) // lax.axis_size("ang") + 2 * HALO
    vmem = pl.BlockSpec(memory_space=pltpu.VMEM)
    return pl.pallas_call(
        functools.partial(block_kernel, apart),
        out_shape=pltpu.VMEM((window, vm.shape[1]), jnp.float32),
        in_specs=[vmem] * 4,
        out_specs=vmem,
        cost_estimate=pl.CostEstimate(flops=10**9, transcendentals=0, bytes_accessed=10**6),
        compiler_params=pltpu.CompilerParams(vmem_limit_bytes=VMEM_LIMIT),
    )(wave, grid, vm, got_edge)


def on_chip(*arrays):
    return [pltpu.with_memory_space_constraint(array, pltpu.VMEM) for array in arrays]


def project_paired(data, offsets, view_index, taps, view_weight, volume, multiplier):
    sent, data, offsets, view_index, taps, view_weight, own, wave, near, near_sent = pack(
        data, offsets, view_index, taps, view_weight, volume, multiplier
    )
    near_got = lax.ppermute(near_sent, "gy", [(0, 1), (1, 0)])
    got = lax.ppermute(sent, "gy", [(0, 1), (1, 0)])
    spread = spread_of(*on_chip(offsets, view_index, taps, view_weight))
    count = lax.axis_size("gx")
    route = []
    for low in range(count):
        pair = (count + low, (low + 1) % count)
        route += [pair, pair[::-1]]
    got_edge = lax.ppermute(near + near_got, ("gy", "gx"), route)
    gridded, vm = grid(*on_chip(data, own, got, spread))
    wave, gridded, vm, got_edge = on_chip(wave, gridded, vm, got_edge)
    angs = lax.axis_size("ang")
    parts = []
    for apart in range(angs - 1, 0, -1):
        part = block_of(apart, wave, gridded, vm, got_edge)
        parts.append(lax.ppermute(part, "ang", [(ang, ang ^ apart) for ang in range(angs)]))
    return [block_of(0, wave, gridded, vm, got_edge)] + parts


def per_device(spectrum_data, offsets, view_index, kernel, view_weight, volume, multiplier):
    local_planes, rows, columns = volume.shape
    planes = spectrum_data.shape[1]
    samples = spectrum_data.shape[3]
    dests = lax.axis_size("ang") * lax.axis_size("gy")
    local_lines = local_planes * rows
    lines = planes * rows

    volume = volume.reshape(local_lines, columns)
    multiplier = multiplier.reshape(local_lines, columns)
    arrays = (
        spectrum_data.reshape(2 * lines, samples),
        offsets.reshape(samples // 128, 128),
        view_index.reshape(samples // 128, 128),
        kernel,
        view_weight,
        volume,
        multiplier,
    )
    angs = lax.axis_size("ang")
    if lax.axis_size("gy") == 2 and columns // 2 == samples and angs & (angs - 1) == 0:
        parts = project_paired(*arrays)
    else:
        first_edge = volume[:, :HALO] + multiplier[:, :HALO]
        last_edge = volume[:, -HALO:] + multiplier[:, -HALO:]
        even = lax.axis_index("gx") % 2 == 0
        inner = exchanged(jnp.where(even, last_edge, first_edge), "gx", 0)
        outer = exchanged(jnp.where(even, first_edge, last_edge), "gx", 1)
        parts = close(project(*arrays, dests), *on_chip(inner, outer))
        parts = [lax.all_to_all(parts, ("gy", "ang"), split_axis=0, concat_axis=0)]
    done = smooth(on_chip(*parts), planes, local_lines, columns)
    done = lax.all_to_all(done, ("gy", "ang"), split_axis=0, concat_axis=0)
    return jnp.transpose(done, (1, 0, 2)).reshape(local_planes, rows, columns)


def solution(mesh):
    placed = (
        P(None, None, "gy", "ang"),
        P("ang"),
        P("ang"),
        P(None, "ang"),
        P(),
        P("ang", "gy", "gx"),
        P("ang", "gy", "gx"),
    )
    return jax.shard_map(per_device, mesh=mesh, in_specs=placed, out_specs=P("ang", "gy", "gx"), check_vma=False)
```

```python
import functools
import math

import jax
import jax.numpy as jnp
from jax import lax
from jax.experimental import pallas as pl
from jax.experimental.pallas import tpu as pltpu
from jax.sharding import PartitionSpec as P


NX = 4096
TV_STEPS = 4
HALO = TV_STEPS
CHUNK = 128
PIECE = 72
VMEM_LIMIT = 24 * 2**20

smooth_weight = 0.5
dual_step = 1.0 / 12.0

NT = (((1,), (1,)), ((), ()))


def unit_circle(phase):
    phase = phase & (NX - 1)
    quarter = (phase + NX // 8) // (NX // 4)
    angle = (phase - quarter * (NX // 4)).astype(jnp.float32) * (2.0 * math.pi / NX)
    square = angle * angle
    sine = angle * (1.0 + square * (-1.0 / 6 + square * (1.0 / 120 + square * (-1.0 / 5040 + square * (1.0 / 362880)))))
    cosine = 1.0 + square * (-0.5 + square * (1.0 / 24 + square * (-1.0 / 720 + square * (1.0 / 40320))))
    odd = (quarter & 1) == 1
    first = jnp.where(odd, -sine, cosine)
    second = jnp.where(odd, cosine, sine)
    flip = (quarter & 2) == 2
    return jnp.where(flip, -first, first), jnp.where(flip, -second, second)


def make_spread(offsets_ref, view_ref, taps_ref, weight_ref, spread_ref):
    block_size, samples = spread_ref.shape
    views = weight_ref.shape[0]
    pieces = []
    for piece in range(samples // 128):
        view = view_ref[pl.ds(piece, 1), :]
        found = jnp.zeros((1, 128), jnp.float32)
        lane = jnp.broadcast_to(view & 127, (8, 128))
        for first in range(0, views, 128):
            table = weight_ref[pl.ds(first, min(128, views - first))].reshape(1, -1)
            if views - first < 128:
                table = jnp.concatenate([table, jnp.zeros((1, 128 - (views - first)), jnp.float32)], axis=1)
            picked = jnp.take_along_axis(jnp.broadcast_to(table, (8, 128)), lane, axis=1)[:1]
            found = jnp.where(view // 128 == first // 128, picked, found)
        pieces.append(found)
    weight = jnp.concatenate(pieces, axis=1)
    values = [weight * taps_ref[pl.ds(tap, 1), :] for tap in range(taps_ref.shape[0])]
    offsets = jnp.concatenate([offsets_ref[pl.ds(piece, 1), :] for piece in range(samples // 128)], axis=1)

    rows = 16
    cell = lax.broadcasted_iota(jnp.int32, (rows, samples), 0)
    starts = [jnp.broadcast_to(offsets + index, (rows, samples)) for index in range(len(values))]
    values = [jnp.broadcast_to(value, (rows, samples)) for value in values]
    for first in range(0, block_size, rows):
        here = cell + first
        spread = jnp.zeros((rows, samples), jnp.float32)
        for start, value in zip(starts, values):
            spread = jnp.where(here == start, value, spread)
        spread_ref[pl.ds(first, rows), :] = spread.astype(jnp.bfloat16)


def make_angles(first_column, step_cos_ref, step_sin_ref, part_cos_ref, part_sin_ref):
    block_size = step_cos_ref.shape[1]
    freq = lax.axis_index("ang") * block_size + lax.broadcasted_iota(jnp.int32, (8, block_size), 1)
    row = lax.broadcasted_iota(jnp.int32, (8, block_size), 0)
    for first in range(0, CHUNK // 8, 8):
        step_cos_ref[pl.ds(first, 8), :], step_sin_ref[pl.ds(first, 8), :] = unit_circle(-freq * (8 * (row + first)))
    for first in range(0, part_cos_ref.shape[0], 8):
        part_cos_ref[pl.ds(first, 8), :], part_sin_ref[pl.ds(first, 8), :] = unit_circle(
            -freq * (CHUNK * (row + first))
        )
    return unit_circle(-freq * (first_column + row))


def make_waves(base, part, count, step_cos_ref, step_sin_ref, part_cos_ref, part_sin_ref, put):
    base_cos, base_sin = base
    part_cos, part_sin = part_cos_ref[pl.ds(part, 1), :], part_sin_ref[pl.ds(part, 1), :]
    here_cos = base_cos * part_cos - base_sin * part_sin
    here_sin = base_sin * part_cos + base_cos * part_sin
    for step in range(0, pl.cdiv(count, 8), 2):
        pair_cos, pair_sin = [], []
        for one in (step, step + 1):
            step_cos, step_sin = step_cos_ref[pl.ds(one, 1), :], step_sin_ref[pl.ds(one, 1), :]
            pair_cos.append(here_cos * step_cos - here_sin * step_sin)
            pair_sin.append(here_sin * step_cos + here_cos * step_sin)
        put(
            8 * step,
            jnp.concatenate(pair_cos, axis=0).astype(jnp.bfloat16),
            jnp.concatenate(pair_sin, axis=0).astype(jnp.bfloat16),
        )


def chunks(total):
    return [(part, part * CHUNK, min(CHUNK, total - part * CHUNK)) for part in range(pl.cdiv(total, CHUNK))]


def put_windows(out_ref, first, count, sent):
    dests, window, _ = out_ref.shape
    block = window - 2 * HALO
    for dest in range(dests):
        low, high = max(first, dest * block), min(first + count, dest * block + window)
        if low < high:
            out_ref[dest, pl.ds(low - dest * block, high - low), :] = sent[low - first : high - first]


def project_kernel(
    data_ref, offsets_ref, view_ref, taps_ref, weight_ref, volume_ref, multiplier_ref,
    out_ref,
    spread_ref, grid_ref, cos_ref, sin_ref, step_cos_ref, step_sin_ref, part_cos_ref, part_sin_ref, lines_ref, vm_ref,
):
    ang, gx = lax.axis_index("ang"), lax.axis_index("gx")
    lines = data_ref.shape[0] // 2
    local_lines, columns = volume_ref.shape

    make_spread(offsets_ref, view_ref, taps_ref, weight_ref, spread_ref)
    grid_ref[...] = lax.dot_general(
        data_ref[...], spread_ref[...], NT, preferred_element_type=jnp.float32
    ).astype(jnp.bfloat16)

    lines_ref[...] = jnp.zeros_like(lines_ref)
    lines_ref[pl.ds(pl.multiple_of(ang * local_lines, 8), local_lines), :] = volume_ref[...] + multiplier_ref[...]
    vm_ref[pl.ds(0, HALO), :] = jnp.zeros((HALO, lines), jnp.float32)
    vm_ref[pl.ds(HALO + columns, HALO), :] = jnp.zeros((HALO, lines), jnp.float32)
    for first in range(0, columns, 128):
        vm_ref[pl.ds(HALO + first, 128), :] = lines_ref[:, pl.ds(first, 128)].T

    angles = (step_cos_ref, step_sin_ref, part_cos_ref, part_sin_ref)
    base = make_angles(gx * columns - HALO, *angles)
    for part, first, count in chunks(columns + 2 * HALO):
        slot = part % 2

        def put(at, cosines, sines):
            cos_ref[slot, pl.ds(at, 16), :] = cosines
            sin_ref[slot, pl.ds(at, 16), :] = sines

        make_waves(base, part, count, *angles, put)
        made = max(16, count)
        total_part = lax.dot_general(
            cos_ref[slot, pl.ds(0, made), :], grid_ref[pl.ds(0, lines), :], NT, preferred_element_type=jnp.float32
        ) + lax.dot_general(
            sin_ref[slot, pl.ds(0, made), :], grid_ref[pl.ds(lines, lines), :], NT, preferred_element_type=jnp.float32
        )
        put_windows(out_ref, first, count, vm_ref[pl.ds(first, count), :] - total_part[:count] * NX ** (-0.5))


def project(data, offsets, view_index, taps, view_weight, volume, multiplier, dests):
    lines = data.shape[0] // 2
    samples = data.shape[1]
    columns = volume.shape[1]
    block_size = NX // lax.axis_size("ang")
    window = columns // dests + 2 * HALO
    parts = pl.cdiv(columns + 2 * HALO, CHUNK)
    vmem = pl.BlockSpec(memory_space=pltpu.VMEM)
    return pl.pallas_call(
        project_kernel,
        out_shape=pltpu.VMEM((dests, window, lines), jnp.float32),
        in_specs=[vmem] * 7,
        out_specs=vmem,
        scratch_shapes=[
            pltpu.VMEM((block_size, samples), jnp.bfloat16),
            pltpu.VMEM((2 * lines, block_size), jnp.bfloat16),
            pltpu.VMEM((2, CHUNK, block_size), jnp.bfloat16),
            pltpu.VMEM((2, CHUNK, block_size), jnp.bfloat16),
            pltpu.VMEM((CHUNK // 8, block_size), jnp.float32),
            pltpu.VMEM((CHUNK // 8, block_size), jnp.float32),
            pltpu.VMEM((8 * pl.cdiv(parts, 8), block_size), jnp.float32),
            pltpu.VMEM((8 * pl.cdiv(parts, 8), block_size), jnp.float32),
            pltpu.VMEM((lines, columns), jnp.float32),
            pltpu.VMEM((columns + 2 * HALO, lines), jnp.float32),
        ],
        cost_estimate=pl.CostEstimate(flops=4 * 10**9, transcendentals=0, bytes_accessed=10**6),
        compiler_params=pltpu.CompilerParams(vmem_limit_bytes=VMEM_LIMIT),
        name="project",
    )(data, offsets, view_index, taps, view_weight, volume, multiplier)


def close_kernel(parts_ref, inner_ref, outer_ref, out_ref, halo_ref):
    ang = lax.axis_index("ang")
    even = lax.axis_index("gx") % 2 == 0
    dests, window, _ = parts_ref.shape
    local_lines = inner_ref.shape[0]
    halo_ref[...] = jnp.zeros_like(halo_ref)
    own = pl.ds(pl.multiple_of(ang * local_lines, 8), local_lines)
    inner, outer = inner_ref[...], outer_ref[...]
    halo_ref[own, pl.ds(0, HALO)] = jnp.where(even, outer, inner)
    halo_ref[own, pl.ds(HALO, HALO)] = jnp.where(even, inner, outer)
    edges = halo_ref[...].T
    out_ref[0, pl.ds(0, HALO), :] = parts_ref[0, pl.ds(0, HALO), :] + edges[:HALO]
    last = pl.ds(window - HALO, HALO)
    out_ref[dests - 1, last, :] = parts_ref[dests - 1, last, :] + edges[HALO : 2 * HALO]


def close(parts, inner, outer):
    vmem = pl.BlockSpec(memory_space=pltpu.VMEM)
    return pl.pallas_call(
        close_kernel,
        out_shape=pltpu.VMEM(parts.shape, parts.dtype),
        in_specs=[vmem] * 3,
        out_specs=vmem,
        scratch_shapes=[pltpu.VMEM((parts.shape[2], 128), jnp.float32)],
        input_output_aliases={0: 0},
        compiler_params=pltpu.CompilerParams(vmem_limit_bytes=VMEM_LIMIT),
        name="close",
    )(parts, inner, outer)


def smooth_kernel(planes, columns, *refs):
    *parts_refs, out_ref, done_ref = refs
    _, local_lines, block = out_ref.shape
    window = parts_refs[0].shape[-2]
    angs, groups = lax.axis_size("ang"), lax.axis_size("gy")
    lines = angs * local_lines
    rows = lines // planes
    size = min(PIECE, window)
    pieces = [(first, min(size, window - first)) for first in range(0, window, size)]
    tiles = len(pieces)
    lanes = [lax.broadcasted_iota(jnp.int32, (height, lines), 1) for _, height in pieces]
    inside = lax.broadcasted_iota(jnp.int32, (8, lines), 0)
    plane_opens = [lane // rows < planes - 1 for lane in lanes]
    row_firsts = [lane % rows == 0 for lane in lanes]
    row_lasts = [lane % rows == rows - 1 for lane in lanes]
    place = lax.axis_index("gy") * angs + lax.axis_index("ang")
    first_column = lax.axis_index("gx") * columns + place * block - HALO
    zero = jnp.float32(0.0)

    def part(ang, group, tile):
        at = pl.ds(*pieces[tile])
        if len(parts_refs) > 1:
            return parts_refs[ang][at, pl.ds(group * lines, lines)]
        return parts_refs[0][group * angs + ang, at, :]

    source = [[sum((part(ang, group, tile) for ang in range(1, angs)), part(0, group, tile)) for group in range(groups)]
              for tile in range(tiles)]

    def divergence(flow, tile):
        rolled = [pltpu.roll(flow[tile][group][1], 1, 1) for group in range(groups)]
        result = []
        for group in range(groups):
            f0, f1, f2 = flow[tile][group]
            wrapped = pltpu.roll(flow[tile][group - 1][1], lines - (rows - 1), 1)
            lower_row = jnp.where(row_firsts[tile], wrapped, rolled[group])
            lower_cell = pltpu.roll(f2, 1, 0)
            if tile > 0:
                before = flow[tile - 1][group][2]
                opening = jnp.where(inside == 0, pltpu.roll(before[-8:], 1, 0), lower_cell[:8])
                lower_cell = jnp.concatenate([opening, lower_cell[8:]], axis=0)
            result.append((f0 - pltpu.roll(f0, rows, 1)) + (f1 - lower_row) + (f2 - lower_cell))
        return result

    def target_of(flow, tile):
        scaled = [value * (dual_step / smooth_weight) for value in source[tile]]
        if flow is None:
            return [-value for value in scaled]
        return [dual_step * div - value for div, value in zip(divergence(flow, tile), scaled)]

    flow = None
    for _ in range(TV_STEPS):
        updated = []
        after = target_of(flow, 0)
        for tile in range(tiles):
            target = after
            after = target_of(flow, tile + 1) if tile + 1 < tiles else target
            _, height = pieces[tile]
            plane_open, row_last = plane_opens[tile], row_lasts[tile]
            moved_groups = []
            for group in range(groups):
                here = target[group]
                slope_plane = jnp.where(plane_open, pltpu.roll(here, lines - rows, 1) - here, zero)
                upper_row = pltpu.roll(here, lines - 1, 1)
                if group + 1 < groups:
                    slope_row = jnp.where(row_last, pltpu.roll(target[group + 1], rows - 1, 1), upper_row) - here
                else:
                    slope_row = jnp.where(row_last, zero, upper_row - here)
                upper_cell = pltpu.roll(here, height - 1, 0)
                if tile + 1 < tiles:
                    closing = jnp.where(inside == 7, pltpu.roll(after[group][:8], 7, 0), upper_cell[-8:])
                    upper_cell = jnp.concatenate([upper_cell[:-8], closing], axis=0)
                slope_cell = upper_cell - here
                if tile == 0:
                    opening = jnp.where(first_column + inside >= 0, slope_cell[:8], zero)
                    slope_cell = jnp.concatenate([opening, slope_cell[8:]], axis=0)
                if tile == tiles - 1:
                    column = first_column + window - 8 + inside
                    closing = jnp.where(column < NX - 1, slope_cell[-8:], zero)
                    slope_cell = jnp.concatenate([slope_cell[:-8], closing], axis=0)
                square = slope_plane * slope_plane + slope_row * slope_row + slope_cell * slope_cell
                scale = 1.0 / (1.0 + square * lax.rsqrt(jnp.maximum(square, 1e-30)))
                moved = [slope_plane, slope_row, slope_cell]
                if flow is not None:
                    moved = [f + m for f, m in zip(flow[tile][group], moved)]
                moved_groups.append([m * scale for m in moved])
            updated.append(moved_groups)
        flow = updated
    for tile in range(tiles):
        for group, div in enumerate(divergence(flow, tile)):
            done_ref[group, pl.ds(*pieces[tile]), :] = source[tile][group] - smooth_weight * div
    for group in range(groups):
        turned = done_ref[group, pl.ds(HALO, block), :].T
        for ang in range(angs):
            out_ref[group * angs + ang] = turned[ang * local_lines : (ang + 1) * local_lines]


def smooth(parts, planes, local_lines, columns):
    window = parts[0].shape[-2]
    dests = lax.axis_size("ang") * lax.axis_size("gy")
    vmem = pl.BlockSpec(memory_space=pltpu.VMEM)
    return pl.pallas_call(
        functools.partial(smooth_kernel, planes, columns),
        out_shape=pltpu.VMEM((dests, local_lines, window - 2 * HALO), jnp.float32),
        in_specs=[vmem] * len(parts),
        out_specs=vmem,
        scratch_shapes=[
            pltpu.VMEM((lax.axis_size("gy"), window, lax.axis_size("ang") * local_lines), jnp.float32)
        ],
        compiler_params=pltpu.CompilerParams(vmem_limit_bytes=VMEM_LIMIT),
        name="smooth",
    )(*parts)


def exchanged(block, axis, shift):
    count = lax.axis_size(axis)
    route = []
    for low in range(shift, count + shift - 1, 2):
        pair = (low % count, (low + 1) % count)
        route += [pair, pair[::-1]]
    return lax.ppermute(block, axis, route)


def line_places(lines, local_lines):
    gy, inner = lax.axis_index("gy"), lax.axis_index("ang") * local_lines
    return [
        pl.ds(pl.multiple_of(group * lines + inner, 8), local_lines) for group in (gy, 1 - gy)
    ]


def pack_kernel(
    data_ref, offsets_ref, view_ref, taps_ref, weight_ref, volume_ref, multiplier_ref,
    sent_ref, data_out, offsets_out, view_out, taps_out, weight_out, own_ref, wave_ref, edge_ref, edge_sent_ref,
    volume_here, multiplier_here, step_cos_ref, step_sin_ref, part_cos_ref, part_sin_ref, lines_ref, sems,
):
    rows = data_ref.shape[0]
    lines = rows // 2
    local_lines, columns = volume_ref.shape
    half = columns // 2
    block_size = wave_ref.shape[1] // 2
    gx, gy = lax.axis_index("gx"), lax.axis_index("gy")
    first_core = gy == 0
    pairs = (
        (volume_ref, volume_here),
        (multiplier_ref, multiplier_here),
        (data_ref, data_out),
        (offsets_ref, offsets_out),
        (view_ref, view_out),
        (taps_ref, taps_out),
        (weight_ref, weight_out),
    )
    copies = [pltpu.make_async_copy(source, target, sems.at[at]) for at, (source, target) in enumerate(pairs)]
    for copy in copies:
        copy.start()

    lines_ref[...] = jnp.zeros_like(lines_ref)
    angles = (step_cos_ref, step_sin_ref, part_cos_ref, part_sin_ref)
    base = make_angles(gx * columns + gy * half - HALO, *angles)
    for part, first, count in chunks(half + 2 * HALO):

        def put(at, cosines, sines):
            wave_ref[pl.ds(first + at, 16), pl.ds(0, block_size)] = cosines
            wave_ref[pl.ds(first + at, 16), pl.ds(block_size, block_size)] = sines

        make_waves(base, part, count, *angles, put)

    copies[0].wait()
    copies[1].wait()
    low = volume_here[:, pl.ds(0, half)] + multiplier_here[:, pl.ds(0, half)]
    high = volume_here[:, pl.ds(half, half)] + multiplier_here[:, pl.ds(half, half)]
    outer = (low[:, :HALO], high[:, half - HALO :])
    place = line_places(lines, local_lines)[0]
    lines_ref[place, pl.ds(0, HALO)] = jnp.where(first_core, outer[0], outer[1])
    lines_ref[place, pl.ds(8, HALO)] = jnp.where(first_core, outer[1], outer[0])
    for group in range(2):
        group_lines = pl.ds(group * lines, lines)
        turned = lines_ref[group_lines, :].T
        edge_ref[:, group_lines] = turned[:8]
        edge_sent_ref[:, group_lines] = turned[8:16]

    below, above = low[:, half - HALO :], high[:, :HALO]
    own_ref[:, pl.ds(0, half)] = jnp.where(first_core, low, high)
    own_ref[:, pl.ds(half, HALO)] = jnp.where(first_core, above, below)
    sent_ref[pl.ds(rows, local_lines), :] = jnp.where(first_core, high, low)
    sent_ref[pl.ds(rows + local_lines, local_lines), pl.ds(0, HALO)] = jnp.where(first_core, below, above)
    copies[2].wait()
    sent_ref[pl.ds(0, rows), :] = data_out[...].astype(jnp.float32)
    for copy in copies[3:]:
        copy.wait()


def pack(data, offsets, view_index, taps, view_weight, volume, multiplier):
    rows, samples = data.shape
    local_lines, columns = volume.shape
    block_size = NX // lax.axis_size("ang")
    made = 16 * pl.cdiv(columns // 2 + 2 * HALO, 16)
    parts = 8 * pl.cdiv(pl.cdiv(columns // 2 + 2 * HALO, CHUNK), 8)
    vmem = pl.BlockSpec(memory_space=pltpu.VMEM)
    return pl.pallas_call(
        pack_kernel,
        out_shape=[
            pltpu.VMEM((rows + 2 * local_lines, samples), jnp.float32),
            pltpu.VMEM(data.shape, data.dtype),
            pltpu.VMEM(offsets.shape, offsets.dtype),
            pltpu.VMEM(view_index.shape, view_index.dtype),
            pltpu.VMEM(taps.shape, taps.dtype),
            pltpu.VMEM(view_weight.shape, view_weight.dtype),
            pltpu.VMEM((local_lines, columns // 2 + 128), jnp.float32),
            pltpu.VMEM((made, 2 * block_size), jnp.bfloat16),
            pltpu.VMEM((8, rows), jnp.float32),
            pltpu.VMEM((8, rows), jnp.float32),
        ],
        in_specs=[pl.BlockSpec(memory_space=pltpu.HBM)] * 7,
        out_specs=[vmem] * 10,
        scratch_shapes=[
            pltpu.VMEM(volume.shape, volume.dtype),
            pltpu.VMEM(multiplier.shape, multiplier.dtype),
            pltpu.VMEM((CHUNK // 8, block_size), jnp.float32),
            pltpu.VMEM((CHUNK // 8, block_size), jnp.float32),
            pltpu.VMEM((parts, block_size), jnp.float32),
            pltpu.VMEM((parts, block_size), jnp.float32),
            pltpu.VMEM((rows, 128), jnp.float32),
            pltpu.SemaphoreType.DMA((7,)),
        ],
        compiler_params=pltpu.CompilerParams(vmem_limit_bytes=VMEM_LIMIT),
        name="pack",
    )(
        *(
            pltpu.with_memory_space_constraint(array, pltpu.HBM)
            for array in (data, offsets, view_index, taps, view_weight, volume, multiplier)
        )
    )


def spread_of(offsets, view_index, taps, view_weight):
    block_size = NX // lax.axis_size("ang")
    vmem = pl.BlockSpec(memory_space=pltpu.VMEM)
    return pl.pallas_call(
        make_spread,
        out_shape=pltpu.VMEM((block_size, taps.shape[1]), jnp.bfloat16),
        in_specs=[vmem] * 4,
        out_specs=vmem,
        cost_estimate=pl.CostEstimate(flops=2 * 10**9, transcendentals=0, bytes_accessed=10**6),
        compiler_params=pltpu.CompilerParams(vmem_limit_bytes=VMEM_LIMIT),
        name="spread",
    )(offsets, view_index, taps, view_weight)


def grid_kernel(data_ref, own_ref, got_ref, spread_ref, grid_ref, vm_ref, both_ref, lines_ref):
    rows = data_ref.shape[0]
    lines = rows // 2
    block_size = spread_ref.shape[0]
    local_lines, columns = own_ref.shape[0], own_ref.shape[1] - 128
    gy = lax.axis_index("gy")
    for component in range(2):
        for group, ref in ((gy, data_ref), (1 - gy, got_ref)):
            place = pl.multiple_of((2 * component + group) * lines, 16)
            both_ref[pl.ds(place, lines), :] = ref[pl.ds(component * lines, lines), :].astype(jnp.bfloat16)
    for component in range(2):
        grid_ref[pl.ds(component * block_size, block_size), :] = lax.dot_general(
            spread_ref[...],
            both_ref[pl.ds(2 * component * lines, 2 * lines), :],
            NT,
            preferred_element_type=jnp.float32,
        ).astype(jnp.bfloat16)

    lines_ref[...] = jnp.zeros_like(lines_ref)
    own_place, other_place = line_places(lines, local_lines)
    side = pl.ds(columns, HALO)
    lines_ref[own_place, pl.ds(0, columns)] = own_ref[:, pl.ds(0, columns)]
    lines_ref[own_place, side] = own_ref[:, side]
    lines_ref[other_place, pl.ds(0, columns)] = got_ref[pl.ds(rows, local_lines), :]
    lines_ref[other_place, side] = got_ref[pl.ds(rows + local_lines, local_lines), pl.ds(0, HALO)]
    for group in range(2):
        group_lines = pl.ds(group * lines, lines)
        inner = lines_ref[group_lines, pl.ds(columns, 128)].T[:HALO]
        vm_ref[pl.ds(0, HALO), group_lines] = jnp.where(gy == 0, 0.0, inner)
        vm_ref[pl.ds(HALO + columns, HALO), group_lines] = jnp.where(gy == 0, inner, 0.0)
        for first in range(0, columns, 128):
            vm_ref[pl.ds(HALO + first, 128), group_lines] = lines_ref[group_lines, pl.ds(first, 128)].T


def grid(data, own, got, spread):
    lines = data.shape[0] // 2
    columns = own.shape[1] - 128
    vmem = pl.BlockSpec(memory_space=pltpu.VMEM)
    return pl.pallas_call(
        grid_kernel,
        out_shape=[
            pltpu.VMEM((2 * spread.shape[0], 2 * lines), jnp.bfloat16),
            pltpu.VMEM((columns + 2 * HALO, 2 * lines), jnp.float32),
        ],
        in_specs=[vmem] * 4,
        out_specs=[vmem] * 2,
        scratch_shapes=[
            pltpu.VMEM((4 * lines, data.shape[1]), jnp.bfloat16),
            pltpu.VMEM((2 * lines, columns + 128), jnp.float32),
        ],
        cost_estimate=pl.CostEstimate(flops=10**9, transcendentals=0, bytes_accessed=10**6),
        compiler_params=pltpu.CompilerParams(vmem_limit_bytes=VMEM_LIMIT),
        name="grid",
    )(data, own, got, spread)


def block_kernel(apart, wave_ref, grid_ref, vm_ref, edge_ref, out_ref):
    window = out_ref.shape[0]
    block = window - 2 * HALO
    angs = lax.axis_size("ang")
    dest = lax.axis_index("ang") ^ apart
    gy = lax.axis_index("gy")
    first = pl.multiple_of(dest * block, 16)
    made = 16 * pl.cdiv(window, 16)
    total = jnp.dot(wave_ref[pl.ds(first, made), :], grid_ref[...], preferred_element_type=jnp.float32)
    out_ref[...] = vm_ref[pl.ds(first, window), :] - total[:window] * NX ** (-0.5)
    edge = edge_ref[...][:HALO]
    opens = jnp.logical_and(dest == 0, gy == 0)
    out_ref[pl.ds(0, HALO), :] += jnp.where(opens, edge, 0.0)
    closes = jnp.logical_and(dest == angs - 1, gy == 1)
    out_ref[pl.ds(window - HALO, HALO), :] += jnp.where(closes, edge, 0.0)


def block_of(apart, wave, grid, vm, got_edge):
    window = (vm.shape[0] - 2 * HALO) // lax.axis_size("ang") + 2 * HALO
    vmem = pl.BlockSpec(memory_space=pltpu.VMEM)
    return pl.pallas_call(
        functools.partial(block_kernel, apart),
        out_shape=pltpu.VMEM((window, vm.shape[1]), jnp.float32),
        in_specs=[vmem] * 4,
        out_specs=vmem,
        cost_estimate=pl.CostEstimate(flops=10**9, transcendentals=0, bytes_accessed=10**6),
        compiler_params=pltpu.CompilerParams(vmem_limit_bytes=VMEM_LIMIT),
    )(wave, grid, vm, got_edge)


def on_chip(*arrays):
    return [pltpu.with_memory_space_constraint(array, pltpu.VMEM) for array in arrays]


def project_paired(data, offsets, view_index, taps, view_weight, volume, multiplier):
    sent, data, offsets, view_index, taps, view_weight, own, wave, near, near_sent = pack(
        data, offsets, view_index, taps, view_weight, volume, multiplier
    )
    near_got = lax.ppermute(near_sent, "gy", [(0, 1), (1, 0)])
    got = lax.ppermute(sent, "gy", [(0, 1), (1, 0)])
    spread = spread_of(*on_chip(offsets, view_index, taps, view_weight))
    count = lax.axis_size("gx")
    route = []
    for low in range(count):
        pair = (count + low, (low + 1) % count)
        route += [pair, pair[::-1]]
    got_edge = lax.ppermute(near + near_got, ("gy", "gx"), route)
    gridded, vm = grid(*on_chip(data, own, got, spread))
    wave, gridded, vm, got_edge = on_chip(wave, gridded, vm, got_edge)
    angs = lax.axis_size("ang")
    parts = []
    for apart in range(angs - 1, 0, -1):
        part = block_of(apart, wave, gridded, vm, got_edge)
        parts.append(lax.ppermute(part, "ang", [(ang, ang ^ apart) for ang in range(angs)]))
    return [block_of(0, wave, gridded, vm, got_edge)] + parts


def per_device(spectrum_data, offsets, view_index, kernel, view_weight, volume, multiplier):
    local_planes, rows, columns = volume.shape
    planes = spectrum_data.shape[1]
    samples = spectrum_data.shape[3]
    dests = lax.axis_size("ang") * lax.axis_size("gy")
    local_lines = local_planes * rows
    lines = planes * rows

    volume = volume.reshape(local_lines, columns)
    multiplier = multiplier.reshape(local_lines, columns)
    arrays = (
        spectrum_data.reshape(2 * lines, samples),
        offsets.reshape(samples // 128, 128),
        view_index.reshape(samples // 128, 128),
        kernel,
        view_weight,
        volume,
        multiplier,
    )
    angs = lax.axis_size("ang")
    if lax.axis_size("gy") == 2 and columns // 2 == samples and angs & (angs - 1) == 0:
        parts = project_paired(*arrays)
    else:
        first_edge = volume[:, :HALO] + multiplier[:, :HALO]
        last_edge = volume[:, -HALO:] + multiplier[:, -HALO:]
        even = lax.axis_index("gx") % 2 == 0
        inner = exchanged(jnp.where(even, last_edge, first_edge), "gx", 0)
        outer = exchanged(jnp.where(even, first_edge, last_edge), "gx", 1)
        parts = close(project(*arrays, dests), *on_chip(inner, outer))
        parts = [lax.all_to_all(parts, ("gy", "ang"), split_axis=0, concat_axis=0)]
    done = smooth(on_chip(*parts), planes, local_lines, columns)
    done = lax.all_to_all(done, ("gy", "ang"), split_axis=0, concat_axis=0)
    return jnp.transpose(done, (1, 0, 2)).reshape(local_planes, rows, columns)


def solution(mesh):
    placed = (
        P(None, None, "gy", "ang"),
        P("ang"),
        P("ang"),
        P(None, "ang"),
        P(),
        P("ang", "gy", "gx"),
        P("ang", "gy", "gx"),
    )
    return jax.shard_map(per_device, mesh=mesh, in_specs=placed, out_specs=P("ang", "gy", "gx"), check_vma=False)
```

```python
import functools
import math

import jax
import jax.numpy as jnp
from jax import lax
from jax.experimental import pallas as pl
from jax.experimental.pallas import tpu as pltpu
from jax.sharding import PartitionSpec as P


NX = 4096
TV_STEPS = 4
HALO = TV_STEPS
CHUNK = 128
PIECE = 72
VMEM_LIMIT = 24 * 2**20

smooth_weight = 0.5
dual_step = 1.0 / 12.0

NT = (((1,), (1,)), ((), ()))


def unit_circle(phase):
    phase = phase & (NX - 1)
    quarter = (phase + NX // 8) // (NX // 4)
    angle = (phase - quarter * (NX // 4)).astype(jnp.float32) * (2.0 * math.pi / NX)
    square = angle * angle
    sine = angle * (1.0 + square * (-1.0 / 6 + square * (1.0 / 120 + square * (-1.0 / 5040 + square * (1.0 / 362880)))))
    cosine = 1.0 + square * (-0.5 + square * (1.0 / 24 + square * (-1.0 / 720 + square * (1.0 / 40320))))
    odd = (quarter & 1) == 1
    first = jnp.where(odd, -sine, cosine)
    second = jnp.where(odd, cosine, sine)
    flip = (quarter & 2) == 2
    return jnp.where(flip, -first, first), jnp.where(flip, -second, second)


def make_spread(offsets_ref, view_ref, taps_ref, weight_ref, spread_ref):
    block_size, samples = spread_ref.shape
    views = weight_ref.shape[0]
    pieces = []
    for piece in range(samples // 128):
        view = view_ref[pl.ds(piece, 1), :]
        found = jnp.zeros((1, 128), jnp.float32)
        lane = jnp.broadcast_to(view & 127, (8, 128))
        for first in range(0, views, 128):
            table = weight_ref[pl.ds(first, min(128, views - first))].reshape(1, -1)
            if views - first < 128:
                table = jnp.concatenate([table, jnp.zeros((1, 128 - (views - first)), jnp.float32)], axis=1)
            picked = jnp.take_along_axis(jnp.broadcast_to(table, (8, 128)), lane, axis=1)[:1]
            found = jnp.where(view // 128 == first // 128, picked, found)
        pieces.append(found)
    weight = jnp.concatenate(pieces, axis=1)
    values = [weight * taps_ref[pl.ds(tap, 1), :] for tap in range(taps_ref.shape[0])]
    offsets = jnp.concatenate([offsets_ref[pl.ds(piece, 1), :] for piece in range(samples // 128)], axis=1)

    rows = 16
    cell = lax.broadcasted_iota(jnp.int32, (rows, samples), 0)
    starts = [jnp.broadcast_to(offsets + index, (rows, samples)) for index in range(len(values))]
    values = [jnp.broadcast_to(value, (rows, samples)) for value in values]
    for first in range(0, block_size, rows):
        here = cell + first
        spread = jnp.zeros((rows, samples), jnp.float32)
        for start, value in zip(starts, values):
            spread = jnp.where(here == start, value, spread)
        spread_ref[pl.ds(first, rows), :] = spread.astype(jnp.bfloat16)


def make_angles(first_column, step_cos_ref, step_sin_ref, part_cos_ref, part_sin_ref):
    block_size = step_cos_ref.shape[1]
    freq = lax.axis_index("ang") * block_size + lax.broadcasted_iota(jnp.int32, (8, block_size), 1)
    row = lax.broadcasted_iota(jnp.int32, (8, block_size), 0)
    for first in range(0, CHUNK // 8, 8):
        step_cos_ref[pl.ds(first, 8), :], step_sin_ref[pl.ds(first, 8), :] = unit_circle(-freq * (8 * (row + first)))
    for first in range(0, part_cos_ref.shape[0], 8):
        part_cos_ref[pl.ds(first, 8), :], part_sin_ref[pl.ds(first, 8), :] = unit_circle(
            -freq * (CHUNK * (row + first))
        )
    return unit_circle(-freq * (first_column + row))


def make_waves(base, part, count, step_cos_ref, step_sin_ref, part_cos_ref, part_sin_ref, put):
    base_cos, base_sin = base
    part_cos, part_sin = part_cos_ref[pl.ds(part, 1), :], part_sin_ref[pl.ds(part, 1), :]
    here_cos = base_cos * part_cos - base_sin * part_sin
    here_sin = base_sin * part_cos + base_cos * part_sin
    for step in range(0, pl.cdiv(count, 8), 2):
        pair_cos, pair_sin = [], []
        for one in (step, step + 1):
            step_cos, step_sin = step_cos_ref[pl.ds(one, 1), :], step_sin_ref[pl.ds(one, 1), :]
            pair_cos.append(here_cos * step_cos - here_sin * step_sin)
            pair_sin.append(here_sin * step_cos + here_cos * step_sin)
        put(
            8 * step,
            jnp.concatenate(pair_cos, axis=0).astype(jnp.bfloat16),
            jnp.concatenate(pair_sin, axis=0).astype(jnp.bfloat16),
        )


def chunks(total):
    return [(part, part * CHUNK, min(CHUNK, total - part * CHUNK)) for part in range(pl.cdiv(total, CHUNK))]


def put_windows(out_ref, first, count, sent):
    dests, window, _ = out_ref.shape
    block = window - 2 * HALO
    for dest in range(dests):
        low, high = max(first, dest * block), min(first + count, dest * block + window)
        if low < high:
            out_ref[dest, pl.ds(low - dest * block, high - low), :] = sent[low - first : high - first]


def project_kernel(
    data_ref, offsets_ref, view_ref, taps_ref, weight_ref, volume_ref, multiplier_ref,
    out_ref,
    spread_ref, grid_ref, cos_ref, sin_ref, step_cos_ref, step_sin_ref, part_cos_ref, part_sin_ref, lines_ref, vm_ref,
):
    ang, gx = lax.axis_index("ang"), lax.axis_index("gx")
    lines = data_ref.shape[0] // 2
    local_lines, columns = volume_ref.shape

    make_spread(offsets_ref, view_ref, taps_ref, weight_ref, spread_ref)
    grid_ref[...] = lax.dot_general(
        data_ref[...], spread_ref[...], NT, preferred_element_type=jnp.float32
    ).astype(jnp.bfloat16)

    lines_ref[...] = jnp.zeros_like(lines_ref)
    lines_ref[pl.ds(pl.multiple_of(ang * local_lines, 8), local_lines), :] = volume_ref[...] + multiplier_ref[...]
    vm_ref[pl.ds(0, HALO), :] = jnp.zeros((HALO, lines), jnp.float32)
    vm_ref[pl.ds(HALO + columns, HALO), :] = jnp.zeros((HALO, lines), jnp.float32)
    for first in range(0, columns, 128):
        vm_ref[pl.ds(HALO + first, 128), :] = lines_ref[:, pl.ds(first, 128)].T

    angles = (step_cos_ref, step_sin_ref, part_cos_ref, part_sin_ref)
    base = make_angles(gx * columns - HALO, *angles)
    for part, first, count in chunks(columns + 2 * HALO):
        slot = part % 2

        def put(at, cosines, sines):
            cos_ref[slot, pl.ds(at, 16), :] = cosines
            sin_ref[slot, pl.ds(at, 16), :] = sines

        make_waves(base, part, count, *angles, put)
        made = max(16, count)
        total_part = lax.dot_general(
            cos_ref[slot, pl.ds(0, made), :], grid_ref[pl.ds(0, lines), :], NT, preferred_element_type=jnp.float32
        ) + lax.dot_general(
            sin_ref[slot, pl.ds(0, made), :], grid_ref[pl.ds(lines, lines), :], NT, preferred_element_type=jnp.float32
        )
        put_windows(out_ref, first, count, vm_ref[pl.ds(first, count), :] - total_part[:count] * NX ** (-0.5))


def project(data, offsets, view_index, taps, view_weight, volume, multiplier, dests):
    lines = data.shape[0] // 2
    samples = data.shape[1]
    columns = volume.shape[1]
    block_size = NX // lax.axis_size("ang")
    window = columns // dests + 2 * HALO
    parts = pl.cdiv(columns + 2 * HALO, CHUNK)
    vmem = pl.BlockSpec(memory_space=pltpu.VMEM)
    return pl.pallas_call(
        project_kernel,
        out_shape=pltpu.VMEM((dests, window, lines), jnp.float32),
        in_specs=[vmem] * 7,
        out_specs=vmem,
        scratch_shapes=[
            pltpu.VMEM((block_size, samples), jnp.bfloat16),
            pltpu.VMEM((2 * lines, block_size), jnp.bfloat16),
            pltpu.VMEM((2, CHUNK, block_size), jnp.bfloat16),
            pltpu.VMEM((2, CHUNK, block_size), jnp.bfloat16),
            pltpu.VMEM((CHUNK // 8, block_size), jnp.float32),
            pltpu.VMEM((CHUNK // 8, block_size), jnp.float32),
            pltpu.VMEM((8 * pl.cdiv(parts, 8), block_size), jnp.float32),
            pltpu.VMEM((8 * pl.cdiv(parts, 8), block_size), jnp.float32),
            pltpu.VMEM((lines, columns), jnp.float32),
            pltpu.VMEM((columns + 2 * HALO, lines), jnp.float32),
        ],
        cost_estimate=pl.CostEstimate(flops=4 * 10**9, transcendentals=0, bytes_accessed=10**6),
        compiler_params=pltpu.CompilerParams(vmem_limit_bytes=VMEM_LIMIT),
        name="project",
    )(data, offsets, view_index, taps, view_weight, volume, multiplier)


def close_kernel(parts_ref, inner_ref, outer_ref, out_ref, halo_ref):
    ang = lax.axis_index("ang")
    even = lax.axis_index("gx") % 2 == 0
    dests, window, _ = parts_ref.shape
    local_lines = inner_ref.shape[0]
    halo_ref[...] = jnp.zeros_like(halo_ref)
    own = pl.ds(pl.multiple_of(ang * local_lines, 8), local_lines)
    inner, outer = inner_ref[...], outer_ref[...]
    halo_ref[own, pl.ds(0, HALO)] = jnp.where(even, outer, inner)
    halo_ref[own, pl.ds(HALO, HALO)] = jnp.where(even, inner, outer)
    edges = halo_ref[...].T
    out_ref[0, pl.ds(0, HALO), :] = parts_ref[0, pl.ds(0, HALO), :] + edges[:HALO]
    last = pl.ds(window - HALO, HALO)
    out_ref[dests - 1, last, :] = parts_ref[dests - 1, last, :] + edges[HALO : 2 * HALO]


def close(parts, inner, outer):
    vmem = pl.BlockSpec(memory_space=pltpu.VMEM)
    return pl.pallas_call(
        close_kernel,
        out_shape=pltpu.VMEM(parts.shape, parts.dtype),
        in_specs=[vmem] * 3,
        out_specs=vmem,
        scratch_shapes=[pltpu.VMEM((parts.shape[2], 128), jnp.float32)],
        input_output_aliases={0: 0},
        compiler_params=pltpu.CompilerParams(vmem_limit_bytes=VMEM_LIMIT),
        name="close",
    )(parts, inner, outer)


def smooth_kernel(planes, columns, *refs):
    *parts_refs, out_ref, done_ref = refs
    _, local_lines, block = out_ref.shape
    window = parts_refs[0].shape[-2]
    angs, groups = lax.axis_size("ang"), lax.axis_size("gy")
    lines = angs * local_lines
    rows = lines // planes
    size = min(PIECE, window)
    pieces = [(first, min(size, window - first)) for first in range(0, window, size)]
    tiles = len(pieces)
    lanes = [lax.broadcasted_iota(jnp.int32, (height, lines), 1) for _, height in pieces]
    inside = lax.broadcasted_iota(jnp.int32, (8, lines), 0)
    plane_opens = [lane // rows < planes - 1 for lane in lanes]
    row_firsts = [lane % rows == 0 for lane in lanes]
    row_lasts = [lane % rows == rows - 1 for lane in lanes]
    place = lax.axis_index("gy") * angs + lax.axis_index("ang")
    first_column = lax.axis_index("gx") * columns + place * block - HALO
    zero = jnp.float32(0.0)

    def part(ang, group, tile):
        at = pl.ds(*pieces[tile])
        if len(parts_refs) > 1:
            return parts_refs[ang][at, pl.ds(group * lines, lines)]
        return parts_refs[0][group * angs + ang, at, :]

    source = [[sum((part(ang, group, tile) for ang in range(1, angs)), part(0, group, tile)) for group in range(groups)]
              for tile in range(tiles)]

    def divergence(flow, tile):
        rolled = [pltpu.roll(flow[tile][group][1], 1, 1) for group in range(groups)]
        result = []
        for group in range(groups):
            f0, f1, f2 = flow[tile][group]
            wrapped = pltpu.roll(flow[tile][group - 1][1], lines - (rows - 1), 1)
            lower_row = jnp.where(row_firsts[tile], wrapped, rolled[group])
            lower_cell = pltpu.roll(f2, 1, 0)
            if tile > 0:
                before = flow[tile - 1][group][2]
                opening = jnp.where(inside == 0, pltpu.roll(before[-8:], 1, 0), lower_cell[:8])
                lower_cell = jnp.concatenate([opening, lower_cell[8:]], axis=0)
            result.append((f0 - pltpu.roll(f0, rows, 1)) + (f1 - lower_row) + (f2 - lower_cell))
        return result

    def target_of(flow, tile):
        scaled = [value * (dual_step / smooth_weight) for value in source[tile]]
        if flow is None:
            return [-value for value in scaled]
        return [dual_step * div - value for div, value in zip(divergence(flow, tile), scaled)]

    flow = None
    for _ in range(TV_STEPS):
        updated = []
        after = target_of(flow, 0)
        for tile in range(tiles):
            target = after
            after = target_of(flow, tile + 1) if tile + 1 < tiles else target
            _, height = pieces[tile]
            plane_open, row_last = plane_opens[tile], row_lasts[tile]
            moved_groups = []
            for group in range(groups):
                here = target[group]
                slope_plane = jnp.where(plane_open, pltpu.roll(here, lines - rows, 1) - here, zero)
                upper_row = pltpu.roll(here, lines - 1, 1)
                if group + 1 < groups:
                    slope_row = jnp.where(row_last, pltpu.roll(target[group + 1], rows - 1, 1), upper_row) - here
                else:
                    slope_row = jnp.where(row_last, zero, upper_row - here)
                upper_cell = pltpu.roll(here, height - 1, 0)
                if tile + 1 < tiles:
                    closing = jnp.where(inside == 7, pltpu.roll(after[group][:8], 7, 0), upper_cell[-8:])
                    upper_cell = jnp.concatenate([upper_cell[:-8], closing], axis=0)
                slope_cell = upper_cell - here
                if tile == 0:
                    opening = jnp.where(first_column + inside >= 0, slope_cell[:8], zero)
                    slope_cell = jnp.concatenate([opening, slope_cell[8:]], axis=0)
                if tile == tiles - 1:
                    column = first_column + window - 8 + inside
                    closing = jnp.where(column < NX - 1, slope_cell[-8:], zero)
                    slope_cell = jnp.concatenate([slope_cell[:-8], closing], axis=0)
                square = slope_plane * slope_plane + slope_row * slope_row + slope_cell * slope_cell
                scale = 1.0 / (1.0 + square * lax.rsqrt(jnp.maximum(square, 1e-30)))
                moved = [slope_plane, slope_row, slope_cell]
                if flow is not None:
                    moved = [f + m for f, m in zip(flow[tile][group], moved)]
                moved_groups.append([m * scale for m in moved])
            updated.append(moved_groups)
        flow = updated
    for tile in range(tiles):
        for group, div in enumerate(divergence(flow, tile)):
            done_ref[group, pl.ds(*pieces[tile]), :] = source[tile][group] - smooth_weight * div
    for group in range(groups):
        turned = done_ref[group, pl.ds(HALO, block), :].T
        for ang in range(angs):
            out_ref[group * angs + ang] = turned[ang * local_lines : (ang + 1) * local_lines]


def smooth(parts, planes, local_lines, columns):
    window = parts[0].shape[-2]
    dests = lax.axis_size("ang") * lax.axis_size("gy")
    vmem = pl.BlockSpec(memory_space=pltpu.VMEM)
    return pl.pallas_call(
        functools.partial(smooth_kernel, planes, columns),
        out_shape=pltpu.VMEM((dests, local_lines, window - 2 * HALO), jnp.float32),
        in_specs=[vmem] * len(parts),
        out_specs=vmem,
        scratch_shapes=[
            pltpu.VMEM((lax.axis_size("gy"), window, lax.axis_size("ang") * local_lines), jnp.float32)
        ],
        compiler_params=pltpu.CompilerParams(vmem_limit_bytes=VMEM_LIMIT),
        name="smooth",
    )(*parts)


def exchanged(block, axis, shift):
    count = lax.axis_size(axis)
    route = []
    for low in range(shift, count + shift - 1, 2):
        pair = (low % count, (low + 1) % count)
        route += [pair, pair[::-1]]
    return lax.ppermute(block, axis, route)


def line_places(lines, local_lines):
    gy, inner = lax.axis_index("gy"), lax.axis_index("ang") * local_lines
    return [
        pl.ds(pl.multiple_of(group * lines + inner, 8), local_lines) for group in (gy, 1 - gy)
    ]


def pack_kernel(
    data_ref, offsets_ref, view_ref, taps_ref, weight_ref, volume_ref, multiplier_ref,
    sent_ref, data_out, offsets_out, view_out, taps_out, weight_out, own_ref, wave_ref, edge_ref, edge_sent_ref,
    volume_here, multiplier_here, step_cos_ref, step_sin_ref, part_cos_ref, part_sin_ref, lines_ref, sems,
):
    rows = data_ref.shape[0]
    lines = rows // 2
    local_lines, columns = volume_ref.shape
    half = columns // 2
    block_size = wave_ref.shape[1] // 2
    gx, gy = lax.axis_index("gx"), lax.axis_index("gy")
    first_core = gy == 0
    pairs = (
        (volume_ref, volume_here),
        (multiplier_ref, multiplier_here),
        (data_ref, data_out),
        (offsets_ref, offsets_out),
        (view_ref, view_out),
        (taps_ref, taps_out),
        (weight_ref, weight_out),
    )
    copies = [pltpu.make_async_copy(source, target, sems.at[at]) for at, (source, target) in enumerate(pairs)]
    for copy in copies:
        copy.start()

    lines_ref[...] = jnp.zeros_like(lines_ref)
    angles = (step_cos_ref, step_sin_ref, part_cos_ref, part_sin_ref)
    base = make_angles(gx * columns + gy * half - HALO, *angles)
    for part, first, count in chunks(half + 2 * HALO):

        def put(at, cosines, sines):
            wave_ref[pl.ds(first + at, 16), pl.ds(0, block_size)] = cosines
            wave_ref[pl.ds(first + at, 16), pl.ds(block_size, block_size)] = sines

        make_waves(base, part, count, *angles, put)

    copies[0].wait()
    copies[1].wait()
    low = volume_here[:, pl.ds(0, half)] + multiplier_here[:, pl.ds(0, half)]
    high = volume_here[:, pl.ds(half, half)] + multiplier_here[:, pl.ds(half, half)]
    outer = (low[:, :HALO], high[:, half - HALO :])
    place = line_places(lines, local_lines)[0]
    lines_ref[place, pl.ds(0, HALO)] = jnp.where(first_core, outer[0], outer[1])
    lines_ref[place, pl.ds(8, HALO)] = jnp.where(first_core, outer[1], outer[0])
    for group in range(2):
        group_lines = pl.ds(group * lines, lines)
        turned = lines_ref[group_lines, :].T
        edge_ref[:, group_lines] = turned[:8]
        edge_sent_ref[:, group_lines] = turned[8:16]

    below, above = low[:, half - HALO :], high[:, :HALO]
    own_ref[:, pl.ds(0, half)] = jnp.where(first_core, low, high)
    own_ref[:, pl.ds(half, HALO)] = jnp.where(first_core, above, below)
    sent_ref[pl.ds(rows, local_lines), :] = jnp.where(first_core, high, low)
    sent_ref[pl.ds(rows + local_lines, local_lines), pl.ds(0, HALO)] = jnp.where(first_core, below, above)
    copies[2].wait()
    sent_ref[pl.ds(0, rows), :] = data_out[...].astype(jnp.float32)
    for copy in copies[3:]:
        copy.wait()


def pack(data, offsets, view_index, taps, view_weight, volume, multiplier):
    rows, samples = data.shape
    local_lines, columns = volume.shape
    block_size = NX // lax.axis_size("ang")
    made = 16 * pl.cdiv(columns // 2 + 2 * HALO, 16)
    parts = 8 * pl.cdiv(pl.cdiv(columns // 2 + 2 * HALO, CHUNK), 8)
    vmem = pl.BlockSpec(memory_space=pltpu.VMEM)
    return pl.pallas_call(
        pack_kernel,
        out_shape=[
            pltpu.VMEM((rows + 2 * local_lines, samples), jnp.float32),
            pltpu.VMEM(data.shape, data.dtype),
            pltpu.VMEM(offsets.shape, offsets.dtype),
            pltpu.VMEM(view_index.shape, view_index.dtype),
            pltpu.VMEM(taps.shape, taps.dtype),
            pltpu.VMEM(view_weight.shape, view_weight.dtype),
            pltpu.VMEM((local_lines, columns // 2 + 128), jnp.float32),
            pltpu.VMEM((made, 2 * block_size), jnp.bfloat16),
            pltpu.VMEM((8, rows), jnp.float32),
            pltpu.VMEM((8, rows), jnp.float32),
        ],
        in_specs=[pl.BlockSpec(memory_space=pltpu.HBM)] * 7,
        out_specs=[vmem] * 10,
        scratch_shapes=[
            pltpu.VMEM(volume.shape, volume.dtype),
            pltpu.VMEM(multiplier.shape, multiplier.dtype),
            pltpu.VMEM((CHUNK // 8, block_size), jnp.float32),
            pltpu.VMEM((CHUNK // 8, block_size), jnp.float32),
            pltpu.VMEM((parts, block_size), jnp.float32),
            pltpu.VMEM((parts, block_size), jnp.float32),
            pltpu.VMEM((rows, 128), jnp.float32),
            pltpu.SemaphoreType.DMA((7,)),
        ],
        compiler_params=pltpu.CompilerParams(vmem_limit_bytes=VMEM_LIMIT),
        name="pack",
    )(
        *(
            pltpu.with_memory_space_constraint(array, pltpu.HBM)
            for array in (data, offsets, view_index, taps, view_weight, volume, multiplier)
        )
    )


def spread_of(offsets, view_index, taps, view_weight):
    block_size = NX // lax.axis_size("ang")
    vmem = pl.BlockSpec(memory_space=pltpu.VMEM)
    return pl.pallas_call(
        make_spread,
        out_shape=pltpu.VMEM((block_size, taps.shape[1]), jnp.bfloat16),
        in_specs=[vmem] * 4,
        out_specs=vmem,
        cost_estimate=pl.CostEstimate(flops=2 * 10**9, transcendentals=0, bytes_accessed=10**6),
        compiler_params=pltpu.CompilerParams(vmem_limit_bytes=VMEM_LIMIT),
        name="spread",
    )(offsets, view_index, taps, view_weight)


def grid_kernel(data_ref, own_ref, got_ref, spread_ref, grid_ref, vm_ref, both_ref, lines_ref):
    rows = data_ref.shape[0]
    lines = rows // 2
    block_size = spread_ref.shape[0]
    local_lines, columns = own_ref.shape[0], own_ref.shape[1] - 128
    gy = lax.axis_index("gy")
    for component in range(2):
        for group, ref in ((gy, data_ref), (1 - gy, got_ref)):
            place = pl.multiple_of((2 * component + group) * lines, 16)
            both_ref[pl.ds(place, lines), :] = ref[pl.ds(component * lines, lines), :].astype(jnp.bfloat16)
    for component in range(2):
        grid_ref[pl.ds(component * block_size, block_size), :] = lax.dot_general(
            spread_ref[...],
            both_ref[pl.ds(2 * component * lines, 2 * lines), :],
            NT,
            preferred_element_type=jnp.float32,
        ).astype(jnp.bfloat16)

    lines_ref[...] = jnp.zeros_like(lines_ref)
    own_place, other_place = line_places(lines, local_lines)
    side = pl.ds(columns, HALO)
    lines_ref[own_place, pl.ds(0, columns)] = own_ref[:, pl.ds(0, columns)]
    lines_ref[own_place, side] = own_ref[:, side]
    lines_ref[other_place, pl.ds(0, columns)] = got_ref[pl.ds(rows, local_lines), :]
    lines_ref[other_place, side] = got_ref[pl.ds(rows + local_lines, local_lines), pl.ds(0, HALO)]
    for group in range(2):
        group_lines = pl.ds(group * lines, lines)
        inner = lines_ref[group_lines, pl.ds(columns, 128)].T[:HALO]
        vm_ref[pl.ds(0, HALO), group_lines] = jnp.where(gy == 0, 0.0, inner)
        vm_ref[pl.ds(HALO + columns, HALO), group_lines] = jnp.where(gy == 0, inner, 0.0)
        for first in range(0, columns, 128):
            vm_ref[pl.ds(HALO + first, 128), group_lines] = lines_ref[group_lines, pl.ds(first, 128)].T


def grid(data, own, got, spread):
    lines = data.shape[0] // 2
    columns = own.shape[1] - 128
    vmem = pl.BlockSpec(memory_space=pltpu.VMEM)
    return pl.pallas_call(
        grid_kernel,
        out_shape=[
            pltpu.VMEM((2 * spread.shape[0], 2 * lines), jnp.bfloat16),
            pltpu.VMEM((columns + 2 * HALO, 2 * lines), jnp.float32),
        ],
        in_specs=[vmem] * 4,
        out_specs=[vmem] * 2,
        scratch_shapes=[
            pltpu.VMEM((4 * lines, data.shape[1]), jnp.bfloat16),
            pltpu.VMEM((2 * lines, columns + 128), jnp.float32),
        ],
        cost_estimate=pl.CostEstimate(flops=10**9, transcendentals=0, bytes_accessed=10**6),
        compiler_params=pltpu.CompilerParams(vmem_limit_bytes=VMEM_LIMIT),
        name="grid",
    )(data, own, got, spread)


def block_kernel(apart, wave_ref, grid_ref, vm_ref, edge_ref, out_ref):
    window = out_ref.shape[0]
    block = window - 2 * HALO
    angs = lax.axis_size("ang")
    dest = lax.axis_index("ang") ^ apart
    gy = lax.axis_index("gy")
    first = pl.multiple_of(dest * block, 16)
    made = 16 * pl.cdiv(window, 16)
    total = jnp.dot(wave_ref[pl.ds(first, made), :], grid_ref[...], preferred_element_type=jnp.float32)
    out_ref[...] = vm_ref[pl.ds(first, window), :] - total[:window] * NX ** (-0.5)
    edge = edge_ref[...][:HALO]
    opens = jnp.logical_and(dest == 0, gy == 0)
    out_ref[pl.ds(0, HALO), :] += jnp.where(opens, edge, 0.0)
    closes = jnp.logical_and(dest == angs - 1, gy == 1)
    out_ref[pl.ds(window - HALO, HALO), :] += jnp.where(closes, edge, 0.0)


def block_of(apart, wave, grid, vm, got_edge):
    window = (vm.shape[0] - 2 * HALO) // lax.axis_size("ang") + 2 * HALO
    vmem = pl.BlockSpec(memory_space=pltpu.VMEM)
    return pl.pallas_call(
        functools.partial(block_kernel, apart),
        out_shape=pltpu.VMEM((window, vm.shape[1]), jnp.float32),
        in_specs=[vmem] * 4,
        out_specs=vmem,
        cost_estimate=pl.CostEstimate(flops=10**9, transcendentals=0, bytes_accessed=10**6),
        compiler_params=pltpu.CompilerParams(vmem_limit_bytes=VMEM_LIMIT),
    )(wave, grid, vm, got_edge)


def on_chip(*arrays):
    return [pltpu.with_memory_space_constraint(array, pltpu.VMEM) for array in arrays]


def project_paired(data, offsets, view_index, taps, view_weight, volume, multiplier):
    sent, data, offsets, view_index, taps, view_weight, own, wave, near, near_sent = pack(
        data, offsets, view_index, taps, view_weight, volume, multiplier
    )
    near_got = lax.ppermute(near_sent, "gy", [(0, 1), (1, 0)])
    got = lax.ppermute(sent, "gy", [(0, 1), (1, 0)])
    spread = spread_of(*on_chip(offsets, view_index, taps, view_weight))
    count = lax.axis_size("gx")
    route = []
    angs = lax.axis_size("ang")
    for ang in range(angs):
        for low in range(count - 1):
            pair = ((2 * ang + 1) * count + low, 2 * ang * count + low + 1)
            route += [pair, pair[::-1]]
        beside = ang ^ 1 if angs > 1 else ang
        route.append((2 * ang * count, 2 * beside * count))
        route.append(((2 * ang + 2) * count - 1, (2 * beside + 2) * count - 1))
    got_edge = lax.ppermute(near + near_got, ("ang", "gy", "gx"), route)
    gridded, vm = grid(*on_chip(data, own, got, spread))
    wave, gridded, vm, got_edge = on_chip(wave, gridded, vm, got_edge)
    parts = []
    for apart in range(angs - 1, 0, -1):
        part = block_of(apart, wave, gridded, vm, got_edge)
        parts.append(lax.ppermute(part, "ang", [(ang, ang ^ apart) for ang in range(angs)]))
    return [block_of(0, wave, gridded, vm, got_edge)] + parts


def per_device(spectrum_data, offsets, view_index, kernel, view_weight, volume, multiplier):
    local_planes, rows, columns = volume.shape
    planes = spectrum_data.shape[1]
    samples = spectrum_data.shape[3]
    dests = lax.axis_size("ang") * lax.axis_size("gy")
    local_lines = local_planes * rows
    lines = planes * rows

    volume = volume.reshape(local_lines, columns)
    multiplier = multiplier.reshape(local_lines, columns)
    arrays = (
        spectrum_data.reshape(2 * lines, samples),
        offsets.reshape(samples // 128, 128),
        view_index.reshape(samples // 128, 128),
        kernel,
        view_weight,
        volume,
        multiplier,
    )
    angs = lax.axis_size("ang")
    if lax.axis_size("gy") == 2 and columns // 2 == samples and angs & (angs - 1) == 0:
        parts = project_paired(*arrays)
    else:
        first_edge = volume[:, :HALO] + multiplier[:, :HALO]
        last_edge = volume[:, -HALO:] + multiplier[:, -HALO:]
        even = lax.axis_index("gx") % 2 == 0
        inner = exchanged(jnp.where(even, last_edge, first_edge), "gx", 0)
        outer = exchanged(jnp.where(even, first_edge, last_edge), "gx", 1)
        parts = close(project(*arrays, dests), *on_chip(inner, outer))
        parts = [lax.all_to_all(parts, ("gy", "ang"), split_axis=0, concat_axis=0)]
    done = smooth(on_chip(*parts), planes, local_lines, columns)
    done = lax.all_to_all(done, ("gy", "ang"), split_axis=0, concat_axis=0)
    done = done.reshape(done.shape[0], local_planes, rows, done.shape[2])
    return jnp.transpose(done, (1, 2, 0, 3)).reshape(local_planes, rows, columns)


def solution(mesh):
    placed = (
        P(None, None, "gy", "ang"),
        P("ang"),
        P("ang"),
        P(None, "ang"),
        P(),
        P("ang", "gy", "gx"),
        P("ang", "gy", "gx"),
    )
    return jax.shard_map(per_device, mesh=mesh, in_specs=placed, out_specs=P("ang", "gy", "gx"), check_vma=False)
```

```python
import functools
import math

import jax
import jax.numpy as jnp
from jax import lax
from jax.experimental import pallas as pl
from jax.experimental.pallas import tpu as pltpu
from jax.sharding import PartitionSpec as P


NX = 4096
TV_STEPS = 4
HALO = TV_STEPS
CHUNK = 128
PIECE = 72
VMEM_LIMIT = 24 * 2**20

smooth_weight = 0.5
dual_step = 1.0 / 12.0

NT = (((1,), (1,)), ((), ()))


def unit_circle(phase):
    phase = phase & (NX - 1)
    quarter = (phase + NX // 8) // (NX // 4)
    angle = (phase - quarter * (NX // 4)).astype(jnp.float32) * (2.0 * math.pi / NX)
    square = angle * angle
    sine = angle * (1.0 + square * (-1.0 / 6 + square * (1.0 / 120 + square * (-1.0 / 5040 + square * (1.0 / 362880)))))
    cosine = 1.0 + square * (-0.5 + square * (1.0 / 24 + square * (-1.0 / 720 + square * (1.0 / 40320))))
    odd = (quarter & 1) == 1
    first = jnp.where(odd, -sine, cosine)
    second = jnp.where(odd, cosine, sine)
    flip = (quarter & 2) == 2
    return jnp.where(flip, -first, first), jnp.where(flip, -second, second)


def make_spread(offsets_ref, view_ref, taps_ref, weight_ref, spread_ref):
    block_size, samples = spread_ref.shape
    views = weight_ref.shape[0]
    pieces = []
    for piece in range(samples // 128):
        view = view_ref[pl.ds(piece, 1), :]
        found = jnp.zeros((1, 128), jnp.float32)
        lane = jnp.broadcast_to(view & 127, (8, 128))
        for first in range(0, views, 128):
            table = weight_ref[pl.ds(first, min(128, views - first))].reshape(1, -1)
            if views - first < 128:
                table = jnp.concatenate([table, jnp.zeros((1, 128 - (views - first)), jnp.float32)], axis=1)
            picked = jnp.take_along_axis(jnp.broadcast_to(table, (8, 128)), lane, axis=1)[:1]
            found = jnp.where(view // 128 == first // 128, picked, found)
        pieces.append(found)
    weight = jnp.concatenate(pieces, axis=1)
    values = [weight * taps_ref[pl.ds(tap, 1), :] for tap in range(taps_ref.shape[0])]
    offsets = jnp.concatenate([offsets_ref[pl.ds(piece, 1), :] for piece in range(samples // 128)], axis=1)

    rows = 16
    cell = lax.broadcasted_iota(jnp.int32, (rows, samples), 0)
    starts = [jnp.broadcast_to(offsets + index, (rows, samples)) for index in range(len(values))]
    values = [jnp.broadcast_to(value, (rows, samples)) for value in values]
    for first in range(0, block_size, rows):
        here = cell + first
        spread = jnp.zeros((rows, samples), jnp.float32)
        for start, value in zip(starts, values):
            spread = jnp.where(here == start, value, spread)
        spread_ref[pl.ds(first, rows), :] = spread.astype(jnp.bfloat16)


def make_angles(first_column, step_cos_ref, step_sin_ref, part_cos_ref, part_sin_ref):
    block_size = step_cos_ref.shape[1]
    freq = lax.axis_index("ang") * block_size + lax.broadcasted_iota(jnp.int32, (8, block_size), 1)
    row = lax.broadcasted_iota(jnp.int32, (8, block_size), 0)
    for first in range(0, CHUNK // 8, 8):
        step_cos_ref[pl.ds(first, 8), :], step_sin_ref[pl.ds(first, 8), :] = unit_circle(-freq * (8 * (row + first)))
    for first in range(0, part_cos_ref.shape[0], 8):
        part_cos_ref[pl.ds(first, 8), :], part_sin_ref[pl.ds(first, 8), :] = unit_circle(
            -freq * (CHUNK * (row + first))
        )
    return unit_circle(-freq * (first_column + row))


def make_waves(base, part, count, step_cos_ref, step_sin_ref, part_cos_ref, part_sin_ref, put):
    base_cos, base_sin = base
    part_cos, part_sin = part_cos_ref[pl.ds(part, 1), :], part_sin_ref[pl.ds(part, 1), :]
    here_cos = base_cos * part_cos - base_sin * part_sin
    here_sin = base_sin * part_cos + base_cos * part_sin
    for step in range(0, pl.cdiv(count, 8), 2):
        pair_cos, pair_sin = [], []
        for one in (step, step + 1):
            step_cos, step_sin = step_cos_ref[pl.ds(one, 1), :], step_sin_ref[pl.ds(one, 1), :]
            pair_cos.append(here_cos * step_cos - here_sin * step_sin)
            pair_sin.append(here_sin * step_cos + here_cos * step_sin)
        put(
            8 * step,
            jnp.concatenate(pair_cos, axis=0).astype(jnp.bfloat16),
            jnp.concatenate(pair_sin, axis=0).astype(jnp.bfloat16),
        )


def chunks(total):
    return [(part, part * CHUNK, min(CHUNK, total - part * CHUNK)) for part in range(pl.cdiv(total, CHUNK))]


def put_windows(out_ref, first, count, sent):
    dests, window, _ = out_ref.shape
    block = window - 2 * HALO
    for dest in range(dests):
        low, high = max(first, dest * block), min(first + count, dest * block + window)
        if low < high:
            out_ref[dest, pl.ds(low - dest * block, high - low), :] = sent[low - first : high - first]


def project_kernel(
    data_ref, offsets_ref, view_ref, taps_ref, weight_ref, volume_ref, multiplier_ref,
    out_ref,
    spread_ref, grid_ref, cos_ref, sin_ref, step_cos_ref, step_sin_ref, part_cos_ref, part_sin_ref, lines_ref, vm_ref,
):
    ang, gx = lax.axis_index("ang"), lax.axis_index("gx")
    lines = data_ref.shape[0] // 2
    local_lines, columns = volume_ref.shape

    make_spread(offsets_ref, view_ref, taps_ref, weight_ref, spread_ref)
    grid_ref[...] = lax.dot_general(
        data_ref[...], spread_ref[...], NT, preferred_element_type=jnp.float32
    ).astype(jnp.bfloat16)

    lines_ref[...] = jnp.zeros_like(lines_ref)
    lines_ref[pl.ds(pl.multiple_of(ang * local_lines, 8), local_lines), :] = volume_ref[...] + multiplier_ref[...]
    vm_ref[pl.ds(0, HALO), :] = jnp.zeros((HALO, lines), jnp.float32)
    vm_ref[pl.ds(HALO + columns, HALO), :] = jnp.zeros((HALO, lines), jnp.float32)
    for first in range(0, columns, 128):
        vm_ref[pl.ds(HALO + first, 128), :] = lines_ref[:, pl.ds(first, 128)].T

    angles = (step_cos_ref, step_sin_ref, part_cos_ref, part_sin_ref)
    base = make_angles(gx * columns - HALO, *angles)
    for part, first, count in chunks(columns + 2 * HALO):
        slot = part % 2

        def put(at, cosines, sines):
            cos_ref[slot, pl.ds(at, 16), :] = cosines
            sin_ref[slot, pl.ds(at, 16), :] = sines

        make_waves(base, part, count, *angles, put)
        made = max(16, count)
        total_part = lax.dot_general(
            cos_ref[slot, pl.ds(0, made), :], grid_ref[pl.ds(0, lines), :], NT, preferred_element_type=jnp.float32
        ) + lax.dot_general(
            sin_ref[slot, pl.ds(0, made), :], grid_ref[pl.ds(lines, lines), :], NT, preferred_element_type=jnp.float32
        )
        put_windows(out_ref, first, count, vm_ref[pl.ds(first, count), :] - total_part[:count] * NX ** (-0.5))


def project(data, offsets, view_index, taps, view_weight, volume, multiplier, dests):
    lines = data.shape[0] // 2
    samples = data.shape[1]
    columns = volume.shape[1]
    block_size = NX // lax.axis_size("ang")
    window = columns // dests + 2 * HALO
    parts = pl.cdiv(columns + 2 * HALO, CHUNK)
    vmem = pl.BlockSpec(memory_space=pltpu.VMEM)
    return pl.pallas_call(
        project_kernel,
        out_shape=pltpu.VMEM((dests, window, lines), jnp.float32),
        in_specs=[vmem] * 7,
        out_specs=vmem,
        scratch_shapes=[
            pltpu.VMEM((block_size, samples), jnp.bfloat16),
            pltpu.VMEM((2 * lines, block_size), jnp.bfloat16),
            pltpu.VMEM((2, CHUNK, block_size), jnp.bfloat16),
            pltpu.VMEM((2, CHUNK, block_size), jnp.bfloat16),
            pltpu.VMEM((CHUNK // 8, block_size), jnp.float32),
            pltpu.VMEM((CHUNK // 8, block_size), jnp.float32),
            pltpu.VMEM((8 * pl.cdiv(parts, 8), block_size), jnp.float32),
            pltpu.VMEM((8 * pl.cdiv(parts, 8), block_size), jnp.float32),
            pltpu.VMEM((lines, columns), jnp.float32),
            pltpu.VMEM((columns + 2 * HALO, lines), jnp.float32),
        ],
        cost_estimate=pl.CostEstimate(flops=4 * 10**9, transcendentals=0, bytes_accessed=10**6),
        compiler_params=pltpu.CompilerParams(vmem_limit_bytes=VMEM_LIMIT),
        name="project",
    )(data, offsets, view_index, taps, view_weight, volume, multiplier)


def close_kernel(parts_ref, inner_ref, outer_ref, out_ref, halo_ref):
    ang = lax.axis_index("ang")
    even = lax.axis_index("gx") % 2 == 0
    dests, window, _ = parts_ref.shape
    local_lines = inner_ref.shape[0]
    halo_ref[...] = jnp.zeros_like(halo_ref)
    own = pl.ds(pl.multiple_of(ang * local_lines, 8), local_lines)
    inner, outer = inner_ref[...], outer_ref[...]
    halo_ref[own, pl.ds(0, HALO)] = jnp.where(even, outer, inner)
    halo_ref[own, pl.ds(HALO, HALO)] = jnp.where(even, inner, outer)
    edges = halo_ref[...].T
    out_ref[0, pl.ds(0, HALO), :] = parts_ref[0, pl.ds(0, HALO), :] + edges[:HALO]
    last = pl.ds(window - HALO, HALO)
    out_ref[dests - 1, last, :] = parts_ref[dests - 1, last, :] + edges[HALO : 2 * HALO]


def close(parts, inner, outer):
    vmem = pl.BlockSpec(memory_space=pltpu.VMEM)
    return pl.pallas_call(
        close_kernel,
        out_shape=pltpu.VMEM(parts.shape, parts.dtype),
        in_specs=[vmem] * 3,
        out_specs=vmem,
        scratch_shapes=[pltpu.VMEM((parts.shape[2], 128), jnp.float32)],
        input_output_aliases={0: 0},
        compiler_params=pltpu.CompilerParams(vmem_limit_bytes=VMEM_LIMIT),
        name="close",
    )(parts, inner, outer)


def smooth_kernel(planes, columns, *refs):
    *parts_refs, out_ref, done_ref = refs
    _, local_lines, block = out_ref.shape
    window = parts_refs[0].shape[-2]
    angs, groups = lax.axis_size("ang"), lax.axis_size("gy")
    lines = angs * local_lines
    rows = lines // planes
    size = min(PIECE, window)
    pieces = [(first, min(size, window - first)) for first in range(0, window, size)]
    tiles = len(pieces)
    lanes = [lax.broadcasted_iota(jnp.int32, (height, lines), 1) for _, height in pieces]
    inside = lax.broadcasted_iota(jnp.int32, (8, lines), 0)
    plane_opens = [lane // rows < planes - 1 for lane in lanes]
    row_firsts = [lane % rows == 0 for lane in lanes]
    row_lasts = [lane % rows == rows - 1 for lane in lanes]
    place = lax.axis_index("gy") * angs + lax.axis_index("ang")
    first_column = lax.axis_index("gx") * columns + place * block - HALO
    zero = jnp.float32(0.0)

    def part(ang, group, tile):
        at = pl.ds(*pieces[tile])
        if len(parts_refs) > 1:
            return parts_refs[ang][at, pl.ds(group * lines, lines)]
        return parts_refs[0][group * angs + ang, at, :]

    source = [[sum((part(ang, group, tile) for ang in range(1, angs)), part(0, group, tile)) for group in range(groups)]
              for tile in range(tiles)]

    def divergence(flow, tile):
        rolled = [pltpu.roll(flow[tile][group][1], 1, 1) for group in range(groups)]
        result = []
        for group in range(groups):
            f0, f1, f2 = flow[tile][group]
            wrapped = pltpu.roll(flow[tile][group - 1][1], lines - (rows - 1), 1)
            lower_row = jnp.where(row_firsts[tile], wrapped, rolled[group])
            lower_cell = pltpu.roll(f2, 1, 0)
            if tile > 0:
                before = flow[tile - 1][group][2]
                opening = jnp.where(inside == 0, pltpu.roll(before[-8:], 1, 0), lower_cell[:8])
                lower_cell = jnp.concatenate([opening, lower_cell[8:]], axis=0)
            result.append((f0 - pltpu.roll(f0, rows, 1)) + (f1 - lower_row) + (f2 - lower_cell))
        return result

    def target_of(flow, tile):
        scaled = [value * (dual_step / smooth_weight) for value in source[tile]]
        if flow is None:
            return [-value for value in scaled]
        return [dual_step * div - value for div, value in zip(divergence(flow, tile), scaled)]

    flow = None
    for _ in range(TV_STEPS):
        updated = []
        after = target_of(flow, 0)
        for tile in range(tiles):
            target = after
            after = target_of(flow, tile + 1) if tile + 1 < tiles else target
            _, height = pieces[tile]
            plane_open, row_last = plane_opens[tile], row_lasts[tile]
            moved_groups = []
            for group in range(groups):
                here = target[group]
                slope_plane = jnp.where(plane_open, pltpu.roll(here, lines - rows, 1) - here, zero)
                upper_row = pltpu.roll(here, lines - 1, 1)
                if group + 1 < groups:
                    slope_row = jnp.where(row_last, pltpu.roll(target[group + 1], rows - 1, 1), upper_row) - here
                else:
                    slope_row = jnp.where(row_last, zero, upper_row - here)
                upper_cell = pltpu.roll(here, height - 1, 0)
                if tile + 1 < tiles:
                    closing = jnp.where(inside == 7, pltpu.roll(after[group][:8], 7, 0), upper_cell[-8:])
                    upper_cell = jnp.concatenate([upper_cell[:-8], closing], axis=0)
                slope_cell = upper_cell - here
                if tile == 0:
                    opening = jnp.where(first_column + inside >= 0, slope_cell[:8], zero)
                    slope_cell = jnp.concatenate([opening, slope_cell[8:]], axis=0)
                if tile == tiles - 1:
                    column = first_column + window - 8 + inside
                    closing = jnp.where(column < NX - 1, slope_cell[-8:], zero)
                    slope_cell = jnp.concatenate([slope_cell[:-8], closing], axis=0)
                square = slope_plane * slope_plane + slope_row * slope_row + slope_cell * slope_cell
                scale = 1.0 / (1.0 + square * lax.rsqrt(jnp.maximum(square, 1e-30)))
                moved = [slope_plane, slope_row, slope_cell]
                if flow is not None:
                    moved = [f + m for f, m in zip(flow[tile][group], moved)]
                moved_groups.append([m * scale for m in moved])
            updated.append(moved_groups)
        flow = updated
    for tile in range(tiles):
        for group, div in enumerate(divergence(flow, tile)):
            done_ref[group, pl.ds(*pieces[tile]), :] = source[tile][group] - smooth_weight * div
    for group in range(groups):
        turned = done_ref[group, pl.ds(HALO, block), :].T
        for ang in range(angs):
            out_ref[group * angs + ang] = turned[ang * local_lines : (ang + 1) * local_lines]


def smooth(parts, planes, local_lines, columns):
    window = parts[0].shape[-2]
    dests = lax.axis_size("ang") * lax.axis_size("gy")
    vmem = pl.BlockSpec(memory_space=pltpu.VMEM)
    return pl.pallas_call(
        functools.partial(smooth_kernel, planes, columns),
        out_shape=pltpu.VMEM((dests, local_lines, window - 2 * HALO), jnp.float32),
        in_specs=[vmem] * len(parts),
        out_specs=vmem,
        scratch_shapes=[
            pltpu.VMEM((lax.axis_size("gy"), window, lax.axis_size("ang") * local_lines), jnp.float32)
        ],
        compiler_params=pltpu.CompilerParams(vmem_limit_bytes=VMEM_LIMIT),
        name="smooth",
    )(*parts)


def exchanged(block, axis, shift):
    count = lax.axis_size(axis)
    route = []
    for low in range(shift, count + shift - 1, 2):
        pair = (low % count, (low + 1) % count)
        route += [pair, pair[::-1]]
    return lax.ppermute(block, axis, route)


def line_places(lines, local_lines):
    gy, inner = lax.axis_index("gy"), lax.axis_index("ang") * local_lines
    return [
        pl.ds(pl.multiple_of(group * lines + inner, 8), local_lines) for group in (gy, 1 - gy)
    ]


def pack_kernel(
    data_ref, offsets_ref, view_ref, taps_ref, weight_ref, volume_ref, multiplier_ref,
    sent_ref, data_out, offsets_out, view_out, taps_out, weight_out, own_ref, wave_ref, edge_ref, edge_sent_ref,
    volume_here, multiplier_here, step_cos_ref, step_sin_ref, part_cos_ref, part_sin_ref, lines_ref, sems,
):
    rows = data_ref.shape[0]
    lines = rows // 2
    local_lines, columns = volume_ref.shape
    half = columns // 2
    block_size = wave_ref.shape[1] // 2
    gx, gy = lax.axis_index("gx"), lax.axis_index("gy")
    first_core = gy == 0
    pairs = (
        (volume_ref, volume_here),
        (multiplier_ref, multiplier_here),
        (data_ref, data_out),
        (offsets_ref, offsets_out),
        (view_ref, view_out),
        (taps_ref, taps_out),
        (weight_ref, weight_out),
    )
    copies = [pltpu.make_async_copy(source, target, sems.at[at]) for at, (source, target) in enumerate(pairs)]
    for copy in copies:
        copy.start()

    lines_ref[...] = jnp.zeros_like(lines_ref)
    angles = (step_cos_ref, step_sin_ref, part_cos_ref, part_sin_ref)
    base = make_angles(gx * columns + gy * half - HALO, *angles)
    for part, first, count in chunks(half + 2 * HALO):

        def put(at, cosines, sines):
            wave_ref[pl.ds(first + at, 16), pl.ds(0, block_size)] = cosines
            wave_ref[pl.ds(first + at, 16), pl.ds(block_size, block_size)] = sines

        make_waves(base, part, count, *angles, put)

    copies[0].wait()
    copies[1].wait()
    low = volume_here[:, pl.ds(0, half)] + multiplier_here[:, pl.ds(0, half)]
    high = volume_here[:, pl.ds(half, half)] + multiplier_here[:, pl.ds(half, half)]
    outer = (low[:, :HALO], high[:, half - HALO :])
    place = line_places(lines, local_lines)[0]
    lines_ref[place, pl.ds(0, HALO)] = jnp.where(first_core, outer[0], outer[1])
    lines_ref[place, pl.ds(8, HALO)] = jnp.where(first_core, outer[1], outer[0])
    for group in range(2):
        group_lines = pl.ds(group * lines, lines)
        turned = lines_ref[group_lines, :].T
        edge_ref[:, group_lines] = turned[:8]
        edge_sent_ref[:, group_lines] = turned[8:16]

    below, above = low[:, half - HALO :], high[:, :HALO]
    own_ref[:, pl.ds(0, half)] = jnp.where(first_core, low, high)
    own_ref[:, pl.ds(half, HALO)] = jnp.where(first_core, above, below)
    sent_ref[pl.ds(rows, local_lines), :] = jnp.where(first_core, high, low)
    sent_ref[pl.ds(rows + local_lines, local_lines), pl.ds(0, HALO)] = jnp.where(first_core, below, above)
    copies[2].wait()
    sent_ref[pl.ds(0, rows), :] = data_out[...].astype(jnp.float32)
    for copy in copies[3:]:
        copy.wait()


def pack(data, offsets, view_index, taps, view_weight, volume, multiplier):
    rows, samples = data.shape
    local_lines, columns = volume.shape
    block_size = NX // lax.axis_size("ang")
    made = 16 * pl.cdiv(columns // 2 + 2 * HALO, 16)
    parts = 8 * pl.cdiv(pl.cdiv(columns // 2 + 2 * HALO, CHUNK), 8)
    vmem = pl.BlockSpec(memory_space=pltpu.VMEM)
    return pl.pallas_call(
        pack_kernel,
        out_shape=[
            pltpu.VMEM((rows + 2 * local_lines, samples), jnp.float32),
            pltpu.VMEM(data.shape, data.dtype),
            pltpu.VMEM(offsets.shape, offsets.dtype),
            pltpu.VMEM(view_index.shape, view_index.dtype),
            pltpu.VMEM(taps.shape, taps.dtype),
            pltpu.VMEM(view_weight.shape, view_weight.dtype),
            pltpu.VMEM((local_lines, columns // 2 + 128), jnp.float32),
            pltpu.VMEM((made, 2 * block_size), jnp.bfloat16),
            pltpu.VMEM((8, rows), jnp.float32),
            pltpu.VMEM((8, rows), jnp.float32),
        ],
        in_specs=[pl.BlockSpec(memory_space=pltpu.HBM)] * 7,
        out_specs=[vmem] * 10,
        scratch_shapes=[
            pltpu.VMEM(volume.shape, volume.dtype),
            pltpu.VMEM(multiplier.shape, multiplier.dtype),
            pltpu.VMEM((CHUNK // 8, block_size), jnp.float32),
            pltpu.VMEM((CHUNK // 8, block_size), jnp.float32),
            pltpu.VMEM((parts, block_size), jnp.float32),
            pltpu.VMEM((parts, block_size), jnp.float32),
            pltpu.VMEM((rows, 128), jnp.float32),
            pltpu.SemaphoreType.DMA((7,)),
        ],
        compiler_params=pltpu.CompilerParams(vmem_limit_bytes=VMEM_LIMIT),
        name="pack",
    )(
        *(
            pltpu.with_memory_space_constraint(array, pltpu.HBM)
            for array in (data, offsets, view_index, taps, view_weight, volume, multiplier)
        )
    )


def spread_of(offsets, view_index, taps, view_weight):
    block_size = NX // lax.axis_size("ang")
    vmem = pl.BlockSpec(memory_space=pltpu.VMEM)
    return pl.pallas_call(
        make_spread,
        out_shape=pltpu.VMEM((block_size, taps.shape[1]), jnp.bfloat16),
        in_specs=[vmem] * 4,
        out_specs=vmem,
        cost_estimate=pl.CostEstimate(flops=2 * 10**9, transcendentals=0, bytes_accessed=10**6),
        compiler_params=pltpu.CompilerParams(vmem_limit_bytes=VMEM_LIMIT),
        name="spread",
    )(offsets, view_index, taps, view_weight)


def grid_kernel(data_ref, own_ref, got_ref, spread_ref, grid_ref, vm_ref, both_ref, lines_ref):
    rows = data_ref.shape[0]
    lines = rows // 2
    block_size = spread_ref.shape[0]
    local_lines, columns = own_ref.shape[0], own_ref.shape[1] - 128
    gy = lax.axis_index("gy")
    for component in range(2):
        for group, ref in ((gy, data_ref), (1 - gy, got_ref)):
            place = pl.multiple_of((2 * component + group) * lines, 16)
            both_ref[pl.ds(place, lines), :] = ref[pl.ds(component * lines, lines), :].astype(jnp.bfloat16)
    for component in range(2):
        grid_ref[pl.ds(component * block_size, block_size), :] = lax.dot_general(
            spread_ref[...],
            both_ref[pl.ds(2 * component * lines, 2 * lines), :],
            NT,
            preferred_element_type=jnp.float32,
        ).astype(jnp.bfloat16)

    lines_ref[...] = jnp.zeros_like(lines_ref)
    own_place, other_place = line_places(lines, local_lines)
    side = pl.ds(columns, HALO)
    lines_ref[own_place, pl.ds(0, columns)] = own_ref[:, pl.ds(0, columns)]
    lines_ref[own_place, side] = own_ref[:, side]
    lines_ref[other_place, pl.ds(0, columns)] = got_ref[pl.ds(rows, local_lines), :]
    lines_ref[other_place, side] = got_ref[pl.ds(rows + local_lines, local_lines), pl.ds(0, HALO)]
    for group in range(2):
        group_lines = pl.ds(group * lines, lines)
        inner = lines_ref[group_lines, pl.ds(columns, 128)].T[:HALO]
        vm_ref[pl.ds(0, HALO), group_lines] = jnp.where(gy == 0, 0.0, inner)
        vm_ref[pl.ds(HALO + columns, HALO), group_lines] = jnp.where(gy == 0, inner, 0.0)
        for first in range(0, columns, 128):
            vm_ref[pl.ds(HALO + first, 128), group_lines] = lines_ref[group_lines, pl.ds(first, 128)].T


def grid(data, own, got, spread):
    lines = data.shape[0] // 2
    columns = own.shape[1] - 128
    vmem = pl.BlockSpec(memory_space=pltpu.VMEM)
    return pl.pallas_call(
        grid_kernel,
        out_shape=[
            pltpu.VMEM((2 * spread.shape[0], 2 * lines), jnp.bfloat16),
            pltpu.VMEM((columns + 2 * HALO, 2 * lines), jnp.float32),
        ],
        in_specs=[vmem] * 4,
        out_specs=[vmem] * 2,
        scratch_shapes=[
            pltpu.VMEM((4 * lines, data.shape[1]), jnp.bfloat16),
            pltpu.VMEM((2 * lines, columns + 128), jnp.float32),
        ],
        cost_estimate=pl.CostEstimate(flops=10**9, transcendentals=0, bytes_accessed=10**6),
        compiler_params=pltpu.CompilerParams(vmem_limit_bytes=VMEM_LIMIT),
        name="grid",
    )(data, own, got, spread)


def block_kernel(apart, wave_ref, grid_ref, vm_ref, *refs):
    *edge_refs, out_ref = refs
    window = out_ref.shape[0]
    dest = lax.axis_index("ang") ^ apart
    first = pl.multiple_of(dest * (window - 2 * HALO), 16)
    made = 16 * pl.cdiv(window, 16)
    total = jnp.dot(wave_ref[pl.ds(first, made), :], grid_ref[...], preferred_element_type=jnp.float32)
    out_ref[...] = vm_ref[pl.ds(first, window), :] - total[:window] * NX ** (-0.5)
    if edge_refs:
        add_edge(apart, edge_refs[0], out_ref, out_ref)


def add_edge(apart, edge_ref, in_ref, out_ref):
    window = out_ref.shape[0]
    dest, gy = lax.axis_index("ang") ^ apart, lax.axis_index("gy")
    edge = edge_ref[...][:HALO]
    opens = jnp.logical_and(dest == 0, gy == 0)
    closes = jnp.logical_and(dest == lax.axis_size("ang") - 1, gy == 1)
    for at, here in ((pl.ds(0, HALO), opens), (pl.ds(window - HALO, HALO), closes)):
        out_ref[at, :] = in_ref[at, :] + jnp.where(here, edge, 0.0)


def join_kernel(apart, part_ref, edge_ref, out_ref):
    add_edge(apart, edge_ref, part_ref, out_ref)


def join(apart, part, got_edge):
    vmem = pl.BlockSpec(memory_space=pltpu.VMEM)
    return pl.pallas_call(
        functools.partial(join_kernel, apart),
        out_shape=pltpu.VMEM(part.shape, part.dtype),
        in_specs=[vmem] * 2,
        out_specs=vmem,
        input_output_aliases={0: 0},
        compiler_params=pltpu.CompilerParams(vmem_limit_bytes=VMEM_LIMIT),
    )(part, got_edge)


def block_of(apart, wave, grid, vm, *got_edge):
    window = (vm.shape[0] - 2 * HALO) // lax.axis_size("ang") + 2 * HALO
    vmem = pl.BlockSpec(memory_space=pltpu.VMEM)
    return pl.pallas_call(
        functools.partial(block_kernel, apart),
        out_shape=pltpu.VMEM((window, vm.shape[1]), jnp.float32),
        in_specs=[vmem] * (3 + len(got_edge)),
        out_specs=vmem,
        cost_estimate=pl.CostEstimate(flops=10**9, transcendentals=0, bytes_accessed=10**6),
        compiler_params=pltpu.CompilerParams(vmem_limit_bytes=VMEM_LIMIT),
    )(wave, grid, vm, *got_edge)


def on_chip(*arrays):
    return [pltpu.with_memory_space_constraint(array, pltpu.VMEM) for array in arrays]


def project_paired(data, offsets, view_index, taps, view_weight, volume, multiplier):
    sent, data, offsets, view_index, taps, view_weight, own, wave, near, near_sent = pack(
        data, offsets, view_index, taps, view_weight, volume, multiplier
    )
    near_got = lax.ppermute(near_sent, "gy", [(0, 1), (1, 0)])
    got = lax.ppermute(sent, "gy", [(0, 1), (1, 0)])
    spread = spread_of(*on_chip(offsets, view_index, taps, view_weight))
    count = lax.axis_size("gx")
    route = []
    angs = lax.axis_size("ang")
    for ang in range(angs):
        for low in range(count - 1):
            pair = ((2 * ang + 1) * count + low, 2 * ang * count + low + 1)
            route += [pair, pair[::-1]]
        beside = ang ^ 1 if angs > 1 else ang
        route.append((2 * ang * count, 2 * beside * count))
        route.append(((2 * ang + 2) * count - 1, (2 * beside + 2) * count - 1))
    got_edge = lax.ppermute(near + near_got, ("ang", "gy", "gx"), route)
    gridded, vm = grid(*on_chip(data, own, got, spread))
    wave, gridded, vm, got_edge = on_chip(wave, gridded, vm, got_edge)
    parts = []
    for apart in range(angs - 1, 0, -1):
        if apart == angs - 1:
            part = join(apart, *on_chip(block_of(apart, wave, gridded, vm), got_edge))
        else:
            part = block_of(apart, wave, gridded, vm, got_edge)
        parts.append(lax.ppermute(part, "ang", [(ang, ang ^ apart) for ang in range(angs)]))
    return [block_of(0, wave, gridded, vm, got_edge)] + parts


def per_device(spectrum_data, offsets, view_index, kernel, view_weight, volume, multiplier):
    local_planes, rows, columns = volume.shape
    planes = spectrum_data.shape[1]
    samples = spectrum_data.shape[3]
    dests = lax.axis_size("ang") * lax.axis_size("gy")
    local_lines = local_planes * rows
    lines = planes * rows

    volume = volume.reshape(local_lines, columns)
    multiplier = multiplier.reshape(local_lines, columns)
    arrays = (
        spectrum_data.reshape(2 * lines, samples),
        offsets.reshape(samples // 128, 128),
        view_index.reshape(samples // 128, 128),
        kernel,
        view_weight,
        volume,
        multiplier,
    )
    angs = lax.axis_size("ang")
    if lax.axis_size("gy") == 2 and columns // 2 == samples and angs & (angs - 1) == 0:
        parts = project_paired(*arrays)
    else:
        first_edge = volume[:, :HALO] + multiplier[:, :HALO]
        last_edge = volume[:, -HALO:] + multiplier[:, -HALO:]
        even = lax.axis_index("gx") % 2 == 0
        inner = exchanged(jnp.where(even, last_edge, first_edge), "gx", 0)
        outer = exchanged(jnp.where(even, first_edge, last_edge), "gx", 1)
        parts = close(project(*arrays, dests), *on_chip(inner, outer))
        parts = [lax.all_to_all(parts, ("gy", "ang"), split_axis=0, concat_axis=0)]
    done = smooth(on_chip(*parts), planes, local_lines, columns)
    done = lax.all_to_all(done, ("gy", "ang"), split_axis=0, concat_axis=0)
    done = done.reshape(done.shape[0], local_planes, rows, done.shape[2])
    return jnp.transpose(done, (1, 2, 0, 3)).reshape(local_planes, rows, columns)


def solution(mesh):
    placed = (
        P(None, None, "gy", "ang"),
        P("ang"),
        P("ang"),
        P(None, "ang"),
        P(),
        P("ang", "gy", "gx"),
        P("ang", "gy", "gx"),
    )
    return jax.shard_map(per_device, mesh=mesh, in_specs=placed, out_specs=P("ang", "gy", "gx"), check_vma=False)
```

```python
import functools
import math

import jax
import jax.numpy as jnp
from jax import lax
from jax.experimental import pallas as pl
from jax.experimental.pallas import tpu as pltpu
from jax.sharding import PartitionSpec as P


NX = 4096
TV_STEPS = 4
HALO = TV_STEPS
CHUNK = 128
PIECE = 72
VMEM_LIMIT = 24 * 2**20

smooth_weight = 0.5
dual_step = 1.0 / 12.0

NT = (((1,), (1,)), ((), ()))


def unit_circle(phase):
    phase = phase & (NX - 1)
    quarter = (phase + NX // 8) // (NX // 4)
    angle = (phase - quarter * (NX // 4)).astype(jnp.float32) * (2.0 * math.pi / NX)
    square = angle * angle
    sine = angle * (1.0 + square * (-1.0 / 6 + square * (1.0 / 120 + square * (-1.0 / 5040 + square * (1.0 / 362880)))))
    cosine = 1.0 + square * (-0.5 + square * (1.0 / 24 + square * (-1.0 / 720 + square * (1.0 / 40320))))
    odd = (quarter & 1) == 1
    first = jnp.where(odd, -sine, cosine)
    second = jnp.where(odd, cosine, sine)
    flip = (quarter & 2) == 2
    return jnp.where(flip, -first, first), jnp.where(flip, -second, second)


def make_spread(offsets_ref, view_ref, taps_ref, weight_ref, spread_ref):
    block_size, samples = spread_ref.shape
    views = weight_ref.shape[0]
    pieces = []
    for piece in range(samples // 128):
        view = view_ref[pl.ds(piece, 1), :]
        found = jnp.zeros((1, 128), jnp.float32)
        lane = jnp.broadcast_to(view & 127, (8, 128))
        for first in range(0, views, 128):
            table = weight_ref[pl.ds(first, min(128, views - first))].reshape(1, -1)
            if views - first < 128:
                table = jnp.concatenate([table, jnp.zeros((1, 128 - (views - first)), jnp.float32)], axis=1)
            picked = jnp.take_along_axis(jnp.broadcast_to(table, (8, 128)), lane, axis=1)[:1]
            found = jnp.where(view // 128 == first // 128, picked, found)
        pieces.append(found)
    weight = jnp.concatenate(pieces, axis=1)
    values = [weight * taps_ref[pl.ds(tap, 1), :] for tap in range(taps_ref.shape[0])]
    offsets = jnp.concatenate([offsets_ref[pl.ds(piece, 1), :] for piece in range(samples // 128)], axis=1)

    rows = 16
    cell = lax.broadcasted_iota(jnp.int32, (rows, samples), 0)
    starts = [jnp.broadcast_to(offsets + index, (rows, samples)) for index in range(len(values))]
    values = [jnp.broadcast_to(value, (rows, samples)) for value in values]
    for first in range(0, block_size, rows):
        here = cell + first
        spread = jnp.zeros((rows, samples), jnp.float32)
        for start, value in zip(starts, values):
            spread = jnp.where(here == start, value, spread)
        spread_ref[pl.ds(first, rows), :] = spread.astype(jnp.bfloat16)


def make_angles(first_column, step_cos_ref, step_sin_ref, part_cos_ref, part_sin_ref):
    block_size = step_cos_ref.shape[1]
    freq = lax.axis_index("ang") * block_size + lax.broadcasted_iota(jnp.int32, (8, block_size), 1)
    row = lax.broadcasted_iota(jnp.int32, (8, block_size), 0)
    for first in range(0, CHUNK // 8, 8):
        step_cos_ref[pl.ds(first, 8), :], step_sin_ref[pl.ds(first, 8), :] = unit_circle(-freq * (8 * (row + first)))
    for first in range(0, part_cos_ref.shape[0], 8):
        part_cos_ref[pl.ds(first, 8), :], part_sin_ref[pl.ds(first, 8), :] = unit_circle(
            -freq * (CHUNK * (row + first))
        )
    return unit_circle(-freq * (first_column + row))


def make_waves(base, part, count, step_cos_ref, step_sin_ref, part_cos_ref, part_sin_ref, put):
    base_cos, base_sin = base
    part_cos, part_sin = part_cos_ref[pl.ds(part, 1), :], part_sin_ref[pl.ds(part, 1), :]
    here_cos = base_cos * part_cos - base_sin * part_sin
    here_sin = base_sin * part_cos + base_cos * part_sin
    for step in range(0, pl.cdiv(count, 8), 2):
        pair_cos, pair_sin = [], []
        for one in (step, step + 1):
            step_cos, step_sin = step_cos_ref[pl.ds(one, 1), :], step_sin_ref[pl.ds(one, 1), :]
            pair_cos.append(here_cos * step_cos - here_sin * step_sin)
            pair_sin.append(here_sin * step_cos + here_cos * step_sin)
        put(
            8 * step,
            jnp.concatenate(pair_cos, axis=0).astype(jnp.bfloat16),
            jnp.concatenate(pair_sin, axis=0).astype(jnp.bfloat16),
        )


def chunks(total):
    return [(part, part * CHUNK, min(CHUNK, total - part * CHUNK)) for part in range(pl.cdiv(total, CHUNK))]


def put_windows(out_ref, first, count, sent):
    dests, window, _ = out_ref.shape
    block = window - 2 * HALO
    for dest in range(dests):
        low, high = max(first, dest * block), min(first + count, dest * block + window)
        if low < high:
            out_ref[dest, pl.ds(low - dest * block, high - low), :] = sent[low - first : high - first]


def project_kernel(
    data_ref, offsets_ref, view_ref, taps_ref, weight_ref, volume_ref, multiplier_ref,
    out_ref,
    spread_ref, grid_ref, cos_ref, sin_ref, step_cos_ref, step_sin_ref, part_cos_ref, part_sin_ref, lines_ref, vm_ref,
):
    ang, gx = lax.axis_index("ang"), lax.axis_index("gx")
    lines = data_ref.shape[0] // 2
    local_lines, columns = volume_ref.shape

    make_spread(offsets_ref, view_ref, taps_ref, weight_ref, spread_ref)
    grid_ref[...] = lax.dot_general(
        data_ref[...], spread_ref[...], NT, preferred_element_type=jnp.float32
    ).astype(jnp.bfloat16)

    lines_ref[...] = jnp.zeros_like(lines_ref)
    lines_ref[pl.ds(pl.multiple_of(ang * local_lines, 8), local_lines), :] = volume_ref[...] + multiplier_ref[...]
    vm_ref[pl.ds(0, HALO), :] = jnp.zeros((HALO, lines), jnp.float32)
    vm_ref[pl.ds(HALO + columns, HALO), :] = jnp.zeros((HALO, lines), jnp.float32)
    for first in range(0, columns, 128):
        vm_ref[pl.ds(HALO + first, 128), :] = lines_ref[:, pl.ds(first, 128)].T

    angles = (step_cos_ref, step_sin_ref, part_cos_ref, part_sin_ref)
    base = make_angles(gx * columns - HALO, *angles)
    for part, first, count in chunks(columns + 2 * HALO):
        slot = part % 2

        def put(at, cosines, sines):
            cos_ref[slot, pl.ds(at, 16), :] = cosines
            sin_ref[slot, pl.ds(at, 16), :] = sines

        make_waves(base, part, count, *angles, put)
        made = max(16, count)
        total_part = lax.dot_general(
            cos_ref[slot, pl.ds(0, made), :], grid_ref[pl.ds(0, lines), :], NT, preferred_element_type=jnp.float32
        ) + lax.dot_general(
            sin_ref[slot, pl.ds(0, made), :], grid_ref[pl.ds(lines, lines), :], NT, preferred_element_type=jnp.float32
        )
        put_windows(out_ref, first, count, vm_ref[pl.ds(first, count), :] - total_part[:count] * NX ** (-0.5))


def project(data, offsets, view_index, taps, view_weight, volume, multiplier, dests):
    lines = data.shape[0] // 2
    samples = data.shape[1]
    columns = volume.shape[1]
    block_size = NX // lax.axis_size("ang")
    window = columns // dests + 2 * HALO
    parts = pl.cdiv(columns + 2 * HALO, CHUNK)
    vmem = pl.BlockSpec(memory_space=pltpu.VMEM)
    return pl.pallas_call(
        project_kernel,
        out_shape=pltpu.VMEM((dests, window, lines), jnp.float32),
        in_specs=[vmem] * 7,
        out_specs=vmem,
        scratch_shapes=[
            pltpu.VMEM((block_size, samples), jnp.bfloat16),
            pltpu.VMEM((2 * lines, block_size), jnp.bfloat16),
            pltpu.VMEM((2, CHUNK, block_size), jnp.bfloat16),
            pltpu.VMEM((2, CHUNK, block_size), jnp.bfloat16),
            pltpu.VMEM((CHUNK // 8, block_size), jnp.float32),
            pltpu.VMEM((CHUNK // 8, block_size), jnp.float32),
            pltpu.VMEM((8 * pl.cdiv(parts, 8), block_size), jnp.float32),
            pltpu.VMEM((8 * pl.cdiv(parts, 8), block_size), jnp.float32),
            pltpu.VMEM((lines, columns), jnp.float32),
            pltpu.VMEM((columns + 2 * HALO, lines), jnp.float32),
        ],
        cost_estimate=pl.CostEstimate(flops=4 * 10**9, transcendentals=0, bytes_accessed=10**6),
        compiler_params=pltpu.CompilerParams(vmem_limit_bytes=VMEM_LIMIT),
        name="project",
    )(data, offsets, view_index, taps, view_weight, volume, multiplier)


def close_kernel(parts_ref, inner_ref, outer_ref, out_ref, halo_ref):
    ang = lax.axis_index("ang")
    even = lax.axis_index("gx") % 2 == 0
    dests, window, _ = parts_ref.shape
    local_lines = inner_ref.shape[0]
    halo_ref[...] = jnp.zeros_like(halo_ref)
    own = pl.ds(pl.multiple_of(ang * local_lines, 8), local_lines)
    inner, outer = inner_ref[...], outer_ref[...]
    halo_ref[own, pl.ds(0, HALO)] = jnp.where(even, outer, inner)
    halo_ref[own, pl.ds(HALO, HALO)] = jnp.where(even, inner, outer)
    edges = halo_ref[...].T
    out_ref[0, pl.ds(0, HALO), :] = parts_ref[0, pl.ds(0, HALO), :] + edges[:HALO]
    last = pl.ds(window - HALO, HALO)
    out_ref[dests - 1, last, :] = parts_ref[dests - 1, last, :] + edges[HALO : 2 * HALO]


def close(parts, inner, outer):
    vmem = pl.BlockSpec(memory_space=pltpu.VMEM)
    return pl.pallas_call(
        close_kernel,
        out_shape=pltpu.VMEM(parts.shape, parts.dtype),
        in_specs=[vmem] * 3,
        out_specs=vmem,
        scratch_shapes=[pltpu.VMEM((parts.shape[2], 128), jnp.float32)],
        input_output_aliases={0: 0},
        compiler_params=pltpu.CompilerParams(vmem_limit_bytes=VMEM_LIMIT),
        name="close",
    )(parts, inner, outer)


def smooth_kernel(planes, columns, *refs):
    *parts_refs, out_ref, done_ref = refs
    _, local_lines, block = out_ref.shape
    window = parts_refs[0].shape[-2]
    angs, groups = lax.axis_size("ang"), lax.axis_size("gy")
    lines = angs * local_lines
    rows = lines // planes
    size = min(PIECE, window)
    pieces = [(first, min(size, window - first)) for first in range(0, window, size)]
    tiles = len(pieces)
    lanes = [lax.broadcasted_iota(jnp.int32, (height, lines), 1) for _, height in pieces]
    inside = lax.broadcasted_iota(jnp.int32, (8, lines), 0)
    plane_opens = [lane // rows < planes - 1 for lane in lanes]
    row_firsts = [lane % rows == 0 for lane in lanes]
    row_lasts = [lane % rows == rows - 1 for lane in lanes]
    place = lax.axis_index("gy") * angs + lax.axis_index("ang")
    first_column = lax.axis_index("gx") * columns + place * block - HALO
    zero = jnp.float32(0.0)

    def part(ang, group, tile):
        at = pl.ds(*pieces[tile])
        if len(parts_refs) > 1:
            return parts_refs[ang][at, pl.ds(group * lines, lines)]
        return parts_refs[0][group * angs + ang, at, :]

    source = [[sum((part(ang, group, tile) for ang in range(1, angs)), part(0, group, tile)) for group in range(groups)]
              for tile in range(tiles)]

    def divergence(flow, tile):
        rolled = [pltpu.roll(flow[tile][group][1], 1, 1) for group in range(groups)]
        result = []
        for group in range(groups):
            f0, f1, f2 = flow[tile][group]
            wrapped = pltpu.roll(flow[tile][group - 1][1], lines - (rows - 1), 1)
            lower_row = jnp.where(row_firsts[tile], wrapped, rolled[group])
            lower_cell = pltpu.roll(f2, 1, 0)
            if tile > 0:
                before = flow[tile - 1][group][2]
                opening = jnp.where(inside == 0, pltpu.roll(before[-8:], 1, 0), lower_cell[:8])
                lower_cell = jnp.concatenate([opening, lower_cell[8:]], axis=0)
            result.append((f0 - pltpu.roll(f0, rows, 1)) + (f1 - lower_row) + (f2 - lower_cell))
        return result

    def target_of(flow, tile):
        scaled = [value * (dual_step / smooth_weight) for value in source[tile]]
        if flow is None:
            return [-value for value in scaled]
        return [dual_step * div - value for div, value in zip(divergence(flow, tile), scaled)]

    flow = None
    for _ in range(TV_STEPS):
        updated = []
        after = target_of(flow, 0)
        for tile in range(tiles):
            target = after
            after = target_of(flow, tile + 1) if tile + 1 < tiles else target
            _, height = pieces[tile]
            plane_open, row_last = plane_opens[tile], row_lasts[tile]
            moved_groups = []
            for group in range(groups):
                here = target[group]
                slope_plane = jnp.where(plane_open, pltpu.roll(here, lines - rows, 1) - here, zero)
                upper_row = pltpu.roll(here, lines - 1, 1)
                if group + 1 < groups:
                    slope_row = jnp.where(row_last, pltpu.roll(target[group + 1], rows - 1, 1), upper_row) - here
                else:
                    slope_row = jnp.where(row_last, zero, upper_row - here)
                upper_cell = pltpu.roll(here, height - 1, 0)
                if tile + 1 < tiles:
                    closing = jnp.where(inside == 7, pltpu.roll(after[group][:8], 7, 0), upper_cell[-8:])
                    upper_cell = jnp.concatenate([upper_cell[:-8], closing], axis=0)
                slope_cell = upper_cell - here
                if tile == 0:
                    opening = jnp.where(first_column + inside >= 0, slope_cell[:8], zero)
                    slope_cell = jnp.concatenate([opening, slope_cell[8:]], axis=0)
                if tile == tiles - 1:
                    column = first_column + window - 8 + inside
                    closing = jnp.where(column < NX - 1, slope_cell[-8:], zero)
                    slope_cell = jnp.concatenate([slope_cell[:-8], closing], axis=0)
                square = slope_plane * slope_plane + slope_row * slope_row + slope_cell * slope_cell
                scale = 1.0 / (1.0 + square * lax.rsqrt(jnp.maximum(square, 1e-30)))
                moved = [slope_plane, slope_row, slope_cell]
                if flow is not None:
                    moved = [f + m for f, m in zip(flow[tile][group], moved)]
                moved_groups.append([m * scale for m in moved])
            updated.append(moved_groups)
        flow = updated
    for tile in range(tiles):
        for group, div in enumerate(divergence(flow, tile)):
            done_ref[group, pl.ds(*pieces[tile]), :] = source[tile][group] - smooth_weight * div
    for group in range(groups):
        turned = done_ref[group, pl.ds(HALO, block), :].T
        for ang in range(angs):
            out_ref[group * angs + ang] = turned[ang * local_lines : (ang + 1) * local_lines]


def smooth(parts, planes, local_lines, columns):
    window = parts[0].shape[-2]
    dests = lax.axis_size("ang") * lax.axis_size("gy")
    vmem = pl.BlockSpec(memory_space=pltpu.VMEM)
    return pl.pallas_call(
        functools.partial(smooth_kernel, planes, columns),
        out_shape=pltpu.VMEM((dests, local_lines, window - 2 * HALO), jnp.float32),
        in_specs=[vmem] * len(parts),
        out_specs=vmem,
        scratch_shapes=[
            pltpu.VMEM((lax.axis_size("gy"), window, lax.axis_size("ang") * local_lines), jnp.float32)
        ],
        compiler_params=pltpu.CompilerParams(vmem_limit_bytes=VMEM_LIMIT),
        name="smooth",
    )(*parts)


def exchanged(block, axis, shift):
    count = lax.axis_size(axis)
    route = []
    for low in range(shift, count + shift - 1, 2):
        pair = (low % count, (low + 1) % count)
        route += [pair, pair[::-1]]
    return lax.ppermute(block, axis, route)


def line_places(lines, local_lines):
    gy, inner = lax.axis_index("gy"), lax.axis_index("ang") * local_lines
    return [
        pl.ds(pl.multiple_of(group * lines + inner, 8), local_lines) for group in (gy, 1 - gy)
    ]


def pack_kernel(
    data_ref, offsets_ref, view_ref, taps_ref, weight_ref, volume_ref, multiplier_ref,
    sent_ref, data_out, offsets_out, view_out, taps_out, weight_out, own_ref, wave_ref, edge_ref, edge_sent_ref,
    volume_here, multiplier_here, step_cos_ref, step_sin_ref, part_cos_ref, part_sin_ref, lines_ref, sems,
):
    rows = data_ref.shape[0]
    lines = rows // 2
    local_lines, columns = volume_ref.shape
    half = columns // 2
    block_size = wave_ref.shape[1] // 2
    gx, gy = lax.axis_index("gx"), lax.axis_index("gy")
    first_core = gy == 0
    pairs = (
        (data_ref, data_out),
        (volume_ref, volume_here),
        (multiplier_ref, multiplier_here),
        (offsets_ref, offsets_out),
        (view_ref, view_out),
        (taps_ref, taps_out),
        (weight_ref, weight_out),
    )
    copies = [pltpu.make_async_copy(source, target, sems.at[at]) for at, (source, target) in enumerate(pairs)]
    for copy in copies:
        copy.start()

    lines_ref[...] = jnp.zeros_like(lines_ref)
    angles = (step_cos_ref, step_sin_ref, part_cos_ref, part_sin_ref)
    base = make_angles(gx * columns + gy * half - HALO, *angles)
    for part, first, count in chunks(half + 2 * HALO):

        def put(at, cosines, sines):
            wave_ref[pl.ds(first + at, 16), pl.ds(0, block_size)] = cosines
            wave_ref[pl.ds(first + at, 16), pl.ds(block_size, block_size)] = sines

        make_waves(base, part, count, *angles, put)

    for copy in copies:
        copy.wait()
    sent_ref[pl.ds(0, rows), :] = data_out[...].astype(jnp.float32)
    low = volume_here[:, pl.ds(0, half)] + multiplier_here[:, pl.ds(0, half)]
    high = volume_here[:, pl.ds(half, half)] + multiplier_here[:, pl.ds(half, half)]
    outer = (low[:, :HALO], high[:, half - HALO :])
    place = line_places(lines, local_lines)[0]
    lines_ref[place, pl.ds(0, HALO)] = jnp.where(first_core, outer[0], outer[1])
    lines_ref[place, pl.ds(8, HALO)] = jnp.where(first_core, outer[1], outer[0])
    for group in range(2):
        group_lines = pl.ds(group * lines, lines)
        turned = lines_ref[group_lines, :].T
        edge_ref[:, group_lines] = turned[:8]
        edge_sent_ref[:, group_lines] = turned[8:16]

    below, above = low[:, half - HALO :], high[:, :HALO]
    own_ref[:, pl.ds(0, half)] = jnp.where(first_core, low, high)
    own_ref[:, pl.ds(half, HALO)] = jnp.where(first_core, above, below)
    sent_ref[pl.ds(rows, local_lines), :] = jnp.where(first_core, high, low)
    sent_ref[pl.ds(rows + local_lines, local_lines), pl.ds(0, HALO)] = jnp.where(first_core, below, above)


def pack(data, offsets, view_index, taps, view_weight, volume, multiplier):
    rows, samples = data.shape
    local_lines, columns = volume.shape
    block_size = NX // lax.axis_size("ang")
    made = 16 * pl.cdiv(columns // 2 + 2 * HALO, 16)
    parts = 8 * pl.cdiv(pl.cdiv(columns // 2 + 2 * HALO, CHUNK), 8)
    vmem = pl.BlockSpec(memory_space=pltpu.VMEM)
    return pl.pallas_call(
        pack_kernel,
        out_shape=[
            pltpu.VMEM((rows + 2 * local_lines, samples), jnp.float32),
            pltpu.VMEM(data.shape, data.dtype),
            pltpu.VMEM(offsets.shape, offsets.dtype),
            pltpu.VMEM(view_index.shape, view_index.dtype),
            pltpu.VMEM(taps.shape, taps.dtype),
            pltpu.VMEM(view_weight.shape, view_weight.dtype),
            pltpu.VMEM((local_lines, columns // 2 + 128), jnp.float32),
            pltpu.VMEM((made, 2 * block_size), jnp.bfloat16),
            pltpu.VMEM((8, rows), jnp.float32),
            pltpu.VMEM((8, rows), jnp.float32),
        ],
        in_specs=[pl.BlockSpec(memory_space=pltpu.HBM)] * 7,
        out_specs=[vmem] * 10,
        scratch_shapes=[
            pltpu.VMEM(volume.shape, volume.dtype),
            pltpu.VMEM(multiplier.shape, multiplier.dtype),
            pltpu.VMEM((CHUNK // 8, block_size), jnp.float32),
            pltpu.VMEM((CHUNK // 8, block_size), jnp.float32),
            pltpu.VMEM((parts, block_size), jnp.float32),
            pltpu.VMEM((parts, block_size), jnp.float32),
            pltpu.VMEM((rows, 128), jnp.float32),
            pltpu.SemaphoreType.DMA((7,)),
        ],
        compiler_params=pltpu.CompilerParams(vmem_limit_bytes=VMEM_LIMIT),
        name="pack",
    )(
        *(
            pltpu.with_memory_space_constraint(array, pltpu.HBM)
            for array in (data, offsets, view_index, taps, view_weight, volume, multiplier)
        )
    )


def spread_of(offsets, view_index, taps, view_weight):
    block_size = NX // lax.axis_size("ang")
    vmem = pl.BlockSpec(memory_space=pltpu.VMEM)
    return pl.pallas_call(
        make_spread,
        out_shape=pltpu.VMEM((block_size, taps.shape[1]), jnp.bfloat16),
        in_specs=[vmem] * 4,
        out_specs=vmem,
        cost_estimate=pl.CostEstimate(flops=2 * 10**9, transcendentals=0, bytes_accessed=10**6),
        compiler_params=pltpu.CompilerParams(vmem_limit_bytes=VMEM_LIMIT),
        name="spread",
    )(offsets, view_index, taps, view_weight)


def grid_kernel(data_ref, own_ref, got_ref, spread_ref, grid_ref, vm_ref, both_ref, lines_ref):
    rows = data_ref.shape[0]
    lines = rows // 2
    block_size = spread_ref.shape[0]
    local_lines, columns = own_ref.shape[0], own_ref.shape[1] - 128
    gy = lax.axis_index("gy")
    for component in range(2):
        for group, ref in ((gy, data_ref), (1 - gy, got_ref)):
            place = pl.multiple_of((2 * component + group) * lines, 16)
            both_ref[pl.ds(place, lines), :] = ref[pl.ds(component * lines, lines), :].astype(jnp.bfloat16)
    for component in range(2):
        grid_ref[pl.ds(component * block_size, block_size), :] = lax.dot_general(
            spread_ref[...],
            both_ref[pl.ds(2 * component * lines, 2 * lines), :],
            NT,
            preferred_element_type=jnp.float32,
        ).astype(jnp.bfloat16)

    lines_ref[...] = jnp.zeros_like(lines_ref)
    own_place, other_place = line_places(lines, local_lines)
    side = pl.ds(columns, HALO)
    lines_ref[own_place, pl.ds(0, columns)] = own_ref[:, pl.ds(0, columns)]
    lines_ref[own_place, side] = own_ref[:, side]
    lines_ref[other_place, pl.ds(0, columns)] = got_ref[pl.ds(rows, local_lines), :]
    lines_ref[other_place, side] = got_ref[pl.ds(rows + local_lines, local_lines), pl.ds(0, HALO)]
    for group in range(2):
        group_lines = pl.ds(group * lines, lines)
        inner = lines_ref[group_lines, pl.ds(columns, 128)].T[:HALO]
        vm_ref[pl.ds(0, HALO), group_lines] = jnp.where(gy == 0, 0.0, inner)
        vm_ref[pl.ds(HALO + columns, HALO), group_lines] = jnp.where(gy == 0, inner, 0.0)
        for first in range(0, columns, 128):
            vm_ref[pl.ds(HALO + first, 128), group_lines] = lines_ref[group_lines, pl.ds(first, 128)].T


def grid(data, own, got, spread):
    lines = data.shape[0] // 2
    columns = own.shape[1] - 128
    vmem = pl.BlockSpec(memory_space=pltpu.VMEM)
    return pl.pallas_call(
        grid_kernel,
        out_shape=[
            pltpu.VMEM((2 * spread.shape[0], 2 * lines), jnp.bfloat16),
            pltpu.VMEM((columns + 2 * HALO, 2 * lines), jnp.float32),
        ],
        in_specs=[vmem] * 4,
        out_specs=[vmem] * 2,
        scratch_shapes=[
            pltpu.VMEM((4 * lines, data.shape[1]), jnp.bfloat16),
            pltpu.VMEM((2 * lines, columns + 128), jnp.float32),
        ],
        cost_estimate=pl.CostEstimate(flops=10**9, transcendentals=0, bytes_accessed=10**6),
        compiler_params=pltpu.CompilerParams(vmem_limit_bytes=VMEM_LIMIT),
        name="grid",
    )(data, own, got, spread)


def block_kernel(apart, wave_ref, grid_ref, vm_ref, *refs):
    *edge_refs, out_ref = refs
    window = out_ref.shape[0]
    dest = lax.axis_index("ang") ^ apart
    first = pl.multiple_of(dest * (window - 2 * HALO), 16)
    made = 16 * pl.cdiv(window, 16)
    total = jnp.dot(wave_ref[pl.ds(first, made), :], grid_ref[...], preferred_element_type=jnp.float32)
    out_ref[...] = vm_ref[pl.ds(first, window), :] - total[:window] * NX ** (-0.5)
    if edge_refs:
        add_edge(apart, edge_refs[0], out_ref, out_ref)


def add_edge(apart, edge_ref, in_ref, out_ref):
    window = out_ref.shape[0]
    dest, gy = lax.axis_index("ang") ^ apart, lax.axis_index("gy")
    edge = edge_ref[...][:HALO]
    opens = jnp.logical_and(dest == 0, gy == 0)
    closes = jnp.logical_and(dest == lax.axis_size("ang") - 1, gy == 1)
    for at, here in ((pl.ds(0, HALO), opens), (pl.ds(window - HALO, HALO), closes)):
        out_ref[at, :] = in_ref[at, :] + jnp.where(here, edge, 0.0)


def join_kernel(apart, part_ref, edge_ref, out_ref):
    add_edge(apart, edge_ref, part_ref, out_ref)


def join(apart, part, got_edge):
    vmem = pl.BlockSpec(memory_space=pltpu.VMEM)
    return pl.pallas_call(
        functools.partial(join_kernel, apart),
        out_shape=pltpu.VMEM(part.shape, part.dtype),
        in_specs=[vmem] * 2,
        out_specs=vmem,
        input_output_aliases={0: 0},
        compiler_params=pltpu.CompilerParams(vmem_limit_bytes=VMEM_LIMIT),
    )(part, got_edge)


def block_of(apart, wave, grid, vm, *got_edge):
    window = (vm.shape[0] - 2 * HALO) // lax.axis_size("ang") + 2 * HALO
    vmem = pl.BlockSpec(memory_space=pltpu.VMEM)
    return pl.pallas_call(
        functools.partial(block_kernel, apart),
        out_shape=pltpu.VMEM((window, vm.shape[1]), jnp.float32),
        in_specs=[vmem] * (3 + len(got_edge)),
        out_specs=vmem,
        cost_estimate=pl.CostEstimate(flops=10**9, transcendentals=0, bytes_accessed=10**6),
        compiler_params=pltpu.CompilerParams(vmem_limit_bytes=VMEM_LIMIT),
    )(wave, grid, vm, *got_edge)


def on_chip(*arrays):
    return [pltpu.with_memory_space_constraint(array, pltpu.VMEM) for array in arrays]


def project_paired(data, offsets, view_index, taps, view_weight, volume, multiplier):
    sent, data, offsets, view_index, taps, view_weight, own, wave, near, near_sent = pack(
        data, offsets, view_index, taps, view_weight, volume, multiplier
    )
    near_got = lax.ppermute(near_sent, "gy", [(0, 1), (1, 0)])
    got = lax.ppermute(sent, "gy", [(0, 1), (1, 0)])
    spread = spread_of(*on_chip(offsets, view_index, taps, view_weight))
    count = lax.axis_size("gx")
    route = []
    angs = lax.axis_size("ang")
    for ang in range(angs):
        for low in range(count - 1):
            pair = ((2 * ang + 1) * count + low, 2 * ang * count + low + 1)
            route += [pair, pair[::-1]]
        beside = ang ^ 1 if angs > 1 else ang
        route.append((2 * ang * count, 2 * beside * count))
        route.append(((2 * ang + 2) * count - 1, (2 * beside + 2) * count - 1))
    got_edge = lax.ppermute(near + near_got, ("ang", "gy", "gx"), route)
    gridded, vm = grid(*on_chip(data, own, got, spread))
    wave, gridded, vm, got_edge = on_chip(wave, gridded, vm, got_edge)
    parts = []
    for apart in range(angs - 1, 0, -1):
        if apart == angs - 1:
            part = join(apart, *on_chip(block_of(apart, wave, gridded, vm), got_edge))
        else:
            part = block_of(apart, wave, gridded, vm, got_edge)
        parts.append(lax.ppermute(part, "ang", [(ang, ang ^ apart) for ang in range(angs)]))
    return [block_of(0, wave, gridded, vm, got_edge)] + parts


def per_device(spectrum_data, offsets, view_index, kernel, view_weight, volume, multiplier):
    local_planes, rows, columns = volume.shape
    planes = spectrum_data.shape[1]
    samples = spectrum_data.shape[3]
    dests = lax.axis_size("ang") * lax.axis_size("gy")
    local_lines = local_planes * rows
    lines = planes * rows

    volume = volume.reshape(local_lines, columns)
    multiplier = multiplier.reshape(local_lines, columns)
    arrays = (
        spectrum_data.reshape(2 * lines, samples),
        offsets.reshape(samples // 128, 128),
        view_index.reshape(samples // 128, 128),
        kernel,
        view_weight,
        volume,
        multiplier,
    )
    angs = lax.axis_size("ang")
    if lax.axis_size("gy") == 2 and columns // 2 == samples and angs & (angs - 1) == 0:
        parts = project_paired(*arrays)
    else:
        first_edge = volume[:, :HALO] + multiplier[:, :HALO]
        last_edge = volume[:, -HALO:] + multiplier[:, -HALO:]
        even = lax.axis_index("gx") % 2 == 0
        inner = exchanged(jnp.where(even, last_edge, first_edge), "gx", 0)
        outer = exchanged(jnp.where(even, first_edge, last_edge), "gx", 1)
        parts = close(project(*arrays, dests), *on_chip(inner, outer))
        parts = [lax.all_to_all(parts, ("gy", "ang"), split_axis=0, concat_axis=0)]
    done = smooth(on_chip(*parts), planes, local_lines, columns)
    done = lax.all_to_all(done, ("gy", "ang"), split_axis=0, concat_axis=0)
    done = done.reshape(done.shape[0], local_planes, rows, done.shape[2])
    return jnp.transpose(done, (1, 2, 0, 3)).reshape(local_planes, rows, columns)


def solution(mesh):
    placed = (
        P(None, None, "gy", "ang"),
        P("ang"),
        P("ang"),
        P(None, "ang"),
        P(),
        P("ang", "gy", "gx"),
        P("ang", "gy", "gx"),
    )
    return jax.shard_map(per_device, mesh=mesh, in_specs=placed, out_specs=P("ang", "gy", "gx"), check_vma=False)
```
